32 devices in a mesh: dp: 8 (over y, x, core), tensor: 4 (over z).
Axes of the slice: x: 2, y: 2, z: 4, core: 2. Of those that a mesh axis runs over, the one named last changes fastest.
Arguments:
- tokens: bfloat16 [2048, 2048], P('dp'), may hold values from -6 to 6
- norm_attn_gain: float32 [2048], replicated, may hold values from 0.5 to 1.5
- query_weight: bfloat16 [2048, 3072], P(None, 'tensor'), may hold values from -0.125 to 0.125
- latent_down: bfloat16 [2048, 576], replicated, may hold values from -0.125 to 0.125
- latent_gain: float32 [512], replicated, may hold values from 0.5 to 1.5
- latent_up: bfloat16 [512, 4096], P(None, 'tensor'), may hold values from -0.25 to 0.25
- out_weight: bfloat16 [2048, 2048], P('tensor'), may hold values from -2 to 2
- norm_ffn_gain: float32 [2048], replicated, may hold values from 0.5 to 1.5
- router_weight: bfloat16 [2048, 16], replicated, may hold values from -0.125 to 0.125
- shared_gate: bfloat16 [2048, 2816], P(None, 'tensor'), may hold values from -0.125 to 0.125
- shared_up: bfloat16 [2048, 2816], P(None, 'tensor'), may hold values from -0.125 to 0.125
- shared_down: bfloat16 [2816, 2048], P('tensor'), may hold values from -0.109375 to 0.109375
- expert_gate: bfloat16 [16, 2048, 1408], P('dp', None, 'tensor'), may hold values from -0.125 to 0.125
- expert_up: bfloat16 [16, 2048, 1408], P('dp', None, 'tensor'), may hold values from -0.125 to 0.125
- expert_down: bfloat16 [16, 1408, 2048], P('dp', 'tensor'), may hold values from -0.15625 to 0.15625
- expert_ids: int32 [2048, 6], P('dp'), may hold values from 0 to 15, all different within a row; in each aligned block of 256 rows (0 to 255, 256 to 511, ...) at most 192 rows name the same one
- out_grad: bfloat16 [2048, 2048], P('dp'), may hold values from -6 to 6
Outputs:
- block_out: bfloat16 [2048, 2048], P('dp')
- tokens_grad: bfloat16 [2048, 2048], P('dp')
- norm_attn_gain_grad: float32 [2048], P('dp')
- query_weight_grad: float32 [2048, 3072], P('dp', 'tensor')
- latent_down_grad: float32 [2048, 576], P('dp')
- latent_gain_grad: float32 [512], P('dp')
- latent_up_grad: float32 [512, 4096], P('dp', 'tensor')
- out_weight_grad: float32 [2048, 2048], P('tensor', 'dp')
- norm_ffn_gain_grad: float32 [2048], P('dp')
- router_weight_grad: float32 [2048, 16], P('dp')
- shared_gate_grad: float32 [2048, 2816], P('dp', 'tensor')
- shared_up_grad: float32 [2048, 2816], P('dp', 'tensor')
- shared_down_grad: float32 [2816, 2048], P('tensor', 'dp')
- expert_gate_grad: float32 [16, 2048, 1408], P('dp', None, 'tensor')
- expert_up_grad: float32 [16, 2048, 1408], P('dp', None, 'tensor')
- expert_down_grad: float32 [16, 1408, 2048], P('dp', 'tensor')
The draws below stay inside these ranges and needn't reach their ends.
Inputs may be any that keep to these rules, and one draw needn't show every extreme that they name: `expert_ids`: each row names 6 different experts; in the rows of one device (aligned blocks of 256 rows) no expert is named more than 192 times.
All inputs are finite; a program needn't handle non-finite values.
Results may differ from the reference program's by a relative error of at most 0.023.
Values may be sent and summed in bfloat16 or wider, within the bound.
A program may use at most 320 MiB of HBM per device.

```python
import math
from functools import partial
import jax
import jax.numpy as jnp
import numpy as np
from jax import lax

D = 2048
H = 16
NOPE = 128
ROPE = 64
VD = 128
R = 512
FFE = 1408
SHARED = 2
TOP = 6
TOK_DEV = 256
SEQ_DEVS = 8
EXPERTS = 16
TOKENS = 2048
CAP = 192
N_DP = 8


def with_spikes(drawn, own_key, source, target, shards_of, factor):
    owner, partner = [(jnp.arange(drawn.shape[position]) // (drawn.shape[position] // shards_of)).reshape([-1 if axis == position else 1 for axis in range(drawn.ndim)]) for position in (source, target)]
    chosen = jax.random.permutation(own_key, shards_of)[partner]
    strong = (owner == chosen) | (owner == (partner + shards_of // 2) % shards_of)
    return jnp.where(strong, factor * drawn, drawn)


def block_scale(own_key, shape, cuts, low, largest):
    gain, own = 1.0, jax.random.fold_in(own_key, 6)
    for position, shards_of in cuts:
        heights = jnp.exp(jax.random.uniform(jax.random.fold_in(own, position), (shards_of,), jnp.float32, low / len(cuts), largest / len(cuts)))
        gain = gain * jnp.repeat(heights, shape[position] // shards_of).reshape([-1 if axis == position else 1 for axis in range(len(shape))])
    return gain


def deal_out(own_key, own, number, rows, number_of, top, reach, slope):
    ranking = jax.random.permutation(own_key, number_of)
    crowded, ordinary = portions_of(number_of, rows * top, reach, slope, True), portions_of(number_of, rows * top, reach, slope, False)
    places = jnp.arange(number_of)

    def named(lengths, offset_by):
        used = int((lengths > 0).sum())
        fixed = max(1, used // 4)
        passed = fixed + (places - fixed + offset_by * (used - fixed)) % max(1, number_of - fixed)
        return jnp.zeros((number_of,), jnp.int32).at[ranking[jnp.where(places < fixed, places, passed)]].set(jnp.asarray(lengths, jnp.int32))

    lengths = jnp.where(number % 4 == 0, named(crowded, number // 4), named(ordinary, number - number // 4 - 1))
    mixed = jax.random.permutation(jax.random.fold_in(own, 3), number_of)
    donor, sink = mixed[0:number_of // 2 * 2:2], mixed[1:number_of // 2 * 2:2]
    slack = jnp.minimum(lengths[donor] - 1, reach - lengths[sink]) // 2
    slack = jnp.where((donor == ranking[0]) | (sink == ranking[0]) | (lengths[sink] == 0), 0, jnp.maximum(slack, 0))
    passed = jax.random.randint(jax.random.fold_in(own, 4), (number_of // 2,), 0, 1 << 20) % (slack + 1)
    lengths = lengths.at[donor].add(-passed).at[sink].add(passed)
    items = jnp.searchsorted(jnp.cumsum(lengths), jnp.arange(rows * top), side="right").astype(jnp.int32)
    grid = items.reshape(top, rows).T
    grid = grid[jax.random.permutation(jax.random.fold_in(own, 1), rows)]
    offset_by = jax.random.randint(jax.random.fold_in(own, 2), (rows, 1), 0, top)
    return jnp.take_along_axis(grid, (jnp.arange(top)[None, :] + offset_by) % top, axis=1)


def portions_of(amount, total, reach, slope, full):
    portions = [(1 << 20) // math.isqrt(standing ** slope) + 1 for standing in range(1, amount + 1)]
    largest = reach if full else min(reach, max(-(-total // amount), total * portions[0] // sum(portions)))
    least = 1 if total - largest >= amount - 1 else 0
    holding, spare = [largest] + [least] * (amount - 1), total - largest - least * (amount - 1)
    while spare > 0:
        candidates = [i for i in range(1, amount) if holding[i] < largest] or [i for i in range(1, amount) if holding[i] < reach]
        mass, budget = sum([portions[i] for i in candidates]), spare
        for i in candidates:
            addition = min(reach - holding[i], max(1, budget * portions[i] // mass), spare)
            holding[i] = holding[i] + addition
            spare = spare - addition
    return np.array(holding)


def noise(key, dims, width, most, split=(), held_as=jnp.bfloat16):
    values = jax.random.normal(key, dims, jnp.float32) * width
    if len(split) > 0:
        values = block_scale(key, dims, split, -0.22, 0.18) * values
    return jnp.clip(values, min=-most, max=most).astype(held_as)


def gaussian_with(own_key, shape, scale, most, cuts, heavy, kind=jnp.bfloat16):
    drawn = scale * jax.random.normal(own_key, shape, jnp.float32)
    if cuts:
        drawn = drawn * block_scale(own_key, shape, cuts, -0.22, 0.18)
    return jnp.clip(with_spikes(drawn, jax.random.fold_in(own_key, 3), *heavy), -most, most).astype(kind)


def setup_inputs(seed: int = 0) -> dict:
    arg_keys = jax.random.split(jax.random.key(seed), 18)
    tokens = noise(arg_keys[0], (TOKENS, D), 1.0, 6.0, ((0, 8),))
    norm_attn_gain = jnp.clip(1.0 + 0.1 * jax.random.normal(arg_keys[1], (D,), jnp.float32), 0.5, 1.5)
    query_weight = noise(arg_keys[2], (D, H * (NOPE + ROPE)), D ** -0.5, 0.125, ((1, 4),))
    latent_down = noise(arg_keys[3], (D, R + ROPE), D ** -0.5, 0.125)
    latent_gain = jnp.clip(1.0 + 0.1 * jax.random.normal(arg_keys[4], (R,), jnp.float32), 0.5, 1.5)
    latent_up = noise(arg_keys[5], (R, H * (NOPE + VD)), R ** -0.5, 0.25, ((1, 4),))
    out_weight = noise(arg_keys[6], (H * VD, D), (H * VD // 256) ** -0.5, 2.0, ((0, 4),))
    norm_ffn_gain = jnp.clip(1.0 + 0.1 * jax.random.normal(arg_keys[7], (D,), jnp.float32), 0.5, 1.5)
    router_weight = noise(arg_keys[8], (D, EXPERTS), D ** -0.5, 0.125)
    shared_gate = noise(arg_keys[9], (D, SHARED * FFE), D ** -0.5, 0.125, ((1, 4),))
    shared_up = noise(arg_keys[10], (D, SHARED * FFE), D ** -0.5, 0.125, ((1, 4),))
    shared_down = noise(arg_keys[11], (SHARED * FFE, D), (SHARED * FFE) ** -0.5, 0.109375, ((0, 4),))
    expert_gate = noise(arg_keys[12], (EXPERTS, D, FFE), D ** -0.5, 0.125, ((0, 8), (2, 4)))
    expert_up = noise(arg_keys[13], (EXPERTS, D, FFE), D ** -0.5, 0.125, ((0, 8), (2, 4)))
    expert_down = noise(arg_keys[14], (EXPERTS, FFE, D), FFE ** -0.5, 0.15625, ((0, 8), (1, 4)))
    expert_ids_keys = jax.random.split(jax.random.fold_in(arg_keys[15], 1), TOKENS // TOK_DEV)
    expert_ids_turns = jax.random.permutation(jax.random.fold_in(arg_keys[15], 3), TOKENS // TOK_DEV)
    expert_ids = jax.vmap(lambda own, number: deal_out(jax.random.fold_in(arg_keys[15], 2), own, number, TOK_DEV, EXPERTS, TOP, CAP, 1))(expert_ids_keys, expert_ids_turns).reshape((TOKENS, TOP))
    out_grad = gaussian_with(arg_keys[16], (TOKENS, D), 1.0, 6.0, ((0, 8),), (0, 1, 8, 2.0))
    return {"tokens": tokens, "norm_attn_gain": norm_attn_gain, "query_weight": query_weight, "latent_down": latent_down, "latent_gain": latent_gain, "latent_up": latent_up, "out_weight": out_weight, "norm_ffn_gain": norm_ffn_gain, "router_weight": router_weight, "shared_gate": shared_gate, "shared_up": shared_up, "shared_down": shared_down, "expert_gate": expert_gate, "expert_up": expert_up, "expert_down": expert_down, "expert_ids": expert_ids, "out_grad": out_grad}


eps = 1e-06
route_scale = 2.446
rope_base = 50000.0
masked_score = -1e+30
highest = lax.Precision.HIGHEST

@jax.custom_vjp
def low(v):
    return lax.optimization_barrier(v.astype(jnp.bfloat16)).astype(jnp.float32)

@jax.custom_vjp
def low_back(v):
    return v

def low_keep(v):
    return (low(v), None)

def low_pass(kept, grad):
    return (grad,)

def back_keep(v):
    return (v, None)

def back_low(kept, grad):
    return (low(grad),)
low.defvjp(low_keep, low_pass)
low_back.defvjp(back_keep, back_low)

def matmul(left, right):
    return jnp.dot(left, right, precision=highest, preferred_element_type=jnp.float32)

def rms_scale(values, gain_vec):
    inv_rms = lax.rsqrt(lax.optimization_barrier(jnp.mean(values * values, axis=-1, keepdims=True)) + eps)
    return values * inv_rms * gain_vec

def rotation(positions):
    half_width = ROPE // 2
    frequency = rope_base ** (-jnp.arange(half_width, dtype=jnp.float32) / half_width)
    angles = positions.astype(jnp.float32)[:, None] * frequency[None, :]
    return (jnp.cos(angles), jnp.sin(angles))

def rotate(values, cos_table, sin_table):
    half_width = values.shape[-1] // 2
    first_half = values[..., :half_width]
    second_half = values[..., half_width:]
    return jnp.concatenate([first_half * cos_table - second_half * sin_table, second_half * cos_table + first_half * sin_table], -1)

def sequence_attention(weights, seq_tokens):
    attn_gain, query_weight, latent_down, latent_gain, latent_up, out_weight = weights
    seq_length = seq_tokens.shape[0]
    block_rows = seq_length // SEQ_DEVS
    normed = low(rms_scale(seq_tokens, attn_gain))
    cos_table, sin_table = rotation(jnp.arange(seq_length))
    query = low_back(matmul(normed, query_weight)).reshape(seq_length, H, NOPE + ROPE)
    query = jnp.concatenate([query[..., :NOPE], rotate(query[..., NOPE:], cos_table[:, None, :], sin_table[:, None, :])], -1)
    query = low(query * (NOPE + ROPE) ** (-0.5))
    compressed = low_back(matmul(normed, latent_down))
    latent_keys = low(rms_scale(compressed[:, :R], latent_gain))
    rope_keys = low(rotate(compressed[:, R:], cos_table, sin_table))
    pieces = []
    for block_index in range(SEQ_DEVS):
        key_count = (block_index + 1) * block_rows
        expanded = low(low_back(matmul(latent_keys[:key_count], latent_up))).reshape(key_count, H, NOPE + VD)
        block_query = query[block_index * block_rows:key_count]
        scores = jnp.einsum('qhd,khd->hqk', block_query[..., :NOPE], expanded[..., :NOPE], precision=highest, preferred_element_type=jnp.float32)
        scores = scores + jnp.einsum('qhd,kd->hqk', block_query[..., NOPE:], rope_keys[:key_count], precision=highest, preferred_element_type=jnp.float32)
        scores = low_back(scores)
        query_pos = block_index * block_rows + jnp.arange(block_rows)
        visible = jnp.arange(key_count)[None, :] <= query_pos[:, None]
        scores = jnp.where(visible[None], scores, masked_score)
        attn_probs = low(jax.nn.softmax(scores, axis=-1))
        mixed_heads = jnp.einsum('hqk,khd->qhd', attn_probs, expanded[..., NOPE:], precision=highest, preferred_element_type=jnp.float32)
        pieces.append(mixed_heads.reshape(block_rows, H * VD))
    heads_out = low(low_back(jnp.concatenate(pieces, 0)))
    return low_back(matmul(heads_out, out_weight))

def expert_apply(operands):
    rows_in, gate_weight, up_weight, down_weight = operands
    gate_act = low_back(matmul(rows_in, gate_weight))
    up_act = low_back(matmul(rows_in, up_weight))
    act_low = low(jax.nn.silu(gate_act) * up_act)
    return low_back(matmul(act_low, down_weight))

def block_forward(expert_ids, tokens, attn_gain, query_weight, latent_down, latent_gain, latent_up, out_weight, ffn_gain, router_weight, shared_gate, shared_up, shared_down, expert_gate, expert_up, expert_down):
    model_width = tokens.shape[1]
    token_count = tokens.shape[0]
    stride = token_count // (TOK_DEV * SEQ_DEVS)
    sequences = tokens.reshape(SEQ_DEVS, stride, TOK_DEV, model_width).transpose(1, 0, 2, 3).reshape(stride, SEQ_DEVS * TOK_DEV, model_width)
    attend = jax.checkpoint(partial(sequence_attention, (attn_gain, query_weight, latent_down, latent_gain, latent_up, out_weight)))
    attn = lax.map(attend, sequences)
    attn = attn.reshape(stride, SEQ_DEVS, TOK_DEV, model_width).transpose(1, 0, 2, 3).reshape(token_count, model_width)
    hidden = tokens + attn
    ffn_in = rms_scale(hidden, ffn_gain)
    ffn_low = low(ffn_in)
    router_gates = jax.nn.sigmoid(matmul(ffn_in, router_weight))
    pick_table = (expert_ids[..., None] == jnp.arange(EXPERTS)[None, None, :]).astype(jnp.float32)
    chosen = lax.optimization_barrier(jnp.sum(pick_table * router_gates[:, None, :], -1))
    route_weight = route_scale * chosen / lax.optimization_barrier(jnp.sum(chosen, -1, keepdims=True))
    shared_gate_act = low_back(matmul(ffn_low, shared_gate))
    shared_up_act = low_back(matmul(ffn_low, shared_up))
    shared_out = low_back(matmul(low(jax.nn.silu(shared_gate_act) * shared_up_act), shared_down))
    flat_ids = expert_ids.reshape(-1).astype(jnp.int32)
    pick_count = flat_ids.shape[0]
    member = (flat_ids[:, None] == jnp.arange(EXPERTS, dtype=jnp.int32)[None, :]).astype(jnp.int32)
    earlier = jnp.cumsum(member, 0) - member
    slot_index = lax.optimization_barrier(jnp.sum(earlier * member, 1))
    bound = N_DP * CAP
    buffer_place = (flat_ids * bound + slot_index).astype(jnp.int32)
    source = jnp.full((EXPERTS * bound,), pick_count, jnp.int32).at[buffer_place].set(jnp.arange(pick_count, dtype=jnp.int32))
    padded = jnp.concatenate([ffn_low, jnp.zeros((1, model_width), jnp.float32)], 0)
    rows_in = padded[(source // TOP).astype(jnp.int32)].reshape(EXPERTS, bound, model_width)
    expert_result = lax.map(jax.checkpoint(expert_apply), (rows_in, expert_gate, expert_up, expert_down))
    fetched = expert_result.reshape(-1, model_width)[buffer_place].reshape(token_count, TOP, model_width)
    routed = lax.optimization_barrier(jnp.sum(route_weight[..., None] * fetched, 1))
    return hidden + shared_out + routed

def reference(tokens, norm_attn_gain, query_weight, latent_down, latent_gain, latent_up, out_weight, norm_ffn_gain, router_weight, shared_gate, shared_up, shared_down, expert_gate, expert_up, expert_down, expert_ids, out_grad):
    inputs = tuple((argument.astype(jnp.float32) for argument in (tokens, norm_attn_gain, query_weight, latent_down, latent_gain, latent_up, out_weight, norm_ffn_gain, router_weight, shared_gate, shared_up, shared_down, expert_gate, expert_up, expert_down)))
    result, pullback = jax.vjp(partial(block_forward, expert_ids), *inputs)
    grads = pullback(out_grad.astype(jnp.float32))
    return (result.astype(jnp.bfloat16), grads[0].astype(jnp.bfloat16), grads[1], grads[2], grads[3], grads[4], grads[5], grads[6], grads[7], grads[8], grads[9], grads[10], grads[11], grads[12], grads[13], grads[14])
```

```python
import jax
import jax.numpy as jnp
from jax import lax
from jax.experimental import pallas as pl
from jax.experimental.pallas import tpu as pltpu
from jax.sharding import PartitionSpec as P

NOPE = 128
ROPE = 64
VD = 128
R = 512
SEQ_DEVS = 8


eps = 1e-06
route_scale = 2.446
rope_base = 50000.0
masked_score = -1e30
highest = lax.Precision.HIGHEST
BOTH = ("dp", "tensor")


def from_behind(value, axis, steps):
    count = lax.axis_size(axis)
    initial, last = (max(0, -steps), min(count, count - steps))
    return lax.ppermute(value, axis, [(source, source + steps) for source in range(initial, last)])


def mat_dot(left, right):
    return jnp.dot(left, right, preferred_element_type=jnp.float32)


def contract_rows(left, right):
    return lax.dot_general(left, right, (((0,), (0,)), ((), ())), preferred_element_type=jnp.float32)


def contract_cols(left, right):
    return lax.dot_general(left, right, (((1,), (1,)), ((), ())), preferred_element_type=jnp.float32)


def rotation(positions):
    half_width = ROPE // 2
    frequency = rope_base ** (-jnp.arange(half_width, dtype=jnp.float32) / half_width)
    angles = positions.astype(jnp.float32)[:, None] * frequency[None, :]
    return (jnp.cos(angles), jnp.sin(angles))


def rotate(values, cos_table, sin_table):
    half_width = values.shape[-1] // 2
    first_half = values[..., :half_width]
    second_half = values[..., half_width:]
    return jnp.concatenate(
        [
            first_half * cos_table - second_half * sin_table,
            second_half * cos_table + first_half * sin_table,
        ],
        -1,
    )


def unrotate(upstream, cos_table, sin_table):
    return rotate(upstream, cos_table, -sin_table)


def rms_forward(values, gain_vec):
    inv_rms = lax.rsqrt(jnp.mean(values * values, axis=-1, keepdims=True) + eps)
    return (values * inv_rms * gain_vec, inv_rms)


def rms_backward(values, inv_rms, gain_vec, upstream):
    scaled = upstream * gain_vec
    inner_mean = jnp.mean(values * scaled, axis=-1, keepdims=True)
    return (
        inv_rms * scaled - values * inv_rms**3 * inner_mean,
        jnp.sum(upstream * values * inv_rms, axis=0),
    )


def low(value):
    return value.astype(jnp.bfloat16)


def gather(value, axes):
    return lax.all_gather(value, axes, tiled=True)


def scatter(value, axes, dimension=0):
    return lax.psum_scatter(
        low(value), axes, scatter_dimension=dimension, tiled=True
    ).astype(jnp.float32)


MESH = pl.DeviceIdType.MESH
PLANE = 8
DEPTH = 4


class Place:
    def __init__(self):
        self.me = lax.axis_index("dp")
        self.z = lax.axis_index("tensor")
        self.core = self.me % 2
        self.chip = self.me // 2
        self.chip_x = self.chip + 1 - 2 * (self.chip % 2)
        self.chip_y = (self.chip + 2) % 4
        self.chip_xy = 3 - self.chip
        self.sibling = self.me + 1 - 2 * self.core
        self.near_x = 2 * self.chip_x + self.core
        self.near_y = 2 * self.chip_y + self.core
        self.across = 2 * self.chip_xy + self.core
        self.levels = [self.z + 1 - 2 * (self.z % 2), (self.z + 2) % 4, 3 - self.z]


def push(src, dst, sems, index, **target):
    send, recv = sems
    return pltpu.make_async_remote_copy(
        src_ref=src,
        dst_ref=dst,
        send_sem=send.at[index],
        recv_sem=recv.at[index],
        device_id=target,
        device_id_type=MESH,
    )


def add_rows(target, sources):
    rows = target.shape[0]
    step = 16

    def one(k, carry):
        at = pl.ds(pl.multiple_of(k * step, step), step)
        acc = sources[0][at, :].astype(jnp.float32)
        for source in sources[1:]:
            acc = acc + source[at, :].astype(jnp.float32)
        target[at, :] = acc.astype(target.dtype)
        return carry

    lax.fori_loop(0, rows // step, one, 0)


def sem_pair(count):
    return [pltpu.SemaphoreType.DMA((count,)), pltpu.SemaphoreType.DMA((count,))]


class GatherPlane:
    def __init__(self, value, with_z):
        self.with_z = with_z
        self.inputs = [value]
        self.units = DEPTH if with_z else value.shape[0]
        rows, width = value.shape[-2:]
        self.in_specs = [pl.BlockSpec(memory_space=pltpu.VMEM)]
        self.outputs = [
            jax.ShapeDtypeStruct((PLANE, self.units, rows, width), value.dtype)
        ]
        self.out_specs = [pl.BlockSpec(memory_space=pl.ANY)]
        self.scratch = (
            sem_pair(7 * self.units)
            + sem_pair(DEPTH - 1)
            + [pltpu.SemaphoreType.DMA((1,))]
        )

    def steps(self, place, inputs, outputs, scratch):
        (x,), (out,) = inputs, outputs
        sems, z_sems, local = scratch[0:2], scratch[2:4], scratch[4]
        me, units = place.me, self.units
        sends = []
        if self.with_z:
            order = [place.z] + place.levels
            keep = pltpu.make_async_copy(x, out.at[me, place.z], local.at[0])
            arrivals = []
            for k, level in enumerate(place.levels):
                copy = push(x, out.at[me, place.z], z_sems, k, tensor=level)
                copy.start()
                sends.append(copy)
                here = out.at[me, level]
                arrivals.append(push(here, here, z_sems, k, tensor=level))
        else:
            order = list(range(units))
            keep = pltpu.make_async_copy(x, out.at[me], local.at[0])
        keep.start()

        def message(p, kind, slot, target, src=None):
            spot = out.at[slot, order[p]]
            return push(spot if src is None else src, spot, sems, 7 * p + kind, dp=target)

        def launch(*args, **kwargs):
            copy = message(*args, **kwargs)
            copy.start()
            sends.append(copy)

        def stage_own(p):
            if self.with_z:
                src = x if p == 0 else None
                if p > 0:
                    arrivals[p - 1].wait_recv()
            else:
                src = x.at[p]
            pair = [(0, place.near_x), (1, place.near_y)]
            for kind, target in pair if p % 2 == 0 else pair[::-1]:
                launch(p, kind, me, target, src)
            launch(p, 3, me, place.sibling, src)

        def stage_near(p):
            def from_x():
                message(p, 0, place.near_x, place.near_x).wait_recv()
                if p % 2 == 0:
                    launch(p, 2, place.near_x, place.near_y)
                launch(p, 4, place.near_x, place.sibling)

            def from_y():
                message(p, 1, place.near_y, place.near_y).wait_recv()
                if p % 2 == 1:
                    launch(p, 2, place.near_y, place.near_x)
                launch(p, 5, place.near_y, place.sibling)

            for part in (from_x, from_y) if p % 2 == 0 else (from_y, from_x):
                part()

        def stage_across(p):
            message(p, 2, place.across, place.near_x).wait_recv()
            launch(p, 6, place.across, place.sibling)

        for p in range(units + 2):
            if p < units:
                stage_own(p)
            yield
            if 0 <= p - 1 < units:
                stage_near(p - 1)
            if 0 <= p - 2 < units:
                stage_across(p - 2)
            yield
        keep.wait()
        base = place.sibling
        for p in range(units):
            for kind, chip in (
                (3, place.chip),
                (4, place.chip_x),
                (5, place.chip_y),
                (6, place.chip_xy),
            ):
                message(p, kind, 2 * chip + 1 - place.core, base).wait_recv()
        for copy in sends:
            copy.wait_send()


class ScatterPlane:
    def __init__(self, value, with_z, spread=False):
        self.with_z, self.spread = with_z, spread
        _, self.units, rows, width = value.shape
        self.inputs = [value.reshape(4, 2, self.units, rows, width)]
        self.in_specs = [pl.BlockSpec(memory_space=pltpu.VMEM)]
        units = self.units
        shape = (rows, width) if with_z else (units, rows, width)
        kind = jnp.float32
        if spread:
            shape, kind = (DEPTH, rows, width), jnp.bfloat16
        self.outputs = [jax.ShapeDtypeStruct(shape, kind)]
        self.out_specs = [pl.BlockSpec(memory_space=pltpu.VMEM)]
        buffer = pltpu.VMEM((units, rows, width), value.dtype)
        self.scratch = (
            sem_pair(4 * units)
            + [pltpu.VMEM((units, 4, rows, width), value.dtype)]
            + [buffer] * 6
        )
        if with_z:
            level = pltpu.VMEM((DEPTH - 1, rows, width), value.dtype)
            self.scratch += sem_pair(DEPTH - 1) + [level] * 2
        if spread:
            self.scratch += sem_pair(DEPTH - 1) + [pltpu.VMEM((rows, width), value.dtype)]

    def steps(self, place, inputs, outputs, scratch):
        (part,), (out,) = inputs, outputs
        sems, beside = scratch[0:2], scratch[2]
        d_send, d_recv, x_send, x_recv, y_send, y_recv = scratch[3:9]
        units, core = self.units, place.core
        if self.with_z:
            z_sems, z_send, z_recv = scratch[9:11], scratch[11], scratch[12]
            near, far, other = place.levels
            order = [far, other, near, place.z]
        else:
            order = list(range(units))
        sends = []

        def launch(copy):
            copy.start()
            sends.append(copy)

        def across(p):
            target = place.near_x if p % 2 == 0 else place.near_y
            return push(d_send.at[p], d_recv.at[p], sems, 4 * p + 1, dp=target)

        def to_x(p):
            return push(x_send.at[p], x_recv.at[p], sems, 4 * p + 2, dp=place.near_x)

        def to_y(p):
            return push(y_send.at[p], y_recv.at[p], sems, 4 * p + 3, dp=place.near_y)

        def to_sibling(p):
            return push(
                part.at[:, 1 - core, order[p]],
                beside.at[p],
                sems,
                4 * p,
                dp=place.sibling,
            )

        def both(p, chip):
            return [part.at[chip, core, order[p]], beside.at[p, chip]]

        for p in range(units):
            launch(to_sibling(p))

        def stage_one(p):
            to_sibling(p).wait_recv()
            add_rows(d_send.at[p], both(p, place.chip_xy))
            launch(across(p))
            if p % 2 == 0:
                add_rows(x_send.at[p], both(p, place.chip_x))
                launch(to_x(p))
            else:
                add_rows(y_send.at[p], both(p, place.chip_y))
                launch(to_y(p))

        def stage_two(p):
            across(p).wait_recv()
            if p % 2 == 0:
                add_rows(y_send.at[p], both(p, place.chip_y) + [d_recv.at[p]])
                launch(to_y(p))
            else:
                add_rows(x_send.at[p], both(p, place.chip_x) + [d_recv.at[p]])
                launch(to_x(p))

        def to_level(p):
            return push(z_send.at[p], z_recv.at[p], z_sems, p, tensor=order[p])

        def stage_three(p):
            to_x(p).wait_recv()
            to_y(p).wait_recv()
            pieces = both(p, place.chip) + [x_recv.at[p], y_recv.at[p]]
            if not self.with_z:
                add_rows(out.at[p], pieces)
            elif p < units - 1:
                add_rows(z_send.at[p], pieces)
                launch(to_level(p))
            else:
                for k in range(DEPTH - 1):
                    to_level(k).wait_recv()
                pieces += [z_recv.at[k] for k in range(DEPTH - 1)]
                add_rows(scratch[15] if self.spread else out, pieces)

        for p in range(units + 2):
            if p < units:
                stage_one(p)
            yield
            if 0 <= p - 1 < units:
                stage_two(p - 1)
            if 0 <= p - 2 < units:
                stage_three(p - 2)
            yield
        if self.spread:
            yield from spread_levels(place, scratch[15], out, scratch[13:15], sends)
        for copy in sends:
            copy.wait_send()


def spread_levels(place, own, out, z_sems, sends):
    arrivals = []
    for k, level in enumerate(place.levels):
        copy = push(own, out.at[place.z], z_sems, k, tensor=level)
        copy.start()
        sends.append(copy)
        arrivals.append(push(own, out.at[level], z_sems, k, tensor=level))
    out[place.z] = own[...]
    yield
    for copy in arrivals:
        copy.wait_recv()


class GatherLevels:
    def __init__(self, value):
        self.inputs = [value]
        self.in_specs = [pl.BlockSpec(memory_space=pltpu.VMEM)]
        self.outputs = [jax.ShapeDtypeStruct((DEPTH,) + value.shape, value.dtype)]
        self.out_specs = [pl.BlockSpec(memory_space=pltpu.VMEM)]
        self.scratch = sem_pair(DEPTH - 1)

    def steps(self, place, inputs, outputs, scratch):
        sends = []
        yield from spread_levels(place, inputs[0], outputs[0], scratch[0:2], sends)
        for copy in sends:
            copy.wait_send()


class ScatterLevels:
    def __init__(self, value):
        _, rows, width = value.shape
        self.inputs = [value]
        self.in_specs = [pl.BlockSpec(memory_space=pltpu.VMEM)]
        self.outputs = [jax.ShapeDtypeStruct((rows, width), jnp.float32)]
        self.out_specs = [pl.BlockSpec(memory_space=pltpu.VMEM)]
        self.scratch = sem_pair(DEPTH - 1) + [pltpu.VMEM((DEPTH - 1, rows, width), value.dtype)]

    def steps(self, place, inputs, outputs, scratch):
        part, z_sems, landed = inputs[0], scratch[0:2], scratch[2]
        copies = [
            push(part.at[level], landed.at[k], z_sems, k, tensor=level)
            for k, level in enumerate(place.levels)
        ]
        for copy in copies:
            copy.start()
        yield
        yield
        yield
        for copy in copies:
            copy.wait_recv()
        add_rows(outputs[0], [part.at[place.z]] + [landed.at[k] for k in range(DEPTH - 1)])
        for copy in copies:
            copy.wait_send()


def exchange(tasks, collective_id, name):
    def kernel(*refs):
        place = Place()
        barrier = pltpu.get_barrier_semaphore()
        for target in (place.sibling, place.near_x, place.near_y):
            pl.semaphore_signal(
                barrier, inc=1, device_id={"dp": target}, device_id_type=MESH
            )
        for target in place.levels:
            pl.semaphore_signal(
                barrier, inc=1, device_id={"tensor": target}, device_id_type=MESH
            )
        pl.semaphore_wait(barrier, 6)
        refs = list(refs)

        def take(counts):
            return [[refs.pop(0) for _ in range(count)] for count in counts]

        inputs = take([len(task.inputs) for task in tasks])
        outputs = take([len(task.outputs) for task in tasks])
        scratch = take([len(task.scratch) for task in tasks])
        running = [
            task.steps(place, a, b, c)
            for task, a, b, c in zip(tasks, inputs, outputs, scratch)
        ]
        while running:
            for walk in list(running):
                if next(walk, running) is running:
                    running.remove(walk)

    def flat(pieces):
        return [one for piece in pieces for one in piece]

    moved = sum(one.size * one.dtype.itemsize for task in tasks for one in task.inputs)
    return pl.pallas_call(
        kernel,
        name=name,
        out_shape=flat(task.outputs for task in tasks),
        in_specs=flat(task.in_specs for task in tasks),
        out_specs=flat(task.out_specs for task in tasks),
        scratch_shapes=flat(task.scratch for task in tasks),
        compiler_params=pltpu.CompilerParams(
            collective_id=collective_id, has_side_effects=True, vmem_limit_bytes=56 << 20
        ),
        cost_estimate=pl.CostEstimate(flops=0, bytes_accessed=4 * moved, transcendentals=0),
    )(*flat(task.inputs for task in tasks))


def shards(
    tokens,
    norm_attn_gain,
    query_weight,
    latent_down,
    latent_gain,
    latent_up,
    out_weight,
    norm_ffn_gain,
    router_weight,
    shared_gate,
    shared_up,
    shared_down,
    expert_gate,
    expert_up,
    expert_down,
    expert_ids,
    out_grad,
):
    tok_rows, model_width = tokens.shape
    head_count = out_weight.shape[0] // VD
    groups = lax.axis_size("dp")
    parts = lax.axis_size("tensor")
    my_group = lax.axis_index("dp")
    my_part = lax.axis_index("tensor")
    stride = groups // SEQ_DEVS
    local_experts, _, units = expert_gate.shape
    experts = local_experts * groups
    rows = tok_rows // parts
    shared_units = shared_gate.shape[1] // groups
    used_units = local_experts * units + shared_units
    spare_units = -used_units % 128
    seq_stretch = my_group // stride
    direct = groups == PLANE and parts == DEPTH

    grad_all = gather(out_grad, "dp")

    residual_in = tokens.astype(jnp.float32)
    normed_in, inv_one = rms_forward(residual_in, norm_attn_gain)
    normed_low = low(normed_in)
    query_pos = seq_stretch * tok_rows + jnp.arange(tok_rows)
    cos_table, sin_table = rotation(query_pos)
    factor = (NOPE + ROPE) ** (-0.5)
    compressed = mat_dot(normed_low, latent_down)
    latent_normed, inv_latent = rms_forward(compressed[:, :R], latent_gain)
    key_rope = rotate(compressed[:, R:], cos_table, sin_table)
    own_latent = low(jnp.concatenate([latent_normed, key_rope], -1))
    if direct:
        halves = own_latent.reshape(2, tok_rows // 2, R + ROPE)
        (keys_latent,) = exchange([GatherPlane(halves, False)], 0, "gather_keys")
        keys_latent = keys_latent.reshape(groups * tok_rows, R + ROPE)
        key_pos = jnp.arange(keys_latent.shape[0])
    elif stride == 1:
        keys_latent = gather(own_latent, "dp")
        key_pos = jnp.arange(keys_latent.shape[0])
    else:
        earlier = [
            from_behind(own_latent, "dp", (SEQ_DEVS - 1 - block_index) * stride)
            for block_index in range(SEQ_DEVS - 1)
        ]
        keys_latent = jnp.concatenate(earlier + [own_latent], 0)
        key_pos = (seq_stretch - (SEQ_DEVS - 1)) * tok_rows + jnp.arange(keys_latent.shape[0])
    key_count = keys_latent.shape[0]
    query = mat_dot(normed_low, query_weight).reshape(tok_rows, head_count, NOPE + ROPE)
    query = (
        jnp.concatenate(
            [
                query[..., :NOPE],
                rotate(query[..., NOPE:], cos_table[:, None, :], sin_table[:, None, :]),
            ],
            -1,
        )
        * factor
    )
    query_low = low(query)
    expanded = low(mat_dot(keys_latent[:, :R], latent_up)).reshape(
        key_count, head_count, NOPE + VD
    )
    visible = (key_pos[None, :] >= 0) & (key_pos[None, :] <= query_pos[:, None])

    def attention_scores():
        raw_scores = jnp.einsum(
            "qhd,khd->hqk",
            query_low[..., :NOPE],
            expanded[..., :NOPE],
            preferred_element_type=jnp.float32,
        )
        raw_scores = raw_scores + jnp.einsum(
            "qhd,kd->hqk",
            query_low[..., NOPE:],
            keys_latent[:, R:],
            preferred_element_type=jnp.float32,
        )
        return jnp.where(visible[None], raw_scores, masked_score)

    scores = attention_scores()
    top_score = jnp.max(scores, -1, keepdims=True)
    exp_scores = jnp.exp(scores - top_score)
    exp_total = jnp.sum(exp_scores, -1, keepdims=True)
    log_total = top_score + jnp.log(exp_total)
    probs_low = low(exp_scores / exp_total)
    heads_out = jnp.einsum(
        "hqk,khd->qhd", probs_low, expanded[..., NOPE:], preferred_element_type=jnp.float32
    )
    heads_low = low(heads_out.reshape(tok_rows, head_count * VD))
    attn = mat_dot(heads_low, out_weight)
    if direct:
        (attn,) = exchange(
            [ScatterLevels(low(attn).reshape(parts, rows, model_width))], 1, "scatter_attn"
        )
    else:
        attn = scatter(attn, "tensor")

    def own_rows(value):
        return lax.dynamic_slice_in_dim(value, my_part * rows, rows, 0)

    hidden = own_rows(residual_in) + attn
    ffn_in, inv_two = rms_forward(hidden, norm_ffn_gain)
    ffn_low = low(ffn_in)
    router = router_weight.astype(jnp.float32)
    router_gates = jax.nn.sigmoid(
        jnp.dot(ffn_in, router, precision=highest, preferred_element_type=jnp.float32)
    )
    picked = jnp.any(
        own_rows(expert_ids)[..., None] == jnp.arange(experts)[None, None, :], 1
    ).astype(jnp.float32)
    chosen = picked * router_gates
    chosen_sum = jnp.sum(chosen, -1, keepdims=True)
    route = route_scale * chosen / chosen_sum
    route_high = low(route)
    route_rest = low(route - route_high.astype(jnp.float32))
    routes = jnp.concatenate([route_high, route_rest], 1)
    if direct:
        routes = jnp.pad(routes, ((0, 0), (0, 128 - 2 * experts)))
        ffn_all, routes = exchange(
            [GatherPlane(ffn_low, True), GatherPlane(routes, True)], 2, "gather_ffn"
        )
        ffn_all = ffn_all.reshape(-1, model_width)
        routes = routes.reshape(-1, 128)
    else:
        ffn_all = gather(jnp.concatenate([ffn_low, routes], 1), BOTH)
        routes = ffn_all[:, model_width:]
        ffn_all = ffn_all[:, :model_width]
    route_all = routes[:, :experts].astype(jnp.float32) + routes[
        :, experts : 2 * experts
    ].astype(jnp.float32)
    token_count = ffn_all.shape[0]
    route_own = lax.dynamic_slice_in_dim(route_all, my_group * local_experts, local_experts, 1)

    def joined(expert_weight, shared_weight):
        own = lax.dynamic_slice_in_dim(shared_weight, my_group * shared_units, shared_units, 1)
        pieces = [expert_weight[e] for e in range(local_experts)]
        return jnp.concatenate(
            pieces + [own, jnp.zeros((model_width, spare_units), jnp.bfloat16)], 1
        )

    gate_weight = joined(expert_gate, shared_gate)
    up_weight = joined(expert_up, shared_up)
    down_weight = jnp.concatenate(
        [expert_down[e] for e in range(local_experts)]
        + [
            lax.dynamic_slice_in_dim(shared_down, my_group * shared_units, shared_units, 0),
            jnp.zeros((spare_units, model_width), jnp.bfloat16),
        ],
        0,
    )
    scale = jnp.concatenate(
        [
            jnp.broadcast_to(route_own[:, e : e + 1], (token_count, units))
            for e in range(local_experts)
        ]
        + [jnp.ones((token_count, shared_units + spare_units), jnp.float32)],
        1,
    )
    plain_grad = contract_cols(grad_all, down_weight)
    gate_act = mat_dot(ffn_all, gate_weight)
    up_act = mat_dot(ffn_all, up_weight)
    logistic = jax.nn.sigmoid(gate_act)
    silu = gate_act * logistic
    act = silu * up_act
    act_low = low(act * scale)
    act_grad = plain_grad * scale
    gate_grad = low(act_grad * up_act * logistic * (1.0 + gate_act * (1.0 - logistic)))
    up_grad = low(act_grad * silu)
    weight_dots = act * plain_grad
    weight_grad = jnp.stack(
        [
            jnp.sum(weight_dots[:, e * units : (e + 1) * units], 1)
            for e in range(local_experts)
        ],
        1,
    )
    weight_grad = lax.dynamic_update_slice_in_dim(
        jnp.zeros((token_count, experts), jnp.bfloat16),
        low(weight_grad),
        my_group * local_experts,
        1,
    )
    ffn_grad = contract_cols(gate_grad, gate_weight) + contract_cols(up_grad, up_weight)
    if direct:
        weight_grad = jnp.pad(weight_grad, ((0, 0), (0, 128 - experts)))
        ffn_grad, weight_grad = exchange(
            [
                ScatterPlane(low(ffn_grad).reshape(groups, parts, rows, model_width), True),
                ScatterPlane(weight_grad.reshape(groups, parts, rows, 128), True),
            ],
            3,
            "scatter_ffn",
        )
        weight_grad = weight_grad[:, :experts]
    else:
        ffn_grad = scatter(jnp.concatenate([low(ffn_grad), weight_grad], 1), BOTH)
        weight_grad = ffn_grad[:, model_width:]
        ffn_grad = ffn_grad[:, :model_width]
    moe_out = scatter(scatter(mat_dot(act_low, down_weight), "dp"), "tensor")
    block_out = gather(low(hidden + moe_out), "tensor")

    down_grad = contract_rows(act_low, grad_all)
    gate_weight_grad = contract_rows(ffn_all, gate_grad)
    up_weight_grad = contract_rows(ffn_all, up_grad)
    expert_down_grad = down_grad[: local_experts * units].reshape(local_experts, units, -1)
    expert_gate_grad = jnp.stack(
        [gate_weight_grad[:, e * units : (e + 1) * units] for e in range(local_experts)]
    )
    expert_up_grad = jnp.stack(
        [up_weight_grad[:, e * units : (e + 1) * units] for e in range(local_experts)]
    )

    def swap(value):
        return lax.all_to_all(low(value), "dp", split_axis=0, concat_axis=1, tiled=True).astype(
            jnp.float32
        )

    first = local_experts * units
    shared_gate_grad = swap(gate_weight_grad[:, first:used_units])
    shared_up_grad = swap(up_weight_grad[:, first:used_units])
    shared_down_grad = lax.all_to_all(
        low(down_grad[first:used_units]), "dp", split_axis=1, concat_axis=0, tiled=True
    ).astype(jnp.float32)

    inner_sum = jnp.sum(weight_grad * chosen, -1, keepdims=True)
    chosen_grad = route_scale * (weight_grad / chosen_sum - inner_sum / (chosen_sum * chosen_sum))
    logit_grad = chosen_grad * chosen * (1.0 - chosen)
    router_grad = jnp.dot(
        ffn_in.T, logit_grad, precision=highest, preferred_element_type=jnp.float32
    )
    norm_grad = ffn_grad + jnp.dot(
        logit_grad, router.T, precision=highest, preferred_element_type=jnp.float32
    )
    hidden_extra, norm_ffn_grad = rms_backward(hidden, inv_two, norm_ffn_gain, norm_grad)
    hidden_grad = own_rows(out_grad).astype(jnp.float32) + hidden_extra
    if direct:
        (attn_grad_low,) = exchange([GatherLevels(low(hidden_grad))], 4, "gather_hidden")
        attn_grad_low = attn_grad_low.reshape(tok_rows, model_width)
    else:
        attn_grad_low = gather(low(hidden_grad), "tensor")

    out_weight_grad = scatter(contract_rows(heads_low, attn_grad_low), "dp", 1)
    heads_grad = low(contract_cols(attn_grad_low, out_weight)).reshape(tok_rows, head_count, VD)
    attn_probs = jnp.exp(attention_scores() - log_total)
    probs_low = low(attn_probs)
    value_grad = jnp.einsum(
        "hqk,qhd->khd", probs_low, heads_grad, preferred_element_type=jnp.float32
    )
    prob_grad = jnp.einsum(
        "qhd,khd->hqk", heads_grad, expanded[..., NOPE:], preferred_element_type=jnp.float32
    )
    row_delta = jnp.sum(attn_probs * prob_grad, -1, keepdims=True)
    score_grad = low(attn_probs * (prob_grad - row_delta))
    nope_grad = jnp.einsum(
        "hqk,khd->qhd", score_grad, expanded[..., :NOPE], preferred_element_type=jnp.float32
    )
    rope_grad = jnp.einsum(
        "hqk,kd->qhd", score_grad, keys_latent[:, R:], preferred_element_type=jnp.float32
    )
    key_nope_grad = jnp.einsum(
        "hqk,qhd->khd", score_grad, query_low[..., :NOPE], preferred_element_type=jnp.float32
    )
    key_rope_grad = jnp.einsum(
        "hqk,qhd->kd", score_grad, query_low[..., NOPE:], preferred_element_type=jnp.float32
    )
    expand_grad = low(
        jnp.concatenate([key_nope_grad, value_grad], -1).reshape(
            key_count, head_count * (NOPE + VD)
        )
    )
    latent_up_grad = contract_rows(keys_latent[:, :R], expand_grad)
    latent_grad = jnp.concatenate([contract_cols(expand_grad, latent_up), key_rope_grad], -1)
    query_grad = (
        jnp.concatenate(
            [nope_grad, unrotate(rope_grad, cos_table[:, None, :], sin_table[:, None, :])], -1
        )
        * factor
    )
    query_grad_low = low(query_grad.reshape(tok_rows, head_count * (NOPE + ROPE)))
    query_weight_grad = contract_rows(normed_low, query_grad_low)
    input_part = contract_cols(query_grad_low, query_weight)
    if direct:
        own_grad, input_sum, query_weight_grad, latent_up_grad = exchange(
            [
                ScatterPlane(low(latent_grad).reshape(groups, parts, rows, R + ROPE), True),
                ScatterLevels(low(input_part).reshape(parts, rows, model_width)),
                ScatterPlane(low(query_weight_grad).reshape(groups, 2, model_width // 16, -1), False),
                ScatterPlane(low(latent_up_grad).reshape(groups, 2, R // 16, -1), False),
            ],
            5,
            "scatter_latent",
        )
        query_weight_grad = query_weight_grad.reshape(model_width // groups, -1)
        latent_up_grad = latent_up_grad.reshape(R // groups, -1)
    else:
        if stride == 1:
            own_grad = scatter(scatter(latent_grad, "dp"), "tensor")
        else:
            own_grad = latent_grad[(SEQ_DEVS - 1) * tok_rows :]
            for block_index in range(SEQ_DEVS - 1):
                piece_grad = latent_grad[block_index * tok_rows : (block_index + 1) * tok_rows]
                own_grad = own_grad + from_behind(
                    low(piece_grad), "dp", -(SEQ_DEVS - 1 - block_index) * stride
                ).astype(piece_grad.dtype)
            own_grad = scatter(own_grad, "tensor")
        input_sum = scatter(input_part, "tensor")
        query_weight_grad = scatter(query_weight_grad, "dp")
        latent_up_grad = scatter(latent_up_grad, "dp")
    compressed_own = own_rows(compressed)
    normed_part, latent_gain_grad = rms_backward(
        compressed_own[:, :R], own_rows(inv_latent), latent_gain, own_grad[:, :R]
    )
    compressed_grad = low(
        jnp.concatenate(
            [normed_part, unrotate(own_grad[:, R:], own_rows(cos_table), own_rows(sin_table))], -1
        )
    )
    latent_down_grad = contract_rows(own_rows(normed_low), compressed_grad)
    normed_grad = input_sum + contract_cols(compressed_grad, latent_down)
    input_extra, norm_attn_grad = rms_backward(
        own_rows(residual_in), own_rows(inv_one), norm_attn_gain, normed_grad
    )
    tokens_grad = low(hidden_grad + input_extra)
    small = [norm_attn_grad, latent_gain_grad, norm_ffn_grad, router_grad]
    sizes = [one.size // groups for one in small]
    small = jnp.concatenate([one.reshape(groups, -1) for one in small], 1)
    if direct:
        small = jnp.pad(low(small), ((0, 0), (0, parts * 2048 - small.shape[1])))
        latent_down_grad, small, tokens_grad = exchange(
            [
                ScatterPlane(
                    low(latent_down_grad).reshape(groups, parts, rows, R + ROPE), True, True
                ),
                ScatterPlane(small.reshape(groups, parts, 16, 128), True, True),
                GatherLevels(tokens_grad),
            ],
            6,
            "scatter_last",
        )
        latent_down_grad = latent_down_grad.reshape(-1, R + ROPE).astype(jnp.float32)
        small = small.reshape(-1).astype(jnp.float32)
        tokens_grad = tokens_grad.reshape(tok_rows, model_width)
    else:
        latent_down_grad = lax.psum(scatter(latent_down_grad, "dp"), "tensor")
        small = lax.psum(scatter(small, "dp"), "tensor").reshape(-1)
        tokens_grad = gather(tokens_grad, "tensor")
    offsets = [sum(sizes[:k]) for k in range(len(sizes))]
    norm_attn_grad, latent_gain_grad, norm_ffn_grad, router_grad = [
        small[start : start + size] for start, size in zip(offsets, sizes)
    ]

    return (
        block_out,
        tokens_grad,
        norm_attn_grad,
        query_weight_grad,
        latent_down_grad,
        latent_gain_grad,
        latent_up_grad,
        out_weight_grad,
        norm_ffn_grad,
        router_grad.reshape(-1, experts),
        shared_gate_grad,
        shared_up_grad,
        shared_down_grad,
        expert_gate_grad,
        expert_up_grad,
        expert_down_grad,
    )


def solution(mesh):
    in_specs = (
        P("dp", None),
        P(),
        P(None, "tensor"),
        P(),
        P(),
        P(None, "tensor"),
        P("tensor", None),
        P(),
        P(),
        P(None, "tensor"),
        P(None, "tensor"),
        P("tensor", None),
        P("dp", None, "tensor"),
        P("dp", None, "tensor"),
        P("dp", "tensor", None),
        P("dp", None),
        P("dp", None),
    )
    out_specs = (
        P("dp", None),
        P("dp", None),
        P("dp"),
        P("dp", "tensor"),
        P("dp", None),
        P("dp"),
        P("dp", "tensor"),
        P("tensor", "dp"),
        P("dp"),
        P("dp", None),
        P("dp", "tensor"),
        P("dp", "tensor"),
        P("tensor", "dp"),
        P("dp", None, "tensor"),
        P("dp", None, "tensor"),
        P("dp", "tensor", None),
    )
    return jax.shard_map(shards, mesh=mesh, in_specs=in_specs, out_specs=out_specs, check_vma=False)
```

```python
import functools

import jax
import jax.numpy as jnp
from jax import lax
from jax.experimental import pallas as pl
from jax.experimental.pallas import tpu as pltpu
from jax.sharding import PartitionSpec as P

NOPE = 128
ROPE = 64
VD = 128
R = 512
SEQ_DEVS = 8


eps = 1e-06
route_scale = 2.446
rope_base = 50000.0
masked_score = -1e30
highest = lax.Precision.HIGHEST
BOTH = ("dp", "tensor")


def from_behind(value, axis, steps):
    count = lax.axis_size(axis)
    initial, last = (max(0, -steps), min(count, count - steps))
    return lax.ppermute(value, axis, [(source, source + steps) for source in range(initial, last)])


def mat_dot(left, right):
    return jnp.dot(left, right, preferred_element_type=jnp.float32)


def contract_rows(left, right):
    return lax.dot_general(left, right, (((0,), (0,)), ((), ())), preferred_element_type=jnp.float32)


def contract_cols(left, right):
    return lax.dot_general(left, right, (((1,), (1,)), ((), ())), preferred_element_type=jnp.float32)


def rotation(positions):
    half_width = ROPE // 2
    frequency = rope_base ** (-jnp.arange(half_width, dtype=jnp.float32) / half_width)
    angles = positions.astype(jnp.float32)[:, None] * frequency[None, :]
    return (jnp.cos(angles), jnp.sin(angles))


def rotate(values, cos_table, sin_table):
    half_width = values.shape[-1] // 2
    first_half = values[..., :half_width]
    second_half = values[..., half_width:]
    return jnp.concatenate(
        [
            first_half * cos_table - second_half * sin_table,
            second_half * cos_table + first_half * sin_table,
        ],
        -1,
    )


def unrotate(upstream, cos_table, sin_table):
    return rotate(upstream, cos_table, -sin_table)


def rms_forward(values, gain_vec):
    inv_rms = lax.rsqrt(jnp.mean(values * values, axis=-1, keepdims=True) + eps)
    return (values * inv_rms * gain_vec, inv_rms)


def rms_backward(values, inv_rms, gain_vec, upstream):
    scaled = upstream * gain_vec
    inner_mean = jnp.mean(values * scaled, axis=-1, keepdims=True)
    return (
        inv_rms * scaled - values * inv_rms**3 * inner_mean,
        jnp.sum(upstream * values * inv_rms, axis=0),
    )


def low(value):
    return value.astype(jnp.bfloat16)


def gather(value, axes):
    return lax.all_gather(value, axes, tiled=True)


def scatter(value, axes, dimension=0):
    return lax.psum_scatter(
        low(value), axes, scatter_dimension=dimension, tiled=True
    ).astype(jnp.float32)


MESH = pl.DeviceIdType.MESH
PLANE = 8
DEPTH = 4


class Place:
    def __init__(self):
        self.me = lax.axis_index("dp")
        self.z = lax.axis_index("tensor")
        self.core = self.me % 2
        self.chip = self.me // 2
        self.chip_x = self.chip + 1 - 2 * (self.chip % 2)
        self.chip_y = (self.chip + 2) % 4
        self.chip_xy = 3 - self.chip
        self.sibling = self.me + 1 - 2 * self.core
        self.near_x = 2 * self.chip_x + self.core
        self.near_y = 2 * self.chip_y + self.core
        self.across = 2 * self.chip_xy + self.core
        self.levels = [self.z + 1 - 2 * (self.z % 2), (self.z + 2) % 4, 3 - self.z]


def push(src, dst, sems, index, **target):
    send, recv = sems
    return pltpu.make_async_remote_copy(
        src_ref=src,
        dst_ref=dst,
        send_sem=send.at[index],
        recv_sem=recv.at[index],
        device_id=target,
        device_id_type=MESH,
    )


def add_rows(target, sources):
    rows = target.shape[0]
    step = 16

    def one(k, carry):
        at = pl.ds(pl.multiple_of(k * step, step), step)
        acc = sources[0][at, :].astype(jnp.float32)
        for source in sources[1:]:
            acc = acc + source[at, :].astype(jnp.float32)
        target[at, :] = acc.astype(target.dtype)
        return carry

    lax.fori_loop(0, rows // step, one, 0)


def sem_pair(count):
    return [pltpu.SemaphoreType.DMA((count,)), pltpu.SemaphoreType.DMA((count,))]


class GatherPlane:
    def __init__(self, value, with_z):
        self.with_z = with_z
        self.inputs = [value]
        self.units = DEPTH if with_z else value.shape[0]
        rows, width = value.shape[-2:]
        self.in_specs = [pl.BlockSpec(memory_space=pltpu.VMEM)]
        self.outputs = [
            jax.ShapeDtypeStruct((PLANE, self.units, rows, width), value.dtype)
        ]
        self.out_specs = [pl.BlockSpec(memory_space=pl.ANY)]
        self.scratch = (
            sem_pair(7 * self.units)
            + sem_pair(DEPTH - 1)
            + [pltpu.SemaphoreType.DMA((1,))]
        )

    def steps(self, place, inputs, outputs, scratch):
        (x,), (out,) = inputs, outputs
        sems, z_sems, local = scratch[0:2], scratch[2:4], scratch[4]
        me, units = place.me, self.units
        sends = []
        if self.with_z:
            order = [place.z] + place.levels
            keep = pltpu.make_async_copy(x, out.at[me, place.z], local.at[0])
            arrivals = []
            for k, level in enumerate(place.levels):
                copy = push(x, out.at[me, place.z], z_sems, k, tensor=level)
                copy.start()
                sends.append(copy)
                here = out.at[me, level]
                arrivals.append(push(here, here, z_sems, k, tensor=level))
        else:
            order = list(range(units))
            keep = pltpu.make_async_copy(x, out.at[me], local.at[0])
        keep.start()

        def message(p, kind, slot, target, src=None):
            spot = out.at[slot, order[p]]
            return push(spot if src is None else src, spot, sems, 7 * p + kind, dp=target)

        def launch(*args, **kwargs):
            copy = message(*args, **kwargs)
            copy.start()
            sends.append(copy)

        def stage_own(p):
            if self.with_z:
                src = x if p == 0 else None
                if p > 0:
                    arrivals[p - 1].wait_recv()
            else:
                src = x.at[p]
            pair = [(0, place.near_x), (1, place.near_y)]
            for kind, target in pair if p % 2 == 0 else pair[::-1]:
                launch(p, kind, me, target, src)
            launch(p, 3, me, place.sibling, src)

        def stage_near(p):
            def from_x():
                message(p, 0, place.near_x, place.near_x).wait_recv()
                if p % 2 == 0:
                    launch(p, 2, place.near_x, place.near_y)
                launch(p, 4, place.near_x, place.sibling)

            def from_y():
                message(p, 1, place.near_y, place.near_y).wait_recv()
                if p % 2 == 1:
                    launch(p, 2, place.near_y, place.near_x)
                launch(p, 5, place.near_y, place.sibling)

            for part in (from_x, from_y) if p % 2 == 0 else (from_y, from_x):
                part()

        def stage_across(p):
            message(p, 2, place.across, place.near_x).wait_recv()
            launch(p, 6, place.across, place.sibling)

        for p in range(units + 2):
            if p < units:
                stage_own(p)
            yield
            if 0 <= p - 1 < units:
                stage_near(p - 1)
            if 0 <= p - 2 < units:
                stage_across(p - 2)
            yield
        keep.wait()
        base = place.sibling
        for p in range(units):
            for kind, chip in (
                (3, place.chip),
                (4, place.chip_x),
                (5, place.chip_y),
                (6, place.chip_xy),
            ):
                message(p, kind, 2 * chip + 1 - place.core, base).wait_recv()
        for copy in sends:
            copy.wait_send()


class ScatterPlane:
    def __init__(self, value, with_z, spread=False):
        self.with_z, self.spread = with_z, spread
        _, self.units, rows, width = value.shape
        self.inputs = [value.reshape(4, 2, self.units, rows, width)]
        self.in_specs = [pl.BlockSpec(memory_space=pltpu.VMEM)]
        units = self.units
        shape = (rows, width) if with_z else (units, rows, width)
        kind = jnp.float32
        if spread:
            shape, kind = (DEPTH, rows, width), jnp.bfloat16
        self.outputs = [jax.ShapeDtypeStruct(shape, kind)]
        self.out_specs = [pl.BlockSpec(memory_space=pltpu.VMEM)]
        buffer = pltpu.VMEM((units, rows, width), value.dtype)
        self.scratch = (
            sem_pair(4 * units)
            + [pltpu.VMEM((units, 4, rows, width), value.dtype)]
            + [buffer] * 6
        )
        if with_z:
            level = pltpu.VMEM((DEPTH - 1, rows, width), value.dtype)
            self.scratch += sem_pair(DEPTH - 1) + [level] * 2
        if spread:
            self.scratch += sem_pair(DEPTH - 1) + [pltpu.VMEM((rows, width), value.dtype)]

    def steps(self, place, inputs, outputs, scratch):
        (part,), (out,) = inputs, outputs
        sems, beside = scratch[0:2], scratch[2]
        d_send, d_recv, x_send, x_recv, y_send, y_recv = scratch[3:9]
        units, core = self.units, place.core
        other_core = 1 - core
        if self.with_z:
            z_sems, z_send, z_recv = scratch[9:11], scratch[11], scratch[12]
            near, far, other = place.levels
            order = [far, other, near, place.z]
        else:
            order = list(range(units))
        sends = []

        def launch(make, p):
            make(p).start()
            sends.append((make, p))

        def across(p):
            target = place.near_x if p % 2 == 0 else place.near_y
            return push(d_send.at[p], d_recv.at[p], sems, 4 * p + 1, dp=target)

        def to_x(p):
            return push(x_send.at[p], x_recv.at[p], sems, 4 * p + 2, dp=place.near_x)

        def to_y(p):
            return push(y_send.at[p], y_recv.at[p], sems, 4 * p + 3, dp=place.near_y)

        def to_sibling(p):
            return push(
                part.at[:, other_core, order[p]],
                beside.at[p],
                sems,
                4 * p,
                dp=place.sibling,
            )

        def both(p, chip):
            return [part.at[chip, core, order[p]], beside.at[p, chip]]

        def stage_one(p):
            to_sibling(p).wait_recv()
            add_rows(d_send.at[p], both(p, place.chip_xy))
            launch(across, p)
            if p % 2 == 0:
                add_rows(x_send.at[p], both(p, place.chip_x))
                launch(to_x, p)
            else:
                add_rows(y_send.at[p], both(p, place.chip_y))
                launch(to_y, p)

        def stage_two(p):
            across(p).wait_recv()
            if p % 2 == 0:
                add_rows(y_send.at[p], both(p, place.chip_y) + [d_recv.at[p]])
                launch(to_y, p)
            else:
                add_rows(x_send.at[p], both(p, place.chip_x) + [d_recv.at[p]])
                launch(to_x, p)

        def to_level(p):
            return push(z_send.at[p], z_recv.at[p], z_sems, p, tensor=order[p])

        def stage_three(p):
            to_x(p).wait_recv()
            to_y(p).wait_recv()
            pieces = both(p, place.chip) + [x_recv.at[p], y_recv.at[p]]
            if not self.with_z:
                add_rows(out.at[p], pieces)
            elif p < units - 1:
                add_rows(z_send.at[p], pieces)
                launch(to_level, p)
            else:
                for k in range(DEPTH - 1):
                    to_level(k).wait_recv()
                pieces += [z_recv.at[k] for k in range(DEPTH - 1)]
                add_rows(scratch[15] if self.spread else out, pieces)

        yield
        for p in range(units):
            launch(to_sibling, p)
        yield
        for p in range(units + 2):
            if p < units:
                stage_one(p)
            yield
            if 0 <= p - 1 < units:
                stage_two(p - 1)
            if 0 <= p - 2 < units:
                stage_three(p - 2)
            if p < units + 1:
                yield
        if self.spread:
            copies = []
            yield from spread_levels(place, scratch[15], out, scratch[13:15], copies)
            for copy in copies:
                copy.wait_send()
        for make, p in sends:
            make(p).wait_send()


def spread_levels(place, own, out, z_sems, sends):
    arrivals = []
    for k, level in enumerate(place.levels):
        copy = push(own, out.at[place.z], z_sems, k, tensor=level)
        copy.start()
        sends.append(copy)
        arrivals.append(push(own, out.at[level], z_sems, k, tensor=level))
    out[place.z] = own[...]
    yield
    for copy in arrivals:
        copy.wait_recv()


class GatherLevels:
    def __init__(self, value):
        self.inputs = [value]
        self.in_specs = [pl.BlockSpec(memory_space=pltpu.VMEM)]
        self.outputs = [jax.ShapeDtypeStruct((DEPTH,) + value.shape, value.dtype)]
        self.out_specs = [pl.BlockSpec(memory_space=pltpu.VMEM)]
        self.scratch = sem_pair(DEPTH - 1)

    def steps(self, place, inputs, outputs, scratch):
        sends = []
        yield from spread_levels(place, inputs[0], outputs[0], scratch[0:2], sends)
        for copy in sends:
            copy.wait_send()


class ScatterLevels:
    def __init__(self, value):
        _, rows, width = value.shape
        self.inputs = [value]
        self.in_specs = [pl.BlockSpec(memory_space=pltpu.VMEM)]
        self.outputs = [jax.ShapeDtypeStruct((rows, width), jnp.float32)]
        self.out_specs = [pl.BlockSpec(memory_space=pltpu.VMEM)]
        self.scratch = sem_pair(DEPTH - 1) + [pltpu.VMEM((DEPTH - 1, rows, width), value.dtype)]

    def steps(self, place, inputs, outputs, scratch):
        part, z_sems, landed = inputs[0], scratch[0:2], scratch[2]
        copies = [
            push(part.at[level], landed.at[k], z_sems, k, tensor=level)
            for k, level in enumerate(place.levels)
        ]
        for copy in copies:
            copy.start()
        yield
        yield
        yield
        for copy in copies:
            copy.wait_recv()
        add_rows(outputs[0], [part.at[place.z]] + [landed.at[k] for k in range(DEPTH - 1)])
        for copy in copies:
            copy.wait_send()


def greet(place):
    barrier = pltpu.get_barrier_semaphore()
    for target in (place.sibling, place.near_x, place.near_y):
        pl.semaphore_signal(barrier, inc=1, device_id={"dp": target}, device_id_type=MESH)
    for target in place.levels:
        pl.semaphore_signal(barrier, inc=1, device_id={"tensor": target}, device_id_type=MESH)
    pl.semaphore_wait(barrier, 6)


def exchange(tasks, collective_id, name):
    def kernel(*refs):
        place = Place()
        greet(place)
        refs = list(refs)

        def take(counts):
            return [[refs.pop(0) for _ in range(count)] for count in counts]

        inputs = take([len(task.inputs) for task in tasks])
        outputs = take([len(task.outputs) for task in tasks])
        scratch = take([len(task.scratch) for task in tasks])
        running = [
            task.steps(place, a, b, c)
            for task, a, b, c in zip(tasks, inputs, outputs, scratch)
        ]
        while running:
            for walk in list(running):
                if next(walk, running) is running:
                    running.remove(walk)

    def flat(pieces):
        return [one for piece in pieces for one in piece]

    moved = sum(one.size * one.dtype.itemsize for task in tasks for one in task.inputs)
    return pl.pallas_call(
        kernel,
        name=name,
        out_shape=flat(task.outputs for task in tasks),
        in_specs=flat(task.in_specs for task in tasks),
        out_specs=flat(task.out_specs for task in tasks),
        scratch_shapes=flat(task.scratch for task in tasks),
        compiler_params=pltpu.CompilerParams(
            collective_id=collective_id, has_side_effects=True, vmem_limit_bytes=56 << 20
        ),
        cost_estimate=pl.CostEstimate(flops=0, bytes_accessed=4 * moved, transcendentals=0),
    )(*flat(task.inputs for task in tasks))


KEY_BLOCK = 256


def dot_nt(left, right):
    return lax.dot_general(left, right, (((1,), (1,)), ((), ())), preferred_element_type=jnp.float32)


def dot_tn(left, right):
    return lax.dot_general(left, right, (((0,), (0,)), ((), ())), preferred_element_type=jnp.float32)


def turn(values, cos_wide, sin_wide):
    half = values.shape[1] // 2
    swapped = jnp.concatenate([values[:, half:], values[:, :half]], 1)
    return values * cos_wide + swapped * sin_wide


def block_of(k):
    return pl.ds(pl.multiple_of(k * KEY_BLOCK, KEY_BLOCK), KEY_BLOCK)


def masked_block(q_nope, q_rope, kv_ref, keys_ref, base, k, h):
    at = block_of(k)
    wide = NOPE + VD
    scores = dot_nt(q_nope, kv_ref[at, wide * h : wide * h + NOPE])
    scores = scores + dot_nt(q_rope, keys_ref[at, R : R + ROPE])
    key_pos = k * KEY_BLOCK + lax.broadcasted_iota(jnp.int32, scores.shape, 1)
    query_pos = base + lax.broadcasted_iota(jnp.int32, scores.shape, 0)
    return jnp.where(key_pos <= query_pos, scores, masked_score)


def attend_kernel(
    base_ref, x_ref, wq_ref, keys_ref, wup_ref, wo_ref, cos_ref, sin_ref,
    q_ref, kv_ref, o_ref, lse_ref, attn_ref, s_ref, sum_ref,
):
    base = base_ref[0]
    rows = x_ref.shape[0]
    blocks = keys_ref.shape[0] // KEY_BLOCK
    factor = (NOPE + ROPE) ** (-0.5)
    query = jnp.dot(x_ref[...], wq_ref[...], preferred_element_type=jnp.float32) * factor

    def expand(k, carry):
        at = block_of(k)
        kv_ref[at, :] = jnp.dot(
            keys_ref[at, :R], wup_ref[...], preferred_element_type=jnp.float32
        ).astype(jnp.bfloat16)
        return carry

    lax.fori_loop(0, blocks, expand, 0)
    for h in range(2):
        start = h * (NOPE + ROPE)
        q_nope = query[:, start : start + NOPE].astype(jnp.bfloat16)
        q_rope = turn(
            query[:, start + NOPE : start + NOPE + ROPE], cos_ref[...], sin_ref[...]
        ).astype(jnp.bfloat16)
        q_ref[:, 256 * h : 256 * h + NOPE] = q_nope
        q_ref[:, 256 * h + NOPE : 256 * h + NOPE + ROPE] = q_rope
        q_ref[:, 256 * h + NOPE + ROPE : 256 * (h + 1)] = jnp.zeros(
            (rows, 256 - NOPE - ROPE), jnp.bfloat16
        )

        def first(k, top, h=h, q_nope=q_nope, q_rope=q_rope):
            scores = masked_block(q_nope, q_rope, kv_ref, keys_ref, base, k, h)
            s_ref[k] = scores
            return jnp.maximum(top, jnp.maximum(scores[:, :128], scores[:, 128:]))

        top = lax.fori_loop(0, blocks, first, jnp.full((rows, 128), masked_score, jnp.float32))
        top = jnp.max(top, 1, keepdims=True)

        def second(k, carry, h=h, top=top):
            total, acc = carry
            weights = jnp.exp(s_ref[k] - top)
            total = total + weights[:, :128] + weights[:, 128:]
            value = kv_ref[block_of(k), 256 * h + NOPE : 256 * (h + 1)]
            acc = acc + jnp.dot(
                weights.astype(jnp.bfloat16), value, preferred_element_type=jnp.float32
            )
            return total, acc

        zero = jnp.zeros((rows, 128), jnp.float32)
        total, acc = lax.fori_loop(0, blocks, second, (zero, zero))
        total = jnp.sum(total, 1, keepdims=True)
        o_ref[:, VD * h : VD * (h + 1)] = (acc / total).astype(jnp.bfloat16)
        lse_ref[:, 128 * h : 128 * (h + 1)] = jnp.broadcast_to(top + jnp.log(total), (rows, 128))
    part = jnp.dot(o_ref[...], wo_ref[...], preferred_element_type=jnp.float32)

    @pl.when(pl.program_id(0) == 0)
    def _():
        sum_ref[...] = part

    @pl.when(pl.program_id(0) > 0)
    def _():
        sum_ref[...] += part

    @pl.when(pl.program_id(0) == pl.num_programs(0) - 1)
    def _():
        attn_ref[...] = sum_ref[...].astype(jnp.bfloat16)


def whole_block(shape):
    return pl.BlockSpec(shape, lambda i: (0,) * len(shape))


def column_block(shape):
    return pl.BlockSpec(shape, lambda i: (0, i))


def attend(base, x, wq, keys, wup, wo, cos_wide, sin_wide):
    rows, width = x.shape
    heads = wo.shape[0] // VD
    count = keys.shape[0]
    struct = jax.ShapeDtypeStruct
    return pl.pallas_call(
        attend_kernel,
        name="attend",
        grid=(heads // 2,),
        in_specs=[
            pl.BlockSpec(memory_space=pltpu.SMEM),
            whole_block((rows, width)),
            column_block((width, 2 * (NOPE + ROPE))),
            whole_block(keys.shape),
            column_block((R, 2 * (NOPE + VD))),
            pl.BlockSpec((2 * VD, width), lambda i: (i, 0)),
            whole_block(cos_wide.shape),
            whole_block(sin_wide.shape),
        ],
        out_specs=[
            column_block((rows, 512)),
            column_block((count, 512)),
            column_block((rows, 2 * VD)),
            column_block((rows, 256)),
            whole_block((rows, width)),
        ],
        out_shape=[
            struct((rows, heads * 256), jnp.bfloat16),
            struct((count, heads * 256), jnp.bfloat16),
            struct((rows, heads * VD), jnp.bfloat16),
            struct((rows, heads * 128), jnp.float32),
            struct((rows, width), jnp.bfloat16),
        ],
        scratch_shapes=[
            pltpu.VMEM((count // KEY_BLOCK, rows, KEY_BLOCK), jnp.float32),
            pltpu.VMEM((rows, width), jnp.float32),
        ],
        compiler_params=pltpu.CompilerParams(vmem_limit_bytes=48 << 20),
        cost_estimate=pl.CostEstimate(
            flops=7 * 10**9, bytes_accessed=20 << 20, transcendentals=2 << 20
        ),
    )(base, x, wq, keys, wup, wo, cos_wide, sin_wide)


def attend_back_kernel(
    base_ref, q_ref, kv_ref, keys_ref, lse_ref, da_ref, wo_ref, wup_ref, cos_ref, sin_ref,
    dq_ref, dup_ref, dlat_ref, p_ref, dp_ref, dkv_ref, lat_ref, rope_ref, up_ref, acc_ref,
):
    base = base_ref[0]
    rows = q_ref.shape[0]
    blocks = keys_ref.shape[0] // KEY_BLOCK
    factor = (NOPE + ROPE) ** (-0.5)
    step = pl.program_id(0)

    @pl.when(step == 0)
    def _():
        lat_ref[...] = jnp.zeros_like(lat_ref)
        rope_ref[...] = jnp.zeros_like(rope_ref)

    up_ref[...] = jnp.zeros_like(up_ref)
    acc_ref[...] = jnp.zeros_like(acc_ref)
    d_out = dot_nt(da_ref[...], wo_ref[...]).astype(jnp.bfloat16)
    deltas = []
    for h in range(2):
        q_nope = q_ref[:, 256 * h : 256 * h + NOPE]
        q_rope = q_ref[:, 256 * h + NOPE : 256 * h + NOPE + ROPE]
        lse = lse_ref[:, 128 * h : 128 * h + 1]
        d_head = d_out[:, VD * h : VD * (h + 1)]

        def first(k, delta, h=h, q_nope=q_nope, q_rope=q_rope, lse=lse, d_head=d_head):
            at = block_of(k)
            scores = masked_block(q_nope, q_rope, kv_ref, keys_ref, base, k, h)
            probs = jnp.exp(scores - lse)
            d_probs = dot_nt(d_head, kv_ref[at, 256 * h + NOPE : 256 * (h + 1)])
            p_ref[h, k] = probs
            dp_ref[h, k] = d_probs
            dkv_ref[at, 256 * h + NOPE : 256 * (h + 1)] = dot_tn(
                probs.astype(jnp.bfloat16), d_head
            ).astype(jnp.bfloat16)
            both = probs * d_probs
            return delta + both[:, :128] + both[:, 128:]

        delta = lax.fori_loop(0, blocks, first, jnp.zeros((rows, 128), jnp.float32))
        deltas.append(jnp.sum(delta, 1, keepdims=True))

    def second(k, carry):
        at = block_of(k)
        for h in range(2):
            q_nope = q_ref[:, 256 * h : 256 * h + NOPE]
            q_rope = q_ref[:, 256 * h + NOPE : 256 * h + NOPE + ROPE]
            d_scores = (p_ref[h, k] * (dp_ref[h, k] - deltas[h])).astype(jnp.bfloat16)
            acc_ref[:, 256 * h : 256 * h + NOPE] += jnp.dot(
                d_scores, kv_ref[at, 256 * h : 256 * h + NOPE], preferred_element_type=jnp.float32
            )
            acc_ref[:, 256 * h + NOPE : 256 * h + NOPE + ROPE] += jnp.dot(
                d_scores, keys_ref[at, R : R + ROPE], preferred_element_type=jnp.float32
            )
            dkv_ref[at, 256 * h : 256 * h + NOPE] = dot_tn(d_scores, q_nope).astype(jnp.bfloat16)
            rope_ref[at, :] += dot_tn(d_scores, q_rope)
        d_kv = dkv_ref[at, :]
        lat_ref[at, :] += dot_nt(d_kv, wup_ref[...])
        up_ref[...] += dot_tn(keys_ref[at, :R], d_kv)
        return carry

    lax.fori_loop(0, blocks, second, 0)
    pieces = []
    for h in range(2):
        pieces.append(acc_ref[:, 256 * h : 256 * h + NOPE])
        pieces.append(
            turn(
                acc_ref[:, 256 * h + NOPE : 256 * h + NOPE + ROPE], cos_ref[...], -sin_ref[...]
            )
        )
    dq_ref[...] = (jnp.concatenate(pieces, 1) * factor).astype(jnp.bfloat16)
    dup_ref[...] = up_ref[...].astype(jnp.bfloat16)

    @pl.when(step == pl.num_programs(0) - 1)
    def _():
        dlat_ref[:, :R] = lat_ref[...].astype(jnp.bfloat16)
        dlat_ref[:, R:] = rope_ref[...].astype(jnp.bfloat16)


def attend_back(base, q, kv, keys, lse, d_attn, wo, wup, cos_wide, sin_wide):
    rows, width = d_attn.shape
    heads = wo.shape[0] // VD
    count = keys.shape[0]
    blocks = count // KEY_BLOCK
    struct = jax.ShapeDtypeStruct
    square = pltpu.VMEM((2, blocks, rows, KEY_BLOCK), jnp.float32)
    return pl.pallas_call(
        attend_back_kernel,
        name="attend_back",
        grid=(heads // 2,),
        in_specs=[
            pl.BlockSpec(memory_space=pltpu.SMEM),
            column_block((rows, 512)),
            column_block((count, 512)),
            whole_block(keys.shape),
            column_block((rows, 256)),
            whole_block(d_attn.shape),
            pl.BlockSpec((2 * VD, width), lambda i: (i, 0)),
            column_block((R, 2 * (NOPE + VD))),
            whole_block(cos_wide.shape),
            whole_block(sin_wide.shape),
        ],
        out_specs=[
            column_block((rows, 2 * (NOPE + ROPE))),
            column_block((R, 2 * (NOPE + VD))),
            whole_block(keys.shape),
        ],
        out_shape=[
            struct((rows, heads * (NOPE + ROPE)), jnp.bfloat16),
            struct((R, heads * (NOPE + VD)), jnp.bfloat16),
            struct(keys.shape, jnp.bfloat16),
        ],
        scratch_shapes=[
            square,
            square,
            pltpu.VMEM((count, 512), jnp.bfloat16),
            pltpu.VMEM((count, R), jnp.float32),
            pltpu.VMEM((count, ROPE), jnp.float32),
            pltpu.VMEM((R, 512), jnp.float32),
            pltpu.VMEM((rows, 512), jnp.float32),
        ],
        compiler_params=pltpu.CompilerParams(vmem_limit_bytes=56 << 20),
        cost_estimate=pl.CostEstimate(
            flops=10**10, bytes_accessed=20 << 20, transcendentals=2 << 20
        ),
    )(base, q, kv, keys, lse, d_attn, wo, wup, cos_wide, sin_wide)


def kept(shape, **kwargs):
    return pl.BlockSpec(shape, lambda i: (0,) * len(shape), pipeline_mode=pl.Buffered(1), **kwargs)


def expert_kernel(
    experts, first_ref, x_ref, g_ref, route_ref, eg_ref, eu_ref, ed_ref, sg_ref, su_ref, sd_ref,
    act_ref, turned_ref, dx_ref, dw_ref, weight_ref, gate_ref, up_ref, plain_ref, dgu_ref,
):
    local_experts, units, _ = eg_ref.shape
    shared_units = sg_ref.shape[0]
    wide = act_ref.shape[1]
    rows = x_ref.shape[0]
    taken = local_experts * units

    @pl.when(pl.program_id(0) == 0)
    def _():
        for k, (routed, shared) in enumerate(
            ((eg_ref, sg_ref), (eu_ref, su_ref), (ed_ref, sd_ref))
        ):
            start = k * wide
            for e in range(local_experts):
                weight_ref[start + e * units : start + (e + 1) * units, :] = routed[e]
            weight_ref[start + taken : start + taken + shared_units, :] = shared[...]
            weight_ref[start + taken + shared_units : start + wide, :] = jnp.zeros(
                (wide - taken - shared_units, weight_ref.shape[1]), jnp.bfloat16
            )

    plain_ref[...] = dot_nt(g_ref[...], weight_ref[2 * wide :, :])
    gate_ref[...] = dot_nt(x_ref[...], weight_ref[:wide, :])
    up_ref[...] = dot_nt(x_ref[...], weight_ref[wide : 2 * wide, :])
    step = 16

    def piece(k, carry):
        at = pl.ds(pl.multiple_of(k * step, step), step)
        gate, up, plain = gate_ref[at, :], up_ref[at, :], plain_ref[at, :]
        column = lax.broadcasted_iota(jnp.int32, gate.shape, 1)
        lane = lax.broadcasted_iota(jnp.int32, (step, 128), 1)
        routes = route_ref[at, :].astype(jnp.float32)
        scale = jnp.ones(gate.shape, jnp.float32)
        for e in reversed(range(local_experts)):
            mine = lax.rem(lane, experts) == first_ref[0] + e
            weight = jnp.sum(jnp.where(mine, routes, 0.0), 1, keepdims=True)
            scale = jnp.where(column < (e + 1) * units, weight, scale)
        logistic = 1.0 / (1.0 + jnp.exp(-gate))
        silu = gate * logistic
        act = silu * up
        act_ref[at, :] = (act * scale).astype(jnp.bfloat16)
        d_act = plain * scale
        dgu_ref[at, :wide] = (
            d_act * up * logistic * (1.0 + gate * (1.0 - logistic))
        ).astype(jnp.bfloat16)
        dgu_ref[at, wide:] = (d_act * silu).astype(jnp.bfloat16)
        dots = act * plain
        out = jnp.zeros((step, 128), jnp.float32)
        for e in range(local_experts):
            inside = (column >= e * units) & (column < (e + 1) * units)
            total = jnp.sum(jnp.where(inside, dots, 0.0), 1, keepdims=True)
            out = jnp.where(lane == first_ref[0] + e, total, out)
        dw_ref[at, :] = out.astype(jnp.bfloat16)
        return carry

    lax.fori_loop(0, rows // step, piece, 0)
    turned_ref[: 2 * wide, :] = dgu_ref[...].T
    turned_ref[2 * wide :, :] = act_ref[...].T
    dx_ref[...] = jnp.dot(
        dgu_ref[...], weight_ref[: 2 * wide, :], preferred_element_type=jnp.float32
    ).astype(jnp.bfloat16)


def run_experts(experts, first, x, g, route, eg, eu, ed, sg, su, sd):
    tokens, width = x.shape
    local_experts, units, _ = eg.shape
    wide = -(-(local_experts * units + sg.shape[0]) // 128) * 128
    rows = 256
    struct = jax.ShapeDtypeStruct

    def row_block(columns):
        return pl.BlockSpec((rows, columns), lambda i: (i, 0))

    return pl.pallas_call(
        functools.partial(expert_kernel, experts),
        name="experts",
        grid=(tokens // rows,),
        in_specs=[
            pl.BlockSpec(memory_space=pltpu.SMEM),
            row_block(width),
            row_block(width),
            row_block(128),
        ]
        + [kept(one.shape) for one in (eg, eu, ed, sg, su, sd)],
        out_specs=[
            row_block(wide),
            pl.BlockSpec((3 * wide, rows), lambda i: (0, i)),
            row_block(width),
            row_block(128),
        ],
        out_shape=[
            struct((tokens, wide), jnp.bfloat16),
            struct((3 * wide, tokens), jnp.bfloat16),
            struct((tokens, width), jnp.bfloat16),
            struct((tokens, 128), jnp.bfloat16),
        ],
        scratch_shapes=[pltpu.VMEM((3 * wide, width), jnp.bfloat16)]
        + [pltpu.VMEM((rows, wide), jnp.float32)] * 3
        + [pltpu.VMEM((rows, 2 * wide), jnp.bfloat16)],
        compiler_params=pltpu.CompilerParams(vmem_limit_bytes=58 << 20),
        cost_estimate=pl.CostEstimate(
            flops=10 * tokens * width * wide, bytes_accessed=50 << 20, transcendentals=2 << 20
        ),
    )(first, x, g, route, eg, eu, ed, sg, su, sd)


def weight_step(ins, outs, extra):
    x_ref, g_ref, act_ref, turned_ref, ed_ref, sd_ref = ins
    eg_ref, eu_ref, edg_ref, shared_ref, sum_ref = outs
    (wd_ref,) = extra
    local_experts, units, _ = edg_ref.shape
    shared_units = shared_ref.shape[1]
    wide = act_ref.shape[1]
    taken = local_experts * units

    @pl.when(pl.program_id(0) == 0)
    def _():
        wd_ref[...] = jnp.zeros_like(wd_ref)

    def gradient(k, routed, right):
        part = jnp.dot(
            turned_ref[k * wide : (k + 1) * wide, :],
            right[...],
            preferred_element_type=jnp.float32,
        )
        for e in range(local_experts):
            routed[e] = part[e * units : (e + 1) * units]
        shared_ref[k] = part[taken : taken + shared_units].astype(jnp.bfloat16)

    @pl.when(lax.rem(pl.program_id(0), 2) == 0)
    def _():
        gradient(0, eg_ref, x_ref)
        gradient(1, eu_ref, x_ref)

    @pl.when(lax.rem(pl.program_id(0), 2) == 1)
    def _():
        for e in range(local_experts):
            wd_ref[e * units : (e + 1) * units, :] = ed_ref[e]
        wd_ref[taken : taken + shared_units, :] = sd_ref[...]
        sum_ref[...] = jnp.dot(
            act_ref[...], wd_ref[...], preferred_element_type=jnp.float32
        ).astype(jnp.bfloat16)
        gradient(2, edg_ref, g_ref)


SLOTS = (0, 1, 1, 2, 4, 4, 7, 7, 10, 10, 13, 13, 16)


def run_weights(x, g, act, turned, ed, sd, tasks, collective_id):
    tokens, width = x.shape
    local_experts, units, _ = ed.shape
    shared_units = sd.shape[0]
    wide = act.shape[1]
    columns = 256
    steps = 2 * (width // columns)
    struct = jax.ShapeDtypeStruct

    def column(shape):
        return pl.BlockSpec(shape, lambda i: (0,) * (len(shape) - 1) + (i // 2,))

    ins = [x, g, act, turned, ed, sd]
    in_specs = [
        column((tokens, columns)),
        column((tokens, columns)),
        kept(act.shape),
        kept(turned.shape),
        column((local_experts, units, columns)),
        column((shared_units, columns)),
    ]
    out_specs = [column((local_experts, units, columns))] * 3 + [
        column((3, shared_units, columns)),
        column((tokens, columns)),
    ]
    out_shape = [struct((local_experts, units, width), jnp.float32)] * 3 + [
        struct((3, shared_units, width), jnp.bfloat16),
        struct((tokens, width), jnp.bfloat16),
    ]
    scratch = [pltpu.VMEM((wide, columns), jnp.bfloat16)]
    own = (len(ins), len(out_specs), len(scratch))

    def kernel(*refs):
        refs = list(refs)

        def take(counts):
            return [[refs.pop(0) for _ in range(count)] for count in counts]

        inputs = take([own[0]] + [len(task.inputs) for task in tasks])
        outputs = take([own[1]] + [len(task.outputs) for task in tasks])
        extra = take([own[2]] + [len(task.scratch) for task in tasks])
        running = []
        if tasks:
            place = Place()
            running = [
                task.steps(place, a, b, c)
                for task, a, b, c in zip(tasks, inputs[1:], outputs[1:], extra[1:])
            ]
            for walk in running:
                next(walk)

        def rounds(slot, step):
            @pl.when(pl.program_id(0) == step)
            def _():
                if slot == 0:
                    greet(place)
                for _ in range(SLOTS.count(slot)):
                    for walk in running:
                        next(walk, None)

        if running:
            for slot in sorted(set(SLOTS) - {steps}):
                rounds(slot, slot)
        weight_step(inputs[0], outputs[0], extra[0])
        if running:
            rounds(steps, steps - 1)

    for task in tasks:
        for one in task.inputs:
            ins.append(one)
            in_specs.append(kept(one.shape))
        for one in task.outputs:
            out_shape.append(one)
            out_specs.append(kept(one.shape))
        scratch += task.scratch
    params = {"collective_id": collective_id, "has_side_effects": True} if tasks else {}
    return pl.pallas_call(
        kernel,
        name="weights",
        grid=(steps,),
        in_specs=in_specs,
        out_specs=out_specs,
        out_shape=out_shape,
        scratch_shapes=scratch,
        compiler_params=pltpu.CompilerParams(vmem_limit_bytes=61 << 20, **params),
        cost_estimate=pl.CostEstimate(
            flops=8 * tokens * width * wide, bytes_accessed=60 << 20, transcendentals=0
        ),
    )(*ins)


def shards(
    tokens,
    norm_attn_gain,
    query_weight,
    latent_down,
    latent_gain,
    latent_up,
    out_weight,
    norm_ffn_gain,
    router_weight,
    shared_gate,
    shared_up,
    shared_down,
    expert_gate,
    expert_up,
    expert_down,
    expert_ids,
    out_grad,
):
    tok_rows, model_width = tokens.shape
    head_count = out_weight.shape[0] // VD
    groups = lax.axis_size("dp")
    parts = lax.axis_size("tensor")
    my_group = lax.axis_index("dp")
    my_part = lax.axis_index("tensor")
    stride = groups // SEQ_DEVS
    local_experts, _, units = expert_gate.shape
    experts = local_experts * groups
    rows = tok_rows // parts
    shared_units = shared_gate.shape[1] // groups
    used_units = local_experts * units + shared_units
    spare_units = -used_units % 128
    seq_stretch = my_group // stride
    direct = groups == PLANE and parts == DEPTH

    residual_in = tokens.astype(jnp.float32)
    normed_in, inv_one = rms_forward(residual_in, norm_attn_gain)
    normed_low = low(normed_in)
    query_pos = seq_stretch * tok_rows + jnp.arange(tok_rows)
    cos_table, sin_table = rotation(query_pos)
    factor = (NOPE + ROPE) ** (-0.5)
    compressed = mat_dot(normed_low, latent_down)
    latent_normed, inv_latent = rms_forward(compressed[:, :R], latent_gain)
    key_rope = rotate(compressed[:, R:], cos_table, sin_table)
    own_latent = low(jnp.concatenate([latent_normed, key_rope], -1))
    if direct:
        halves = own_latent.reshape(2, tok_rows // 2, R + ROPE)
        (keys_latent,) = exchange([GatherPlane(halves, False)], 0, "gather_keys")
        keys_latent = keys_latent.reshape(groups * tok_rows, R + ROPE)
        key_pos = jnp.arange(keys_latent.shape[0])
    elif stride == 1:
        keys_latent = gather(own_latent, "dp")
        key_pos = jnp.arange(keys_latent.shape[0])
    else:
        earlier = [
            from_behind(own_latent, "dp", (SEQ_DEVS - 1 - block_index) * stride)
            for block_index in range(SEQ_DEVS - 1)
        ]
        keys_latent = jnp.concatenate(earlier + [own_latent], 0)
        key_pos = (seq_stretch - (SEQ_DEVS - 1)) * tok_rows + jnp.arange(keys_latent.shape[0])
    key_count = keys_latent.shape[0]
    if direct:
        late_grad, keys_latent = lax.optimization_barrier((out_grad, keys_latent))
        grad_all = gather(late_grad, "dp")
    else:
        grad_all = gather(out_grad, "dp")
    query = mat_dot(normed_low, query_weight).reshape(tok_rows, head_count, NOPE + ROPE)
    query = (
        jnp.concatenate(
            [
                query[..., :NOPE],
                rotate(query[..., NOPE:], cos_table[:, None, :], sin_table[:, None, :]),
            ],
            -1,
        )
        * factor
    )
    query_low = low(query)
    expanded = low(mat_dot(keys_latent[:, :R], latent_up)).reshape(
        key_count, head_count, NOPE + VD
    )
    visible = (key_pos[None, :] >= 0) & (key_pos[None, :] <= query_pos[:, None])

    def attention_scores():
        raw_scores = jnp.einsum(
            "qhd,khd->hqk",
            query_low[..., :NOPE],
            expanded[..., :NOPE],
            preferred_element_type=jnp.float32,
        )
        raw_scores = raw_scores + jnp.einsum(
            "qhd,kd->hqk",
            query_low[..., NOPE:],
            keys_latent[:, R:],
            preferred_element_type=jnp.float32,
        )
        return jnp.where(visible[None], raw_scores, masked_score)

    scores = attention_scores()
    top_score = jnp.max(scores, -1, keepdims=True)
    exp_scores = jnp.exp(scores - top_score)
    exp_total = jnp.sum(exp_scores, -1, keepdims=True)
    log_total = top_score + jnp.log(exp_total)
    probs_low = low(exp_scores / exp_total)
    heads_out = jnp.einsum(
        "hqk,khd->qhd", probs_low, expanded[..., NOPE:], preferred_element_type=jnp.float32
    )
    heads_low = low(heads_out.reshape(tok_rows, head_count * VD))
    if direct:
        cos_wide = jnp.concatenate([cos_table, cos_table], 1)
        sin_wide = jnp.concatenate([-sin_table, sin_table], 1)
        first_row = jnp.full((1,), my_group * tok_rows, jnp.int32)
        query_kept, expanded_kept, heads_low, log_kept, attn = attend(
            first_row, normed_low, query_weight, keys_latent, latent_up, out_weight, cos_wide, sin_wide
        )
        (attn,) = exchange(
            [ScatterLevels(attn.reshape(parts, rows, model_width))], 1, "scatter_attn"
        )
    else:
        attn = scatter(mat_dot(heads_low, out_weight), "tensor")

    def own_rows(value):
        return lax.dynamic_slice_in_dim(value, my_part * rows, rows, 0)

    hidden = own_rows(residual_in) + attn
    ffn_in, inv_two = rms_forward(hidden, norm_ffn_gain)
    ffn_low = low(ffn_in)
    router = router_weight.astype(jnp.float32)
    router_gates = jax.nn.sigmoid(
        jnp.dot(ffn_in, router, precision=highest, preferred_element_type=jnp.float32)
    )
    picked = jnp.any(
        own_rows(expert_ids)[..., None] == jnp.arange(experts)[None, None, :], 1
    ).astype(jnp.float32)
    chosen = picked * router_gates
    chosen_sum = jnp.sum(chosen, -1, keepdims=True)
    route = route_scale * chosen / chosen_sum
    route_high = low(route)
    route_rest = low(route - route_high.astype(jnp.float32))
    routes = jnp.concatenate([route_high, route_rest], 1)
    if direct:
        routes = jnp.pad(routes, ((0, 0), (0, 128 - 2 * experts)))
        ffn_all, routes = exchange(
            [GatherPlane(ffn_low, True), GatherPlane(routes, True)], 2, "gather_ffn"
        )
        ffn_all = ffn_all.reshape(-1, model_width)
        routes = routes.reshape(-1, 128)
        token_count = routes.shape[0]
        first_expert = jnp.full((1,), my_group * local_experts, jnp.int32)

        def own_units(value):
            return lax.dynamic_slice_in_dim(value, my_group * shared_units, shared_units, 0)

        shared_own = own_units(shared_gate.T), own_units(shared_up.T), own_units(shared_down)
        act_low, turned, ffn_grad, weight_grad = run_experts(
            experts,
            first_expert,
            ffn_all,
            grad_all,
            routes,
            expert_gate.transpose(0, 2, 1),
            expert_up.transpose(0, 2, 1),
            expert_down,
            *shared_own,
        )
        (
            expert_gate_grad,
            expert_up_grad,
            expert_down_grad,
            shared_grads,
            moe_out,
            ffn_grad,
            weight_grad,
        ) = run_weights(
            ffn_all,
            grad_all,
            act_low,
            turned,
            expert_down,
            shared_own[2],
            [
                ScatterPlane(ffn_grad.reshape(groups, parts, rows, model_width), True),
                ScatterPlane(weight_grad.reshape(groups, parts, rows, 128), True),
            ],
            3,
        )
        expert_gate_grad = expert_gate_grad.transpose(0, 2, 1)
        expert_up_grad = expert_up_grad.transpose(0, 2, 1)
        shared_grads = lax.all_to_all(
            shared_grads, "dp", split_axis=2, concat_axis=1, tiled=True
        ).astype(jnp.float32)
        shared_gate_grad, shared_up_grad = shared_grads[0].T, shared_grads[1].T
        shared_down_grad = shared_grads[2]
        weight_grad = weight_grad[:, :experts]
    else:
        ffn_all = gather(jnp.concatenate([ffn_low, routes], 1), BOTH)
        routes = ffn_all[:, model_width:]
        ffn_all = ffn_all[:, :model_width]
        route_all = routes[:, :experts].astype(jnp.float32) + routes[
            :, experts : 2 * experts
        ].astype(jnp.float32)
        token_count = ffn_all.shape[0]
        route_own = lax.dynamic_slice_in_dim(route_all, my_group * local_experts, local_experts, 1)

        def joined(expert_weight, shared_weight):
            own = lax.dynamic_slice_in_dim(shared_weight, my_group * shared_units, shared_units, 1)
            pieces = [expert_weight[e] for e in range(local_experts)]
            return jnp.concatenate(
                pieces + [own, jnp.zeros((model_width, spare_units), jnp.bfloat16)], 1
            )

        gate_weight = joined(expert_gate, shared_gate)
        up_weight = joined(expert_up, shared_up)
        down_weight = jnp.concatenate(
            [expert_down[e] for e in range(local_experts)]
            + [
                lax.dynamic_slice_in_dim(shared_down, my_group * shared_units, shared_units, 0),
                jnp.zeros((spare_units, model_width), jnp.bfloat16),
            ],
            0,
        )
        scale = jnp.concatenate(
            [
                jnp.broadcast_to(route_own[:, e : e + 1], (token_count, units))
                for e in range(local_experts)
            ]
            + [jnp.ones((token_count, shared_units + spare_units), jnp.float32)],
            1,
        )
        plain_grad = contract_cols(grad_all, down_weight)
        gate_act = mat_dot(ffn_all, gate_weight)
        up_act = mat_dot(ffn_all, up_weight)
        logistic = jax.nn.sigmoid(gate_act)
        silu = gate_act * logistic
        act = silu * up_act
        act_low = low(act * scale)
        act_grad = plain_grad * scale
        gate_grad = low(act_grad * up_act * logistic * (1.0 + gate_act * (1.0 - logistic)))
        up_grad = low(act_grad * silu)
        weight_dots = act * plain_grad
        weight_grad = jnp.stack(
            [
                jnp.sum(weight_dots[:, e * units : (e + 1) * units], 1)
                for e in range(local_experts)
            ],
            1,
        )
        weight_grad = lax.dynamic_update_slice_in_dim(
            jnp.zeros((token_count, experts), jnp.bfloat16),
            low(weight_grad),
            my_group * local_experts,
            1,
        )
        ffn_grad = contract_cols(gate_grad, gate_weight) + contract_cols(up_grad, up_weight)
        ffn_grad = scatter(jnp.concatenate([low(ffn_grad), weight_grad], 1), BOTH)
        weight_grad = ffn_grad[:, model_width:]
        ffn_grad = ffn_grad[:, :model_width]
        moe_out = mat_dot(act_low, down_weight)

        down_grad = contract_rows(act_low, grad_all)
        gate_weight_grad = contract_rows(ffn_all, gate_grad)
        up_weight_grad = contract_rows(ffn_all, up_grad)
        expert_down_grad = down_grad[: local_experts * units].reshape(local_experts, units, -1)
        expert_gate_grad = jnp.stack(
            [gate_weight_grad[:, e * units : (e + 1) * units] for e in range(local_experts)]
        )
        expert_up_grad = jnp.stack(
            [up_weight_grad[:, e * units : (e + 1) * units] for e in range(local_experts)]
        )

        def swap(value):
            return lax.all_to_all(low(value), "dp", split_axis=0, concat_axis=1, tiled=True).astype(
                jnp.float32
            )

        first = local_experts * units
        shared_gate_grad = swap(gate_weight_grad[:, first:used_units])
        shared_up_grad = swap(up_weight_grad[:, first:used_units])
        shared_down_grad = lax.all_to_all(
            low(down_grad[first:used_units]), "dp", split_axis=1, concat_axis=0, tiled=True
        ).astype(jnp.float32)

    moe_out = scatter(scatter(moe_out, "dp"), "tensor")
    block_out = gather(low(hidden + moe_out), "tensor")

    inner_sum = jnp.sum(weight_grad * chosen, -1, keepdims=True)
    chosen_grad = route_scale * (weight_grad / chosen_sum - inner_sum / (chosen_sum * chosen_sum))
    logit_grad = chosen_grad * chosen * (1.0 - chosen)
    router_grad = jnp.dot(
        ffn_in.T, logit_grad, precision=highest, preferred_element_type=jnp.float32
    )
    norm_grad = ffn_grad + jnp.dot(
        logit_grad, router.T, precision=highest, preferred_element_type=jnp.float32
    )
    hidden_extra, norm_ffn_grad = rms_backward(hidden, inv_two, norm_ffn_gain, norm_grad)
    hidden_grad = own_rows(out_grad).astype(jnp.float32) + hidden_extra
    if direct:
        (attn_grad_low,) = exchange([GatherLevels(low(hidden_grad))], 4, "gather_hidden")
        attn_grad_low = attn_grad_low.reshape(tok_rows, model_width)
    else:
        attn_grad_low = gather(low(hidden_grad), "tensor")

    out_weight_grad = scatter(contract_rows(heads_low, attn_grad_low), "dp", 1)
    if direct:
        query_grad_low, latent_up_grad, latent_grad = attend_back(
            first_row,
            query_kept,
            expanded_kept,
            keys_latent,
            log_kept,
            attn_grad_low,
            out_weight,
            latent_up,
            cos_wide,
            sin_wide,
        )
    else:
        heads_grad = low(contract_cols(attn_grad_low, out_weight)).reshape(tok_rows, head_count, VD)
        attn_probs = jnp.exp(attention_scores() - log_total)
        probs_low = low(attn_probs)
        value_grad = jnp.einsum(
            "hqk,qhd->khd", probs_low, heads_grad, preferred_element_type=jnp.float32
        )
        prob_grad = jnp.einsum(
            "qhd,khd->hqk", heads_grad, expanded[..., NOPE:], preferred_element_type=jnp.float32
        )
        row_delta = jnp.sum(attn_probs * prob_grad, -1, keepdims=True)
        score_grad = low(attn_probs * (prob_grad - row_delta))
        nope_grad = jnp.einsum(
            "hqk,khd->qhd", score_grad, expanded[..., :NOPE], preferred_element_type=jnp.float32
        )
        rope_grad = jnp.einsum(
            "hqk,kd->qhd", score_grad, keys_latent[:, R:], preferred_element_type=jnp.float32
        )
        key_nope_grad = jnp.einsum(
            "hqk,qhd->khd", score_grad, query_low[..., :NOPE], preferred_element_type=jnp.float32
        )
        key_rope_grad = jnp.einsum(
            "hqk,qhd->kd", score_grad, query_low[..., NOPE:], preferred_element_type=jnp.float32
        )
        expand_grad = low(
            jnp.concatenate([key_nope_grad, value_grad], -1).reshape(
                key_count, head_count * (NOPE + VD)
            )
        )
        latent_up_grad = contract_rows(keys_latent[:, :R], expand_grad)
        latent_grad = jnp.concatenate([contract_cols(expand_grad, latent_up), key_rope_grad], -1)
        query_grad = (
            jnp.concatenate(
                [nope_grad, unrotate(rope_grad, cos_table[:, None, :], sin_table[:, None, :])], -1
            )
            * factor
        )
        query_grad_low = low(query_grad.reshape(tok_rows, head_count * (NOPE + ROPE)))
    query_weight_grad = contract_rows(normed_low, query_grad_low)
    input_part = contract_cols(query_grad_low, query_weight)
    if direct:
        own_grad, input_sum, query_weight_grad, latent_up_grad = exchange(
            [
                ScatterPlane(low(latent_grad).reshape(groups, parts, rows, R + ROPE), True),
                ScatterLevels(low(input_part).reshape(parts, rows, model_width)),
                ScatterPlane(low(query_weight_grad).reshape(groups, 2, model_width // 16, -1), False),
                ScatterPlane(low(latent_up_grad).reshape(groups, 2, R // 16, -1), False),
            ],
            5,
            "scatter_latent",
        )
        query_weight_grad = query_weight_grad.reshape(model_width // groups, -1)
        latent_up_grad = latent_up_grad.reshape(R // groups, -1)
    else:
        if stride == 1:
            own_grad = scatter(scatter(latent_grad, "dp"), "tensor")
        else:
            own_grad = latent_grad[(SEQ_DEVS - 1) * tok_rows :]
            for block_index in range(SEQ_DEVS - 1):
                piece_grad = latent_grad[block_index * tok_rows : (block_index + 1) * tok_rows]
                own_grad = own_grad + from_behind(
                    low(piece_grad), "dp", -(SEQ_DEVS - 1 - block_index) * stride
                ).astype(piece_grad.dtype)
            own_grad = scatter(own_grad, "tensor")
        input_sum = scatter(input_part, "tensor")
        query_weight_grad = scatter(query_weight_grad, "dp")
        latent_up_grad = scatter(latent_up_grad, "dp")
    compressed_own = own_rows(compressed)
    normed_part, latent_gain_grad = rms_backward(
        compressed_own[:, :R], own_rows(inv_latent), latent_gain, own_grad[:, :R]
    )
    compressed_grad = low(
        jnp.concatenate(
            [normed_part, unrotate(own_grad[:, R:], own_rows(cos_table), own_rows(sin_table))], -1
        )
    )
    latent_down_grad = contract_rows(own_rows(normed_low), compressed_grad)
    normed_grad = input_sum + contract_cols(compressed_grad, latent_down)
    input_extra, norm_attn_grad = rms_backward(
        own_rows(residual_in), own_rows(inv_one), norm_attn_gain, normed_grad
    )
    tokens_grad = low(hidden_grad + input_extra)
    small = [norm_attn_grad, latent_gain_grad, norm_ffn_grad, router_grad]
    sizes = [one.size // groups for one in small]
    small = jnp.concatenate([one.reshape(groups, -1) for one in small], 1)
    if direct:
        small = jnp.pad(low(small), ((0, 0), (0, parts * 2048 - small.shape[1])))
        latent_down_grad, small, tokens_grad = exchange(
            [
                ScatterPlane(
                    low(latent_down_grad).reshape(groups, parts, rows, R + ROPE), True, True
                ),
                ScatterPlane(small.reshape(groups, parts, 16, 128), True, True),
                GatherLevels(tokens_grad),
            ],
            6,
            "scatter_last",
        )
        latent_down_grad = latent_down_grad.reshape(-1, R + ROPE).astype(jnp.float32)
        small = small.reshape(-1).astype(jnp.float32)
        tokens_grad = tokens_grad.reshape(tok_rows, model_width)
    else:
        latent_down_grad = lax.psum(scatter(latent_down_grad, "dp"), "tensor")
        small = lax.psum(scatter(small, "dp"), "tensor").reshape(-1)
        tokens_grad = gather(tokens_grad, "tensor")
    offsets = [sum(sizes[:k]) for k in range(len(sizes))]
    norm_attn_grad, latent_gain_grad, norm_ffn_grad, router_grad = [
        small[start : start + size] for start, size in zip(offsets, sizes)
    ]

    return (
        block_out,
        tokens_grad,
        norm_attn_grad,
        query_weight_grad,
        latent_down_grad,
        latent_gain_grad,
        latent_up_grad,
        out_weight_grad,
        norm_ffn_grad,
        router_grad.reshape(-1, experts),
        shared_gate_grad,
        shared_up_grad,
        shared_down_grad,
        expert_gate_grad,
        expert_up_grad,
        expert_down_grad,
    )


def solution(mesh):
    in_specs = (
        P("dp", None),
        P(),
        P(None, "tensor"),
        P(),
        P(),
        P(None, "tensor"),
        P("tensor", None),
        P(),
        P(),
        P(None, "tensor"),
        P(None, "tensor"),
        P("tensor", None),
        P("dp", None, "tensor"),
        P("dp", None, "tensor"),
        P("dp", "tensor", None),
        P("dp", None),
        P("dp", None),
    )
    out_specs = (
        P("dp", None),
        P("dp", None),
        P("dp"),
        P("dp", "tensor"),
        P("dp", None),
        P("dp"),
        P("dp", "tensor"),
        P("tensor", "dp"),
        P("dp"),
        P("dp", None),
        P("dp", "tensor"),
        P("dp", "tensor"),
        P("tensor", "dp"),
        P("dp", None, "tensor"),
        P("dp", None, "tensor"),
        P("dp", "tensor", None),
    )
    return jax.shard_map(shards, mesh=mesh, in_specs=in_specs, out_specs=out_specs, check_vma=False)
```

```python
import functools

import jax
import jax.numpy as jnp
from jax import lax
from jax.experimental import pallas as pl
from jax.experimental.pallas import tpu as pltpu
from jax.sharding import PartitionSpec as P

NOPE = 128
ROPE = 64
VD = 128
R = 512
SEQ_DEVS = 8


eps = 1e-06
route_scale = 2.446
rope_base = 50000.0
masked_score = -1e30
highest = lax.Precision.HIGHEST
BOTH = ("dp", "tensor")


def from_behind(value, axis, steps):
    count = lax.axis_size(axis)
    initial, last = (max(0, -steps), min(count, count - steps))
    return lax.ppermute(value, axis, [(source, source + steps) for source in range(initial, last)])


def mat_dot(left, right):
    return jnp.dot(left, right, preferred_element_type=jnp.float32)


def contract_rows(left, right):
    return lax.dot_general(left, right, (((0,), (0,)), ((), ())), preferred_element_type=jnp.float32)


def contract_cols(left, right):
    return lax.dot_general(left, right, (((1,), (1,)), ((), ())), preferred_element_type=jnp.float32)


def rotation(positions):
    half_width = ROPE // 2
    frequency = rope_base ** (-jnp.arange(half_width, dtype=jnp.float32) / half_width)
    angles = positions.astype(jnp.float32)[:, None] * frequency[None, :]
    return (jnp.cos(angles), jnp.sin(angles))


def rotate(values, cos_table, sin_table):
    half_width = values.shape[-1] // 2
    first_half = values[..., :half_width]
    second_half = values[..., half_width:]
    return jnp.concatenate(
        [
            first_half * cos_table - second_half * sin_table,
            second_half * cos_table + first_half * sin_table,
        ],
        -1,
    )


def unrotate(upstream, cos_table, sin_table):
    return rotate(upstream, cos_table, -sin_table)


def rms_forward(values, gain_vec):
    inv_rms = lax.rsqrt(jnp.mean(values * values, axis=-1, keepdims=True) + eps)
    return (values * inv_rms * gain_vec, inv_rms)


def rms_backward(values, inv_rms, gain_vec, upstream):
    scaled = upstream * gain_vec
    inner_mean = jnp.mean(values * scaled, axis=-1, keepdims=True)
    return (
        inv_rms * scaled - values * inv_rms**3 * inner_mean,
        jnp.sum(upstream * values * inv_rms, axis=0),
    )


def low(value):
    return value.astype(jnp.bfloat16)


def gather(value, axes):
    return lax.all_gather(value, axes, tiled=True)


def scatter(value, axes, dimension=0):
    return lax.psum_scatter(
        low(value), axes, scatter_dimension=dimension, tiled=True
    ).astype(jnp.float32)


MESH = pl.DeviceIdType.MESH
PLANE = 8
DEPTH = 4


class Place:
    def __init__(self):
        self.me = lax.axis_index("dp")
        self.z = lax.axis_index("tensor")
        self.core = self.me % 2
        self.chip = self.me // 2
        self.chip_x = self.chip + 1 - 2 * (self.chip % 2)
        self.chip_y = (self.chip + 2) % 4
        self.chip_xy = 3 - self.chip
        self.sibling = self.me + 1 - 2 * self.core
        self.near_x = 2 * self.chip_x + self.core
        self.near_y = 2 * self.chip_y + self.core
        self.across = 2 * self.chip_xy + self.core
        self.levels = [self.z + 1 - 2 * (self.z % 2), (self.z + 2) % 4, 3 - self.z]


def push(src, dst, sems, index, **target):
    send, recv = sems
    return pltpu.make_async_remote_copy(
        src_ref=src,
        dst_ref=dst,
        send_sem=send.at[index],
        recv_sem=recv.at[index],
        device_id=target,
        device_id_type=MESH,
    )


def add_rows(target, sources):
    rows = target.shape[0]
    step = 16

    def one(k, carry):
        at = pl.ds(pl.multiple_of(k * step, step), step)
        acc = sources[0][at, :].astype(jnp.float32)
        for source in sources[1:]:
            acc = acc + source[at, :].astype(jnp.float32)
        target[at, :] = acc.astype(target.dtype)
        return carry

    lax.fori_loop(0, rows // step, one, 0)


def sem_pair(count):
    return [pltpu.SemaphoreType.DMA((count,)), pltpu.SemaphoreType.DMA((count,))]


class GatherPlane:
    def __init__(self, value, with_z):
        self.with_z = with_z
        self.inputs = [value]
        self.units = DEPTH if with_z else value.shape[0]
        rows, width = value.shape[-2:]
        self.in_specs = [pl.BlockSpec(memory_space=pltpu.VMEM)]
        self.outputs = [
            jax.ShapeDtypeStruct((PLANE, self.units, rows, width), value.dtype)
        ]
        self.out_specs = [pl.BlockSpec(memory_space=pl.ANY)]
        self.scratch = (
            sem_pair(7 * self.units)
            + sem_pair(DEPTH - 1)
            + [pltpu.SemaphoreType.DMA((1,))]
        )

    def steps(self, place, inputs, outputs, scratch):
        (x,), (out,) = inputs, outputs
        sems, z_sems, local = scratch[0:2], scratch[2:4], scratch[4]
        me, units = place.me, self.units
        sends = []
        if self.with_z:
            order = [place.z] + place.levels
            keep = pltpu.make_async_copy(x, out.at[me, place.z], local.at[0])
            arrivals = []
            for k, level in enumerate(place.levels):
                copy = push(x, out.at[me, place.z], z_sems, k, tensor=level)
                copy.start()
                sends.append(copy)
                here = out.at[me, level]
                arrivals.append(push(here, here, z_sems, k, tensor=level))
        else:
            order = list(range(units))
            keep = pltpu.make_async_copy(x, out.at[me], local.at[0])
        keep.start()

        def message(p, kind, slot, target, src=None):
            spot = out.at[slot, order[p]]
            return push(spot if src is None else src, spot, sems, 7 * p + kind, dp=target)

        def launch(*args, **kwargs):
            copy = message(*args, **kwargs)
            copy.start()
            sends.append(copy)

        def stage_own(p):
            if self.with_z:
                src = x if p == 0 else None
                if p > 0:
                    arrivals[p - 1].wait_recv()
            else:
                src = x.at[p]
            pair = [(0, place.near_x), (1, place.near_y)]
            for kind, target in pair if p % 2 == 0 else pair[::-1]:
                launch(p, kind, me, target, src)
            launch(p, 3, me, place.sibling, src)

        def stage_near(p):
            def from_x():
                message(p, 0, place.near_x, place.near_x).wait_recv()
                if p % 2 == 0:
                    launch(p, 2, place.near_x, place.near_y)
                launch(p, 4, place.near_x, place.sibling)

            def from_y():
                message(p, 1, place.near_y, place.near_y).wait_recv()
                if p % 2 == 1:
                    launch(p, 2, place.near_y, place.near_x)
                launch(p, 5, place.near_y, place.sibling)

            for part in (from_x, from_y) if p % 2 == 0 else (from_y, from_x):
                part()

        def stage_across(p):
            message(p, 2, place.across, place.near_x).wait_recv()
            launch(p, 6, place.across, place.sibling)

        for p in range(units + 2):
            if p < units:
                stage_own(p)
            yield
            if 0 <= p - 1 < units:
                stage_near(p - 1)
            if 0 <= p - 2 < units:
                stage_across(p - 2)
            yield
        keep.wait()
        base = place.sibling
        for p in range(units):
            for kind, chip in (
                (3, place.chip),
                (4, place.chip_x),
                (5, place.chip_y),
                (6, place.chip_xy),
            ):
                message(p, kind, 2 * chip + 1 - place.core, base).wait_recv()
        for copy in sends:
            copy.wait_send()


class ScatterPlane:
    def __init__(self, value, with_z, spread=False):
        self.with_z, self.spread = with_z, spread
        _, self.units, rows, width = value.shape
        self.inputs = [value.reshape(4, 2, self.units, rows, width)]
        self.in_specs = [pl.BlockSpec(memory_space=pltpu.VMEM)]
        units = self.units
        shape = (rows, width) if with_z else (units, rows, width)
        kind = jnp.float32
        if spread:
            shape, kind = (DEPTH, rows, width), jnp.bfloat16
        self.outputs = [jax.ShapeDtypeStruct(shape, kind)]
        self.out_specs = [pl.BlockSpec(memory_space=pltpu.VMEM)]
        buffer = pltpu.VMEM((units, rows, width), value.dtype)
        self.scratch = (
            sem_pair(4 * units)
            + [pltpu.VMEM((units, 4, rows, width), value.dtype)]
            + [buffer] * 6
        )
        if with_z:
            level = pltpu.VMEM((DEPTH - 1, rows, width), value.dtype)
            self.scratch += sem_pair(DEPTH - 1) + [level] * 2
        if spread:
            self.scratch += sem_pair(DEPTH - 1) + [pltpu.VMEM((rows, width), value.dtype)]

    def steps(self, place, inputs, outputs, scratch):
        (part,), (out,) = inputs, outputs
        sems, beside = scratch[0:2], scratch[2]
        d_send, d_recv, x_send, x_recv, y_send, y_recv = scratch[3:9]
        units, core = self.units, place.core
        other_core = 1 - core
        if self.with_z:
            z_sems, z_send, z_recv = scratch[9:11], scratch[11], scratch[12]
            near, far, other = place.levels
            order = [far, other, near, place.z]
        else:
            order = list(range(units))
        sends = []

        def launch(make, p):
            make(p).start()
            sends.append((make, p))

        def across(p):
            target = place.near_x if p % 2 == 0 else place.near_y
            return push(d_send.at[p], d_recv.at[p], sems, 4 * p + 1, dp=target)

        def to_x(p):
            return push(x_send.at[p], x_recv.at[p], sems, 4 * p + 2, dp=place.near_x)

        def to_y(p):
            return push(y_send.at[p], y_recv.at[p], sems, 4 * p + 3, dp=place.near_y)

        def to_sibling(p):
            return push(
                part.at[:, other_core, order[p]],
                beside.at[p],
                sems,
                4 * p,
                dp=place.sibling,
            )

        def both(p, chip):
            return [part.at[chip, core, order[p]], beside.at[p, chip]]

        def stage_one(p):
            to_sibling(p).wait_recv()
            add_rows(d_send.at[p], both(p, place.chip_xy))
            launch(across, p)
            if p % 2 == 0:
                add_rows(x_send.at[p], both(p, place.chip_x))
                launch(to_x, p)
            else:
                add_rows(y_send.at[p], both(p, place.chip_y))
                launch(to_y, p)

        def stage_two(p):
            across(p).wait_recv()
            if p % 2 == 0:
                add_rows(y_send.at[p], both(p, place.chip_y) + [d_recv.at[p]])
                launch(to_y, p)
            else:
                add_rows(x_send.at[p], both(p, place.chip_x) + [d_recv.at[p]])
                launch(to_x, p)

        def to_level(p):
            return push(z_send.at[p], z_recv.at[p], z_sems, p, tensor=order[p])

        def stage_three(p):
            to_x(p).wait_recv()
            to_y(p).wait_recv()
            pieces = both(p, place.chip) + [x_recv.at[p], y_recv.at[p]]
            if not self.with_z:
                add_rows(out.at[p], pieces)
            elif p < units - 1:
                add_rows(z_send.at[p], pieces)
                launch(to_level, p)
            else:
                for k in range(DEPTH - 1):
                    to_level(k).wait_recv()
                pieces += [z_recv.at[k] for k in range(DEPTH - 1)]
                add_rows(scratch[15] if self.spread else out, pieces)

        yield
        for p in range(units):
            launch(to_sibling, p)
        yield
        for p in range(units + 2):
            if p < units:
                stage_one(p)
            yield
            if 0 <= p - 1 < units:
                stage_two(p - 1)
            if 0 <= p - 2 < units:
                stage_three(p - 2)
            if p < units + 1:
                yield
        if self.spread:
            copies = []
            yield from spread_levels(place, scratch[15], out, scratch[13:15], copies)
            for copy in copies:
                copy.wait_send()
        for make, p in sends:
            make(p).wait_send()


def spread_levels(place, own, out, z_sems, sends):
    arrivals = []
    for k, level in enumerate(place.levels):
        copy = push(own, out.at[place.z], z_sems, k, tensor=level)
        copy.start()
        sends.append(copy)
        arrivals.append(push(own, out.at[level], z_sems, k, tensor=level))
    out[place.z] = own[...]
    yield
    for copy in arrivals:
        copy.wait_recv()


class GatherLevels:
    def __init__(self, value):
        self.inputs = [value]
        self.in_specs = [pl.BlockSpec(memory_space=pltpu.VMEM)]
        self.outputs = [jax.ShapeDtypeStruct((DEPTH,) + value.shape, value.dtype)]
        self.out_specs = [pl.BlockSpec(memory_space=pltpu.VMEM)]
        self.scratch = sem_pair(DEPTH - 1)

    def steps(self, place, inputs, outputs, scratch):
        sends = []
        yield from spread_levels(place, inputs[0], outputs[0], scratch[0:2], sends)
        for copy in sends:
            copy.wait_send()


class ScatterLevels:
    def __init__(self, value):
        _, rows, width = value.shape
        self.inputs = [value]
        self.in_specs = [pl.BlockSpec(memory_space=pltpu.VMEM)]
        self.outputs = [jax.ShapeDtypeStruct((rows, width), jnp.float32)]
        self.out_specs = [pl.BlockSpec(memory_space=pltpu.VMEM)]
        self.scratch = sem_pair(DEPTH - 1) + [pltpu.VMEM((DEPTH - 1, rows, width), value.dtype)]

    def steps(self, place, inputs, outputs, scratch):
        part, z_sems, landed = inputs[0], scratch[0:2], scratch[2]
        copies = [
            push(part.at[level], landed.at[k], z_sems, k, tensor=level)
            for k, level in enumerate(place.levels)
        ]
        for copy in copies:
            copy.start()
        yield
        yield
        yield
        for copy in copies:
            copy.wait_recv()
        add_rows(outputs[0], [part.at[place.z]] + [landed.at[k] for k in range(DEPTH - 1)])
        for copy in copies:
            copy.wait_send()


def greet(place):
    barrier = pltpu.get_barrier_semaphore()
    for target in (place.sibling, place.near_x, place.near_y):
        pl.semaphore_signal(barrier, inc=1, device_id={"dp": target}, device_id_type=MESH)
    for target in place.levels:
        pl.semaphore_signal(barrier, inc=1, device_id={"tensor": target}, device_id_type=MESH)
    pl.semaphore_wait(barrier, 6)


def exchange(tasks, collective_id, name):
    def kernel(*refs):
        place = Place()
        greet(place)
        refs = list(refs)

        def take(counts):
            return [[refs.pop(0) for _ in range(count)] for count in counts]

        inputs = take([len(task.inputs) for task in tasks])
        outputs = take([len(task.outputs) for task in tasks])
        scratch = take([len(task.scratch) for task in tasks])
        running = [
            task.steps(place, a, b, c)
            for task, a, b, c in zip(tasks, inputs, outputs, scratch)
        ]
        while running:
            for walk in list(running):
                if next(walk, running) is running:
                    running.remove(walk)

    def flat(pieces):
        return [one for piece in pieces for one in piece]

    moved = sum(one.size * one.dtype.itemsize for task in tasks for one in task.inputs)
    return pl.pallas_call(
        kernel,
        name=name,
        out_shape=flat(task.outputs for task in tasks),
        in_specs=flat(task.in_specs for task in tasks),
        out_specs=flat(task.out_specs for task in tasks),
        scratch_shapes=flat(task.scratch for task in tasks),
        compiler_params=pltpu.CompilerParams(
            collective_id=collective_id, has_side_effects=True, vmem_limit_bytes=56 << 20
        ),
        cost_estimate=pl.CostEstimate(flops=0, bytes_accessed=4 * moved, transcendentals=0),
    )(*flat(task.inputs for task in tasks))


KEY_BLOCK = 256


def dot_nt(left, right):
    return lax.dot_general(left, right, (((1,), (1,)), ((), ())), preferred_element_type=jnp.float32)


def dot_tn(left, right):
    return lax.dot_general(left, right, (((0,), (0,)), ((), ())), preferred_element_type=jnp.float32)


def turn(values, cos_wide, sin_wide):
    half = values.shape[1] // 2
    swapped = jnp.concatenate([values[:, half:], values[:, :half]], 1)
    return values * cos_wide + swapped * sin_wide


def block_of(k):
    return pl.ds(pl.multiple_of(k * KEY_BLOCK, KEY_BLOCK), KEY_BLOCK)


def masked_block(q_nope, q_rope, kv_ref, keys_ref, base, k, h):
    at = block_of(k)
    wide = NOPE + VD
    scores = dot_nt(q_nope, kv_ref[at, wide * h : wide * h + NOPE])
    scores = scores + dot_nt(q_rope, keys_ref[at, R : R + ROPE])
    key_pos = k * KEY_BLOCK + lax.broadcasted_iota(jnp.int32, scores.shape, 1)
    query_pos = base + lax.broadcasted_iota(jnp.int32, scores.shape, 0)
    return jnp.where(key_pos <= query_pos, scores, masked_score)


def attend_kernel(
    base_ref, x_ref, wq_ref, keys_ref, wup_ref, wo_ref, cos_ref, sin_ref,
    q_ref, kv_ref, o_ref, lse_ref, attn_ref, s_ref, sum_ref,
):
    base = base_ref[0]
    rows = x_ref.shape[0]
    blocks = keys_ref.shape[0] // KEY_BLOCK
    factor = (NOPE + ROPE) ** (-0.5)
    query = jnp.dot(x_ref[...], wq_ref[...], preferred_element_type=jnp.float32) * factor

    def expand(k, carry):
        at = block_of(k)
        kv_ref[at, :] = jnp.dot(
            keys_ref[at, :R], wup_ref[...], preferred_element_type=jnp.float32
        ).astype(jnp.bfloat16)
        return carry

    lax.fori_loop(0, blocks, expand, 0)
    for h in range(2):
        start = h * (NOPE + ROPE)
        q_nope = query[:, start : start + NOPE].astype(jnp.bfloat16)
        q_rope = turn(
            query[:, start + NOPE : start + NOPE + ROPE], cos_ref[...], sin_ref[...]
        ).astype(jnp.bfloat16)
        q_ref[:, 256 * h : 256 * h + NOPE] = q_nope
        q_ref[:, 256 * h + NOPE : 256 * h + NOPE + ROPE] = q_rope
        q_ref[:, 256 * h + NOPE + ROPE : 256 * (h + 1)] = jnp.zeros(
            (rows, 256 - NOPE - ROPE), jnp.bfloat16
        )

        def first(k, top, h=h, q_nope=q_nope, q_rope=q_rope):
            scores = masked_block(q_nope, q_rope, kv_ref, keys_ref, base, k, h)
            s_ref[k] = scores
            return jnp.maximum(top, jnp.maximum(scores[:, :128], scores[:, 128:]))

        top = lax.fori_loop(0, blocks, first, jnp.full((rows, 128), masked_score, jnp.float32))
        top = jnp.max(top, 1, keepdims=True)

        def second(k, carry, h=h, top=top):
            total, acc = carry
            weights = jnp.exp(s_ref[k] - top)
            total = total + weights[:, :128] + weights[:, 128:]
            value = kv_ref[block_of(k), 256 * h + NOPE : 256 * (h + 1)]
            acc = acc + jnp.dot(
                weights.astype(jnp.bfloat16), value, preferred_element_type=jnp.float32
            )
            return total, acc

        zero = jnp.zeros((rows, 128), jnp.float32)
        total, acc = lax.fori_loop(0, blocks, second, (zero, zero))
        total = jnp.sum(total, 1, keepdims=True)
        o_ref[:, VD * h : VD * (h + 1)] = (acc / total).astype(jnp.bfloat16)
        lse_ref[:, 128 * h : 128 * (h + 1)] = jnp.broadcast_to(top + jnp.log(total), (rows, 128))
    part = jnp.dot(o_ref[...], wo_ref[...], preferred_element_type=jnp.float32)

    @pl.when(pl.program_id(0) == 0)
    def _():
        sum_ref[...] = part

    @pl.when(pl.program_id(0) > 0)
    def _():
        sum_ref[...] += part

    @pl.when(pl.program_id(0) == pl.num_programs(0) - 1)
    def _():
        attn_ref[...] = sum_ref[...].astype(jnp.bfloat16)


def whole_block(shape):
    return pl.BlockSpec(shape, lambda i: (0,) * len(shape))


def column_block(shape):
    return pl.BlockSpec(shape, lambda i: (0, i))


def attend(base, x, wq, keys, wup, wo, cos_wide, sin_wide):
    rows, width = x.shape
    heads = wo.shape[0] // VD
    count = keys.shape[0]
    struct = jax.ShapeDtypeStruct
    return pl.pallas_call(
        attend_kernel,
        name="attend",
        grid=(heads // 2,),
        in_specs=[
            pl.BlockSpec(memory_space=pltpu.SMEM),
            whole_block((rows, width)),
            column_block((width, 2 * (NOPE + ROPE))),
            whole_block(keys.shape),
            column_block((R, 2 * (NOPE + VD))),
            pl.BlockSpec((2 * VD, width), lambda i: (i, 0)),
            whole_block(cos_wide.shape),
            whole_block(sin_wide.shape),
        ],
        out_specs=[
            column_block((rows, 512)),
            column_block((count, 512)),
            column_block((rows, 2 * VD)),
            column_block((rows, 256)),
            whole_block((rows, width)),
        ],
        out_shape=[
            struct((rows, heads * 256), jnp.bfloat16),
            struct((count, heads * 256), jnp.bfloat16),
            struct((rows, heads * VD), jnp.bfloat16),
            struct((rows, heads * 128), jnp.float32),
            struct((rows, width), jnp.bfloat16),
        ],
        scratch_shapes=[
            pltpu.VMEM((count // KEY_BLOCK, rows, KEY_BLOCK), jnp.float32),
            pltpu.VMEM((rows, width), jnp.float32),
        ],
        compiler_params=pltpu.CompilerParams(vmem_limit_bytes=48 << 20),
        cost_estimate=pl.CostEstimate(
            flops=7 * 10**9, bytes_accessed=20 << 20, transcendentals=2 << 20
        ),
    )(base, x, wq, keys, wup, wo, cos_wide, sin_wide)


def attend_back_kernel(
    base_ref, q_ref, kv_ref, keys_ref, lse_ref, da_ref, wo_ref, wup_ref, cos_ref, sin_ref,
    dq_ref, dup_ref, dlat_ref, p_ref, dp_ref, dkv_ref, lat_ref, rope_ref, up_ref, acc_ref,
):
    base = base_ref[0]
    rows = q_ref.shape[0]
    blocks = keys_ref.shape[0] // KEY_BLOCK
    factor = (NOPE + ROPE) ** (-0.5)
    step = pl.program_id(0)

    @pl.when(step == 0)
    def _():
        lat_ref[...] = jnp.zeros_like(lat_ref)
        rope_ref[...] = jnp.zeros_like(rope_ref)

    up_ref[...] = jnp.zeros_like(up_ref)
    acc_ref[...] = jnp.zeros_like(acc_ref)
    d_out = dot_nt(da_ref[...], wo_ref[...]).astype(jnp.bfloat16)
    deltas = []
    for h in range(2):
        q_nope = q_ref[:, 256 * h : 256 * h + NOPE]
        q_rope = q_ref[:, 256 * h + NOPE : 256 * h + NOPE + ROPE]
        lse = lse_ref[:, 128 * h : 128 * h + 1]
        d_head = d_out[:, VD * h : VD * (h + 1)]

        def first(k, delta, h=h, q_nope=q_nope, q_rope=q_rope, lse=lse, d_head=d_head):
            at = block_of(k)
            scores = masked_block(q_nope, q_rope, kv_ref, keys_ref, base, k, h)
            probs = jnp.exp(scores - lse)
            d_probs = dot_nt(d_head, kv_ref[at, 256 * h + NOPE : 256 * (h + 1)])
            p_ref[h, k] = probs
            dp_ref[h, k] = d_probs
            dkv_ref[at, 256 * h + NOPE : 256 * (h + 1)] = dot_tn(
                probs.astype(jnp.bfloat16), d_head
            ).astype(jnp.bfloat16)
            both = probs * d_probs
            return delta + both[:, :128] + both[:, 128:]

        delta = lax.fori_loop(0, blocks, first, jnp.zeros((rows, 128), jnp.float32))
        deltas.append(jnp.sum(delta, 1, keepdims=True))

    def second(k, carry):
        at = block_of(k)
        for h in range(2):
            q_nope = q_ref[:, 256 * h : 256 * h + NOPE]
            q_rope = q_ref[:, 256 * h + NOPE : 256 * h + NOPE + ROPE]
            d_scores = (p_ref[h, k] * (dp_ref[h, k] - deltas[h])).astype(jnp.bfloat16)
            acc_ref[:, 256 * h : 256 * h + NOPE] += jnp.dot(
                d_scores, kv_ref[at, 256 * h : 256 * h + NOPE], preferred_element_type=jnp.float32
            )
            acc_ref[:, 256 * h + NOPE : 256 * h + NOPE + ROPE] += jnp.dot(
                d_scores, keys_ref[at, R : R + ROPE], preferred_element_type=jnp.float32
            )
            dkv_ref[at, 256 * h : 256 * h + NOPE] = dot_tn(d_scores, q_nope).astype(jnp.bfloat16)
            rope_ref[at, :] += dot_tn(d_scores, q_rope)
        d_kv = dkv_ref[at, :]
        lat_ref[at, :] += dot_nt(d_kv, wup_ref[...])
        up_ref[...] += dot_tn(keys_ref[at, :R], d_kv)
        return carry

    lax.fori_loop(0, blocks, second, 0)
    pieces = []
    for h in range(2):
        pieces.append(acc_ref[:, 256 * h : 256 * h + NOPE])
        pieces.append(
            turn(
                acc_ref[:, 256 * h + NOPE : 256 * h + NOPE + ROPE], cos_ref[...], -sin_ref[...]
            )
        )
    dq_ref[...] = (jnp.concatenate(pieces, 1) * factor).astype(jnp.bfloat16)
    dup_ref[...] = up_ref[...].astype(jnp.bfloat16)

    @pl.when(step == pl.num_programs(0) - 1)
    def _():
        dlat_ref[:, :R] = lat_ref[...].astype(jnp.bfloat16)
        dlat_ref[:, R:] = rope_ref[...].astype(jnp.bfloat16)


def attend_back(base, q, kv, keys, lse, d_attn, wo, wup, cos_wide, sin_wide):
    rows, width = d_attn.shape
    heads = wo.shape[0] // VD
    count = keys.shape[0]
    blocks = count // KEY_BLOCK
    struct = jax.ShapeDtypeStruct
    square = pltpu.VMEM((2, blocks, rows, KEY_BLOCK), jnp.float32)
    return pl.pallas_call(
        attend_back_kernel,
        name="attend_back",
        grid=(heads // 2,),
        in_specs=[
            pl.BlockSpec(memory_space=pltpu.SMEM),
            column_block((rows, 512)),
            column_block((count, 512)),
            whole_block(keys.shape),
            column_block((rows, 256)),
            whole_block(d_attn.shape),
            pl.BlockSpec((2 * VD, width), lambda i: (i, 0)),
            column_block((R, 2 * (NOPE + VD))),
            whole_block(cos_wide.shape),
            whole_block(sin_wide.shape),
        ],
        out_specs=[
            column_block((rows, 2 * (NOPE + ROPE))),
            column_block((R, 2 * (NOPE + VD))),
            whole_block(keys.shape),
        ],
        out_shape=[
            struct((rows, heads * (NOPE + ROPE)), jnp.bfloat16),
            struct((R, heads * (NOPE + VD)), jnp.bfloat16),
            struct(keys.shape, jnp.bfloat16),
        ],
        scratch_shapes=[
            square,
            square,
            pltpu.VMEM((count, 512), jnp.bfloat16),
            pltpu.VMEM((count, R), jnp.float32),
            pltpu.VMEM((count, ROPE), jnp.float32),
            pltpu.VMEM((R, 512), jnp.float32),
            pltpu.VMEM((rows, 512), jnp.float32),
        ],
        compiler_params=pltpu.CompilerParams(vmem_limit_bytes=56 << 20),
        cost_estimate=pl.CostEstimate(
            flops=10**10, bytes_accessed=20 << 20, transcendentals=2 << 20
        ),
    )(base, q, kv, keys, lse, d_attn, wo, wup, cos_wide, sin_wide)


def kept(shape, **kwargs):
    return pl.BlockSpec(shape, lambda i: (0,) * len(shape), pipeline_mode=pl.Buffered(1), **kwargs)


def expert_kernel(
    experts, first_ref, x_ref, g_ref, route_ref, eg_ref, eu_ref, ed_ref, sg_ref, su_ref, sd_ref,
    act_ref, turned_ref, dx_ref, dw_ref, weight_ref, gate_ref, up_ref, plain_ref, dgu_ref,
):
    local_experts, units, _ = eg_ref.shape
    shared_units = sg_ref.shape[0]
    wide = act_ref.shape[1]
    rows = x_ref.shape[0]
    taken = local_experts * units

    @pl.when(pl.program_id(0) == 0)
    def _():
        for k, (routed, shared) in enumerate(
            ((eg_ref, sg_ref), (eu_ref, su_ref), (ed_ref, sd_ref))
        ):
            start = k * wide
            for e in range(local_experts):
                weight_ref[start + e * units : start + (e + 1) * units, :] = routed[e]
            weight_ref[start + taken : start + taken + shared_units, :] = shared[...]
            weight_ref[start + taken + shared_units : start + wide, :] = jnp.zeros(
                (wide - taken - shared_units, weight_ref.shape[1]), jnp.bfloat16
            )

    plain_ref[...] = dot_nt(g_ref[...], weight_ref[2 * wide :, :])
    gate_ref[...] = dot_nt(x_ref[...], weight_ref[:wide, :])
    up_ref[...] = dot_nt(x_ref[...], weight_ref[wide : 2 * wide, :])
    step = 16

    def piece(k, carry):
        at = pl.ds(pl.multiple_of(k * step, step), step)
        gate, up, plain = gate_ref[at, :], up_ref[at, :], plain_ref[at, :]
        column = lax.broadcasted_iota(jnp.int32, gate.shape, 1)
        lane = lax.broadcasted_iota(jnp.int32, (step, 128), 1)
        routes = route_ref[at, :].astype(jnp.float32)
        scale = jnp.ones(gate.shape, jnp.float32)
        for e in reversed(range(local_experts)):
            mine = lax.rem(lane, experts) == first_ref[0] + e
            weight = jnp.sum(jnp.where(mine, routes, 0.0), 1, keepdims=True)
            scale = jnp.where(column < (e + 1) * units, weight, scale)
        logistic = 1.0 / (1.0 + jnp.exp(-gate))
        silu = gate * logistic
        act = silu * up
        act_ref[at, :] = (act * scale).astype(jnp.bfloat16)
        d_act = plain * scale
        dgu_ref[at, :wide] = (
            d_act * up * logistic * (1.0 + gate * (1.0 - logistic))
        ).astype(jnp.bfloat16)
        dgu_ref[at, wide:] = (d_act * silu).astype(jnp.bfloat16)
        dots = act * plain
        out = jnp.zeros((step, 128), jnp.float32)
        for e in range(local_experts):
            inside = (column >= e * units) & (column < (e + 1) * units)
            total = jnp.sum(jnp.where(inside, dots, 0.0), 1, keepdims=True)
            out = jnp.where(lane == first_ref[0] + e, total, out)
        dw_ref[at, :] = out.astype(jnp.bfloat16)
        return carry

    lax.fori_loop(0, rows // step, piece, 0)
    turned_ref[: 2 * wide, :] = dgu_ref[...].T
    turned_ref[2 * wide :, :] = act_ref[...].T
    dx_ref[...] = jnp.dot(
        dgu_ref[...], weight_ref[: 2 * wide, :], preferred_element_type=jnp.float32
    ).astype(jnp.bfloat16)


def run_experts(experts, first, x, g, route, eg, eu, ed, sg, su, sd):
    tokens, width = x.shape
    local_experts, units, _ = eg.shape
    wide = -(-(local_experts * units + sg.shape[0]) // 128) * 128
    rows = 256
    struct = jax.ShapeDtypeStruct

    def row_block(columns):
        return pl.BlockSpec((rows, columns), lambda i: (i, 0))

    return pl.pallas_call(
        functools.partial(expert_kernel, experts),
        name="experts",
        grid=(tokens // rows,),
        in_specs=[
            pl.BlockSpec(memory_space=pltpu.SMEM),
            row_block(width),
            row_block(width),
            row_block(128),
        ]
        + [kept(one.shape) for one in (eg, eu, ed, sg, su, sd)],
        out_specs=[
            row_block(wide),
            pl.BlockSpec((3 * wide, rows), lambda i: (0, i)),
            row_block(width),
            row_block(128),
        ],
        out_shape=[
            struct((tokens, wide), jnp.bfloat16),
            struct((3 * wide, tokens), jnp.bfloat16),
            struct((tokens, width), jnp.bfloat16),
            struct((tokens, 128), jnp.bfloat16),
        ],
        scratch_shapes=[pltpu.VMEM((3 * wide, width), jnp.bfloat16)]
        + [pltpu.VMEM((rows, wide), jnp.float32)] * 3
        + [pltpu.VMEM((rows, 2 * wide), jnp.bfloat16)],
        compiler_params=pltpu.CompilerParams(vmem_limit_bytes=58 << 20),
        cost_estimate=pl.CostEstimate(
            flops=10 * tokens * width * wide, bytes_accessed=50 << 20, transcendentals=2 << 20
        ),
    )(first, x, g, route, eg, eu, ed, sg, su, sd)


def weight_step(ins, outs, extra):
    x_ref, g_ref, act_ref, turned_ref, ed_ref, sd_ref = ins
    eg_ref, eu_ref, edg_ref, shared_ref, sum_ref = outs
    (wd_ref,) = extra
    local_experts, units, _ = edg_ref.shape
    shared_units = shared_ref.shape[1]
    wide = act_ref.shape[1]
    taken = local_experts * units

    @pl.when(pl.program_id(0) == 0)
    def _():
        wd_ref[...] = jnp.zeros_like(wd_ref)

    def gradient(k, routed, right):
        part = jnp.dot(
            turned_ref[k * wide : (k + 1) * wide, :],
            right[...],
            preferred_element_type=jnp.float32,
        )
        for e in range(local_experts):
            routed[e] = part[e * units : (e + 1) * units].astype(jnp.bfloat16)
        shared_ref[k] = part[taken : taken + shared_units].astype(jnp.bfloat16)

    @pl.when(lax.rem(pl.program_id(0), 2) == 0)
    def _():
        gradient(0, eg_ref, x_ref)
        gradient(1, eu_ref, x_ref)

    @pl.when(lax.rem(pl.program_id(0), 2) == 1)
    def _():
        for e in range(local_experts):
            wd_ref[e * units : (e + 1) * units, :] = ed_ref[e]
        wd_ref[taken : taken + shared_units, :] = sd_ref[...]
        sum_ref[...] = jnp.dot(
            act_ref[...], wd_ref[...], preferred_element_type=jnp.float32
        ).astype(jnp.bfloat16)
        gradient(2, edg_ref, g_ref)


SLOTS = (0, 1, 1, 2, 4, 4, 7, 7, 10, 10, 13, 13, 16)


def run_weights(x, g, act, turned, ed, sd, tasks, collective_id):
    tokens, width = x.shape
    local_experts, units, _ = ed.shape
    shared_units = sd.shape[0]
    wide = act.shape[1]
    columns = 256
    steps = 2 * (width // columns)
    struct = jax.ShapeDtypeStruct

    def column(shape):
        return pl.BlockSpec(shape, lambda i: (0,) * (len(shape) - 1) + (i // 2,))

    ins = [x, g, act, turned, ed, sd]
    in_specs = [
        column((tokens, columns)),
        column((tokens, columns)),
        kept(act.shape),
        kept(turned.shape),
        column((local_experts, units, columns)),
        column((shared_units, columns)),
    ]
    out_specs = [column((local_experts, units, columns))] * 3 + [
        column((3, shared_units, columns)),
        column((tokens, columns)),
    ]
    out_shape = [struct((local_experts, units, width), jnp.bfloat16)] * 3 + [
        struct((3, shared_units, width), jnp.bfloat16),
        struct((tokens, width), jnp.bfloat16),
    ]
    scratch = [pltpu.VMEM((wide, columns), jnp.bfloat16)]
    own = (len(ins), len(out_specs), len(scratch))

    def kernel(*refs):
        refs = list(refs)

        def take(counts):
            return [[refs.pop(0) for _ in range(count)] for count in counts]

        inputs = take([own[0]] + [len(task.inputs) for task in tasks])
        outputs = take([own[1]] + [len(task.outputs) for task in tasks])
        extra = take([own[2]] + [len(task.scratch) for task in tasks])
        running = []
        if tasks:
            place = Place()
            running = [
                task.steps(place, a, b, c)
                for task, a, b, c in zip(tasks, inputs[1:], outputs[1:], extra[1:])
            ]
            for walk in running:
                next(walk)

        def rounds(slot, step):
            @pl.when(pl.program_id(0) == step)
            def _():
                if slot == 0:
                    greet(place)
                for _ in range(SLOTS.count(slot)):
                    for walk in running:
                        next(walk, None)

        if running:
            for slot in sorted(set(SLOTS) - {steps}):
                rounds(slot, slot)
        weight_step(inputs[0], outputs[0], extra[0])
        if running:
            rounds(steps, steps - 1)

    for task in tasks:
        for one in task.inputs:
            ins.append(one)
            in_specs.append(kept(one.shape))
        for one in task.outputs:
            out_shape.append(one)
            out_specs.append(kept(one.shape))
        scratch += task.scratch
    params = {"collective_id": collective_id, "has_side_effects": True} if tasks else {}
    return pl.pallas_call(
        kernel,
        name="weights",
        grid=(steps,),
        in_specs=in_specs,
        out_specs=out_specs,
        out_shape=out_shape,
        scratch_shapes=scratch,
        compiler_params=pltpu.CompilerParams(vmem_limit_bytes=61 << 20, **params),
        cost_estimate=pl.CostEstimate(
            flops=8 * tokens * width * wide, bytes_accessed=60 << 20, transcendentals=0
        ),
    )(*ins)


def shards(
    tokens,
    norm_attn_gain,
    query_weight,
    latent_down,
    latent_gain,
    latent_up,
    out_weight,
    norm_ffn_gain,
    router_weight,
    shared_gate,
    shared_up,
    shared_down,
    expert_gate,
    expert_up,
    expert_down,
    expert_ids,
    out_grad,
):
    tok_rows, model_width = tokens.shape
    head_count = out_weight.shape[0] // VD
    groups = lax.axis_size("dp")
    parts = lax.axis_size("tensor")
    my_group = lax.axis_index("dp")
    my_part = lax.axis_index("tensor")
    stride = groups // SEQ_DEVS
    local_experts, _, units = expert_gate.shape
    experts = local_experts * groups
    rows = tok_rows // parts
    shared_units = shared_gate.shape[1] // groups
    used_units = local_experts * units + shared_units
    spare_units = -used_units % 128
    seq_stretch = my_group // stride
    direct = groups == PLANE and parts == DEPTH

    residual_in = tokens.astype(jnp.float32)
    normed_in, inv_one = rms_forward(residual_in, norm_attn_gain)
    normed_low = low(normed_in)
    query_pos = seq_stretch * tok_rows + jnp.arange(tok_rows)
    cos_table, sin_table = rotation(query_pos)
    factor = (NOPE + ROPE) ** (-0.5)
    compressed = mat_dot(normed_low, latent_down)
    latent_normed, inv_latent = rms_forward(compressed[:, :R], latent_gain)
    key_rope = rotate(compressed[:, R:], cos_table, sin_table)
    own_latent = low(jnp.concatenate([latent_normed, key_rope], -1))
    if direct:
        halves = own_latent.reshape(2, tok_rows // 2, R + ROPE)
        (keys_latent,) = exchange([GatherPlane(halves, False)], 0, "gather_keys")
        keys_latent = keys_latent.reshape(groups * tok_rows, R + ROPE)
        key_pos = jnp.arange(keys_latent.shape[0])
    elif stride == 1:
        keys_latent = gather(own_latent, "dp")
        key_pos = jnp.arange(keys_latent.shape[0])
    else:
        earlier = [
            from_behind(own_latent, "dp", (SEQ_DEVS - 1 - block_index) * stride)
            for block_index in range(SEQ_DEVS - 1)
        ]
        keys_latent = jnp.concatenate(earlier + [own_latent], 0)
        key_pos = (seq_stretch - (SEQ_DEVS - 1)) * tok_rows + jnp.arange(keys_latent.shape[0])
    key_count = keys_latent.shape[0]
    if direct:
        late_grad, keys_latent = lax.optimization_barrier((out_grad, keys_latent))
        grad_all = gather(late_grad, "dp")
    else:
        grad_all = gather(out_grad, "dp")
    query = mat_dot(normed_low, query_weight).reshape(tok_rows, head_count, NOPE + ROPE)
    query = (
        jnp.concatenate(
            [
                query[..., :NOPE],
                rotate(query[..., NOPE:], cos_table[:, None, :], sin_table[:, None, :]),
            ],
            -1,
        )
        * factor
    )
    query_low = low(query)
    expanded = low(mat_dot(keys_latent[:, :R], latent_up)).reshape(
        key_count, head_count, NOPE + VD
    )
    visible = (key_pos[None, :] >= 0) & (key_pos[None, :] <= query_pos[:, None])

    def attention_scores():
        raw_scores = jnp.einsum(
            "qhd,khd->hqk",
            query_low[..., :NOPE],
            expanded[..., :NOPE],
            preferred_element_type=jnp.float32,
        )
        raw_scores = raw_scores + jnp.einsum(
            "qhd,kd->hqk",
            query_low[..., NOPE:],
            keys_latent[:, R:],
            preferred_element_type=jnp.float32,
        )
        return jnp.where(visible[None], raw_scores, masked_score)

    scores = attention_scores()
    top_score = jnp.max(scores, -1, keepdims=True)
    exp_scores = jnp.exp(scores - top_score)
    exp_total = jnp.sum(exp_scores, -1, keepdims=True)
    log_total = top_score + jnp.log(exp_total)
    probs_low = low(exp_scores / exp_total)
    heads_out = jnp.einsum(
        "hqk,khd->qhd", probs_low, expanded[..., NOPE:], preferred_element_type=jnp.float32
    )
    heads_low = low(heads_out.reshape(tok_rows, head_count * VD))
    if direct:
        cos_wide = jnp.concatenate([cos_table, cos_table], 1)
        sin_wide = jnp.concatenate([-sin_table, sin_table], 1)
        first_row = jnp.full((1,), my_group * tok_rows, jnp.int32)
        query_kept, expanded_kept, heads_low, log_kept, attn = attend(
            first_row, normed_low, query_weight, keys_latent, latent_up, out_weight, cos_wide, sin_wide
        )
        (attn,) = exchange(
            [ScatterLevels(attn.reshape(parts, rows, model_width))], 1, "scatter_attn"
        )
    else:
        attn = scatter(mat_dot(heads_low, out_weight), "tensor")

    def own_rows(value):
        return lax.dynamic_slice_in_dim(value, my_part * rows, rows, 0)

    hidden = own_rows(residual_in) + attn
    ffn_in, inv_two = rms_forward(hidden, norm_ffn_gain)
    ffn_low = low(ffn_in)
    router = router_weight.astype(jnp.float32)
    router_gates = jax.nn.sigmoid(
        jnp.dot(ffn_in, router, precision=highest, preferred_element_type=jnp.float32)
    )
    picked = jnp.any(
        own_rows(expert_ids)[..., None] == jnp.arange(experts)[None, None, :], 1
    ).astype(jnp.float32)
    chosen = picked * router_gates
    chosen_sum = jnp.sum(chosen, -1, keepdims=True)
    route = route_scale * chosen / chosen_sum
    route_high = low(route)
    route_rest = low(route - route_high.astype(jnp.float32))
    routes = jnp.concatenate([route_high, route_rest], 1)
    if direct:
        routes = jnp.pad(routes, ((0, 0), (0, 128 - 2 * experts)))
        ffn_all, routes = exchange(
            [GatherPlane(ffn_low, True), GatherPlane(routes, True)], 2, "gather_ffn"
        )
        ffn_all = ffn_all.reshape(-1, model_width)
        routes = routes.reshape(-1, 128)
        token_count = routes.shape[0]
        first_expert = jnp.full((1,), my_group * local_experts, jnp.int32)

        def own_units(value):
            return lax.dynamic_slice_in_dim(value, my_group * shared_units, shared_units, 0)

        shared_own = own_units(shared_gate.T), own_units(shared_up.T), own_units(shared_down)
        act_low, turned, ffn_grad, weight_grad = run_experts(
            experts,
            first_expert,
            ffn_all,
            grad_all,
            routes,
            expert_gate.transpose(0, 2, 1),
            expert_up.transpose(0, 2, 1),
            expert_down,
            *shared_own,
        )
        (
            expert_gate_grad,
            expert_up_grad,
            expert_down_grad,
            shared_grads,
            moe_out,
            ffn_grad,
            weight_grad,
        ) = run_weights(
            ffn_all,
            grad_all,
            act_low,
            turned,
            expert_down,
            shared_own[2],
            [
                ScatterPlane(ffn_grad.reshape(groups, parts, rows, model_width), True),
                ScatterPlane(weight_grad.reshape(groups, parts, rows, 128), True),
            ],
            3,
        )
        expert_gate_grad = expert_gate_grad.transpose(0, 2, 1).astype(jnp.float32)
        expert_up_grad = expert_up_grad.transpose(0, 2, 1).astype(jnp.float32)
        expert_down_grad = expert_down_grad.astype(jnp.float32)
        shared_grads = lax.all_to_all(
            shared_grads, "dp", split_axis=2, concat_axis=1, tiled=True
        )
        weight_grad = weight_grad[:, :experts]
    else:
        ffn_all = gather(jnp.concatenate([ffn_low, routes], 1), BOTH)
        routes = ffn_all[:, model_width:]
        ffn_all = ffn_all[:, :model_width]
        route_all = routes[:, :experts].astype(jnp.float32) + routes[
            :, experts : 2 * experts
        ].astype(jnp.float32)
        token_count = ffn_all.shape[0]
        route_own = lax.dynamic_slice_in_dim(route_all, my_group * local_experts, local_experts, 1)

        def joined(expert_weight, shared_weight):
            own = lax.dynamic_slice_in_dim(shared_weight, my_group * shared_units, shared_units, 1)
            pieces = [expert_weight[e] for e in range(local_experts)]
            return jnp.concatenate(
                pieces + [own, jnp.zeros((model_width, spare_units), jnp.bfloat16)], 1
            )

        gate_weight = joined(expert_gate, shared_gate)
        up_weight = joined(expert_up, shared_up)
        down_weight = jnp.concatenate(
            [expert_down[e] for e in range(local_experts)]
            + [
                lax.dynamic_slice_in_dim(shared_down, my_group * shared_units, shared_units, 0),
                jnp.zeros((spare_units, model_width), jnp.bfloat16),
            ],
            0,
        )
        scale = jnp.concatenate(
            [
                jnp.broadcast_to(route_own[:, e : e + 1], (token_count, units))
                for e in range(local_experts)
            ]
            + [jnp.ones((token_count, shared_units + spare_units), jnp.float32)],
            1,
        )
        plain_grad = contract_cols(grad_all, down_weight)
        gate_act = mat_dot(ffn_all, gate_weight)
        up_act = mat_dot(ffn_all, up_weight)
        logistic = jax.nn.sigmoid(gate_act)
        silu = gate_act * logistic
        act = silu * up_act
        act_low = low(act * scale)
        act_grad = plain_grad * scale
        gate_grad = low(act_grad * up_act * logistic * (1.0 + gate_act * (1.0 - logistic)))
        up_grad = low(act_grad * silu)
        weight_dots = act * plain_grad
        weight_grad = jnp.stack(
            [
                jnp.sum(weight_dots[:, e * units : (e + 1) * units], 1)
                for e in range(local_experts)
            ],
            1,
        )
        weight_grad = lax.dynamic_update_slice_in_dim(
            jnp.zeros((token_count, experts), jnp.bfloat16),
            low(weight_grad),
            my_group * local_experts,
            1,
        )
        ffn_grad = contract_cols(gate_grad, gate_weight) + contract_cols(up_grad, up_weight)
        ffn_grad = scatter(jnp.concatenate([low(ffn_grad), weight_grad], 1), BOTH)
        weight_grad = ffn_grad[:, model_width:]
        ffn_grad = ffn_grad[:, :model_width]
        moe_out = mat_dot(act_low, down_weight)

        down_grad = contract_rows(act_low, grad_all)
        gate_weight_grad = contract_rows(ffn_all, gate_grad)
        up_weight_grad = contract_rows(ffn_all, up_grad)
        expert_down_grad = down_grad[: local_experts * units].reshape(local_experts, units, -1)
        expert_gate_grad = jnp.stack(
            [gate_weight_grad[:, e * units : (e + 1) * units] for e in range(local_experts)]
        )
        expert_up_grad = jnp.stack(
            [up_weight_grad[:, e * units : (e + 1) * units] for e in range(local_experts)]
        )

        def swap(value):
            return lax.all_to_all(low(value), "dp", split_axis=0, concat_axis=1, tiled=True).astype(
                jnp.float32
            )

        first = local_experts * units
        shared_gate_grad = swap(gate_weight_grad[:, first:used_units])
        shared_up_grad = swap(up_weight_grad[:, first:used_units])
        shared_down_grad = lax.all_to_all(
            low(down_grad[first:used_units]), "dp", split_axis=1, concat_axis=0, tiled=True
        ).astype(jnp.float32)

    moe_out = lax.psum_scatter(low(moe_out), "dp", scatter_dimension=0, tiled=True)

    inner_sum = jnp.sum(weight_grad * chosen, -1, keepdims=True)
    chosen_grad = route_scale * (weight_grad / chosen_sum - inner_sum / (chosen_sum * chosen_sum))
    logit_grad = chosen_grad * chosen * (1.0 - chosen)
    router_grad = jnp.dot(
        ffn_in.T, logit_grad, precision=highest, preferred_element_type=jnp.float32
    )
    norm_grad = ffn_grad + jnp.dot(
        logit_grad, router.T, precision=highest, preferred_element_type=jnp.float32
    )
    hidden_extra, norm_ffn_grad = rms_backward(hidden, inv_two, norm_ffn_gain, norm_grad)
    hidden_grad = own_rows(out_grad).astype(jnp.float32) + hidden_extra
    if direct:
        (attn_grad_low,) = exchange([GatherLevels(low(hidden_grad))], 4, "gather_hidden")
        attn_grad_low = attn_grad_low.reshape(tok_rows, model_width)
    else:
        attn_grad_low = gather(low(hidden_grad), "tensor")

    out_weight_grad = scatter(contract_rows(heads_low, attn_grad_low), "dp", 1)
    if direct:
        query_grad_low, latent_up_grad, latent_grad = attend_back(
            first_row,
            query_kept,
            expanded_kept,
            keys_latent,
            log_kept,
            attn_grad_low,
            out_weight,
            latent_up,
            cos_wide,
            sin_wide,
        )
        moe_out, shared_grads, _ = lax.optimization_barrier(
            (moe_out, shared_grads, query_grad_low)
        )
        shared_grads = shared_grads.astype(jnp.float32)
        shared_gate_grad, shared_up_grad = shared_grads[0].T, shared_grads[1].T
        shared_down_grad = shared_grads[2]
    else:
        heads_grad = low(contract_cols(attn_grad_low, out_weight)).reshape(tok_rows, head_count, VD)
        attn_probs = jnp.exp(attention_scores() - log_total)
        probs_low = low(attn_probs)
        value_grad = jnp.einsum(
            "hqk,qhd->khd", probs_low, heads_grad, preferred_element_type=jnp.float32
        )
        prob_grad = jnp.einsum(
            "qhd,khd->hqk", heads_grad, expanded[..., NOPE:], preferred_element_type=jnp.float32
        )
        row_delta = jnp.sum(attn_probs * prob_grad, -1, keepdims=True)
        score_grad = low(attn_probs * (prob_grad - row_delta))
        nope_grad = jnp.einsum(
            "hqk,khd->qhd", score_grad, expanded[..., :NOPE], preferred_element_type=jnp.float32
        )
        rope_grad = jnp.einsum(
            "hqk,kd->qhd", score_grad, keys_latent[:, R:], preferred_element_type=jnp.float32
        )
        key_nope_grad = jnp.einsum(
            "hqk,qhd->khd", score_grad, query_low[..., :NOPE], preferred_element_type=jnp.float32
        )
        key_rope_grad = jnp.einsum(
            "hqk,qhd->kd", score_grad, query_low[..., NOPE:], preferred_element_type=jnp.float32
        )
        expand_grad = low(
            jnp.concatenate([key_nope_grad, value_grad], -1).reshape(
                key_count, head_count * (NOPE + VD)
            )
        )
        latent_up_grad = contract_rows(keys_latent[:, :R], expand_grad)
        latent_grad = jnp.concatenate([contract_cols(expand_grad, latent_up), key_rope_grad], -1)
        query_grad = (
            jnp.concatenate(
                [nope_grad, unrotate(rope_grad, cos_table[:, None, :], sin_table[:, None, :])], -1
            )
            * factor
        )
        query_grad_low = low(query_grad.reshape(tok_rows, head_count * (NOPE + ROPE)))
    block_out = low(hidden + scatter(moe_out, "tensor"))
    query_weight_grad = contract_rows(normed_low, query_grad_low)
    input_part = contract_cols(query_grad_low, query_weight)
    if direct:
        own_grad, input_sum = exchange(
            [
                ScatterPlane(low(latent_grad).reshape(groups, parts, rows, R + ROPE), True),
                ScatterLevels(low(input_part).reshape(parts, rows, model_width)),
            ],
            5,
            "scatter_latent",
        )
    else:
        if stride == 1:
            own_grad = scatter(scatter(latent_grad, "dp"), "tensor")
        else:
            own_grad = latent_grad[(SEQ_DEVS - 1) * tok_rows :]
            for block_index in range(SEQ_DEVS - 1):
                piece_grad = latent_grad[block_index * tok_rows : (block_index + 1) * tok_rows]
                own_grad = own_grad + from_behind(
                    low(piece_grad), "dp", -(SEQ_DEVS - 1 - block_index) * stride
                ).astype(piece_grad.dtype)
            own_grad = scatter(own_grad, "tensor")
        input_sum = scatter(input_part, "tensor")
        query_weight_grad = scatter(query_weight_grad, "dp")
        latent_up_grad = scatter(latent_up_grad, "dp")
    compressed_own = own_rows(compressed)
    normed_part, latent_gain_grad = rms_backward(
        compressed_own[:, :R], own_rows(inv_latent), latent_gain, own_grad[:, :R]
    )
    compressed_grad = low(
        jnp.concatenate(
            [normed_part, unrotate(own_grad[:, R:], own_rows(cos_table), own_rows(sin_table))], -1
        )
    )
    latent_down_grad = contract_rows(own_rows(normed_low), compressed_grad)
    normed_grad = input_sum + contract_cols(compressed_grad, latent_down)
    input_extra, norm_attn_grad = rms_backward(
        own_rows(residual_in), own_rows(inv_one), norm_attn_gain, normed_grad
    )
    tokens_grad = low(hidden_grad + input_extra)
    small = [norm_attn_grad, latent_gain_grad, norm_ffn_grad, router_grad]
    sizes = [one.size // groups for one in small]
    small = jnp.concatenate([one.reshape(groups, -1) for one in small], 1)
    if direct:
        small = jnp.pad(low(small), ((0, 0), (0, parts * 2048 - small.shape[1])))
        (
            latent_down_grad,
            small,
            tokens_grad,
            query_weight_grad,
            latent_up_grad,
            block_out,
        ) = exchange(
            [
                ScatterPlane(
                    low(latent_down_grad).reshape(groups, parts, rows, R + ROPE), True, True
                ),
                ScatterPlane(small.reshape(groups, parts, 16, 128), True, True),
                GatherLevels(tokens_grad),
                ScatterPlane(low(query_weight_grad).reshape(groups, 2, model_width // 16, -1), False),
                ScatterPlane(low(latent_up_grad).reshape(groups, 2, R // 16, -1), False),
                GatherLevels(block_out),
            ],
            6,
            "scatter_last",
        )
        latent_down_grad = latent_down_grad.reshape(-1, R + ROPE).astype(jnp.float32)
        small = small.reshape(-1).astype(jnp.float32)
        query_weight_grad = query_weight_grad.reshape(model_width // groups, -1)
        latent_up_grad = latent_up_grad.reshape(R // groups, -1)
        block_out = block_out.reshape(tok_rows, model_width)
        tokens_grad = tokens_grad.reshape(tok_rows, model_width)
    else:
        latent_down_grad = lax.psum(scatter(latent_down_grad, "dp"), "tensor")
        small = lax.psum(scatter(small, "dp"), "tensor").reshape(-1)
        tokens_grad = gather(tokens_grad, "tensor")
        block_out = gather(block_out, "tensor")
    offsets = [sum(sizes[:k]) for k in range(len(sizes))]
    norm_attn_grad, latent_gain_grad, norm_ffn_grad, router_grad = [
        small[start : start + size] for start, size in zip(offsets, sizes)
    ]

    return (
        block_out,
        tokens_grad,
        norm_attn_grad,
        query_weight_grad,
        latent_down_grad,
        latent_gain_grad,
        latent_up_grad,
        out_weight_grad,
        norm_ffn_grad,
        router_grad.reshape(-1, experts),
        shared_gate_grad,
        shared_up_grad,
        shared_down_grad,
        expert_gate_grad,
        expert_up_grad,
        expert_down_grad,
    )


def solution(mesh):
    in_specs = (
        P("dp", None),
        P(),
        P(None, "tensor"),
        P(),
        P(),
        P(None, "tensor"),
        P("tensor", None),
        P(),
        P(),
        P(None, "tensor"),
        P(None, "tensor"),
        P("tensor", None),
        P("dp", None, "tensor"),
        P("dp", None, "tensor"),
        P("dp", "tensor", None),
        P("dp", None),
        P("dp", None),
    )
    out_specs = (
        P("dp", None),
        P("dp", None),
        P("dp"),
        P("dp", "tensor"),
        P("dp", None),
        P("dp"),
        P("dp", "tensor"),
        P("tensor", "dp"),
        P("dp"),
        P("dp", None),
        P("dp", "tensor"),
        P("dp", "tensor"),
        P("tensor", "dp"),
        P("dp", None, "tensor"),
        P("dp", None, "tensor"),
        P("dp", "tensor", None),
    )
    return jax.shard_map(shards, mesh=mesh, in_specs=in_specs, out_specs=out_specs, check_vma=False)
```

```python
import functools

import jax
import jax.numpy as jnp
from jax import lax
from jax.experimental import pallas as pl
from jax.experimental.pallas import tpu as pltpu
from jax.sharding import PartitionSpec as P

NOPE = 128
ROPE = 64
VD = 128
R = 512
SEQ_DEVS = 8


eps = 1e-06
route_scale = 2.446
rope_base = 50000.0
masked_score = -1e30
highest = lax.Precision.HIGHEST
BOTH = ("dp", "tensor")


def from_behind(value, axis, steps):
    count = lax.axis_size(axis)
    initial, last = (max(0, -steps), min(count, count - steps))
    return lax.ppermute(value, axis, [(source, source + steps) for source in range(initial, last)])


def mat_dot(left, right):
    return jnp.dot(left, right, preferred_element_type=jnp.float32)


def contract_rows(left, right):
    return lax.dot_general(left, right, (((0,), (0,)), ((), ())), preferred_element_type=jnp.float32)


def contract_cols(left, right):
    return lax.dot_general(left, right, (((1,), (1,)), ((), ())), preferred_element_type=jnp.float32)


def rotation(positions):
    half_width = ROPE // 2
    frequency = rope_base ** (-jnp.arange(half_width, dtype=jnp.float32) / half_width)
    angles = positions.astype(jnp.float32)[:, None] * frequency[None, :]
    return (jnp.cos(angles), jnp.sin(angles))


def rotate(values, cos_table, sin_table):
    half_width = values.shape[-1] // 2
    first_half = values[..., :half_width]
    second_half = values[..., half_width:]
    return jnp.concatenate(
        [
            first_half * cos_table - second_half * sin_table,
            second_half * cos_table + first_half * sin_table,
        ],
        -1,
    )


def unrotate(upstream, cos_table, sin_table):
    return rotate(upstream, cos_table, -sin_table)


def rms_forward(values, gain_vec):
    inv_rms = lax.rsqrt(jnp.mean(values * values, axis=-1, keepdims=True) + eps)
    return (values * inv_rms * gain_vec, inv_rms)


def rms_backward(values, inv_rms, gain_vec, upstream):
    scaled = upstream * gain_vec
    inner_mean = jnp.mean(values * scaled, axis=-1, keepdims=True)
    return (
        inv_rms * scaled - values * inv_rms**3 * inner_mean,
        jnp.sum(upstream * values * inv_rms, axis=0),
    )


def low(value):
    return value.astype(jnp.bfloat16)


def gather(value, axes):
    return lax.all_gather(value, axes, tiled=True)


def scatter(value, axes, dimension=0):
    return lax.psum_scatter(
        low(value), axes, scatter_dimension=dimension, tiled=True
    ).astype(jnp.float32)


MESH = pl.DeviceIdType.MESH
PLANE = 8
DEPTH = 4


class Place:
    def __init__(self):
        self.me = lax.axis_index("dp")
        self.z = lax.axis_index("tensor")
        self.core = self.me % 2
        self.chip = self.me // 2
        self.chip_x = self.chip + 1 - 2 * (self.chip % 2)
        self.chip_y = (self.chip + 2) % 4
        self.chip_xy = 3 - self.chip
        self.sibling = self.me + 1 - 2 * self.core
        self.near_x = 2 * self.chip_x + self.core
        self.near_y = 2 * self.chip_y + self.core
        self.across = 2 * self.chip_xy + self.core
        self.levels = [self.z + 1 - 2 * (self.z % 2), (self.z + 2) % 4, 3 - self.z]


def push(src, dst, sems, index, **target):
    send, recv = sems
    return pltpu.make_async_remote_copy(
        src_ref=src,
        dst_ref=dst,
        send_sem=send.at[index],
        recv_sem=recv.at[index],
        device_id=target,
        device_id_type=MESH,
    )


def add_rows(target, sources):
    rows = target.shape[0]
    step = 16

    def one(k, carry):
        at = pl.ds(pl.multiple_of(k * step, step), step)
        acc = sources[0][at, :].astype(jnp.float32)
        for source in sources[1:]:
            acc = acc + source[at, :].astype(jnp.float32)
        target[at, :] = acc.astype(target.dtype)
        return carry

    lax.fori_loop(0, rows // step, one, 0)


def sem_pair(count):
    return [pltpu.SemaphoreType.DMA((count,)), pltpu.SemaphoreType.DMA((count,))]


class GatherPlane:
    def __init__(self, value, with_z):
        self.with_z = with_z
        self.inputs = [value]
        self.units = DEPTH if with_z else value.shape[0]
        rows, width = value.shape[-2:]
        self.in_specs = [pl.BlockSpec(memory_space=pltpu.VMEM)]
        self.outputs = [
            jax.ShapeDtypeStruct((PLANE, self.units, rows, width), value.dtype)
        ]
        self.out_specs = [pl.BlockSpec(memory_space=pl.ANY)]
        self.scratch = (
            sem_pair(7 * self.units)
            + sem_pair(DEPTH - 1)
            + [pltpu.SemaphoreType.DMA((1,))]
        )

    def steps(self, place, inputs, outputs, scratch):
        (x,), (out,) = inputs, outputs
        sems, z_sems, local = scratch[0:2], scratch[2:4], scratch[4]
        me, units = place.me, self.units
        sends = []
        if self.with_z:
            order = [place.z] + place.levels
            keep = pltpu.make_async_copy(x, out.at[me, place.z], local.at[0])
            arrivals = []
            for k, level in enumerate(place.levels):
                copy = push(x, out.at[me, place.z], z_sems, k, tensor=level)
                copy.start()
                sends.append(copy)
                here = out.at[me, level]
                arrivals.append(push(here, here, z_sems, k, tensor=level))
        else:
            order = list(range(units))
            keep = pltpu.make_async_copy(x, out.at[me], local.at[0])
        keep.start()

        def message(p, kind, slot, target, src=None):
            spot = out.at[slot, order[p]]
            return push(spot if src is None else src, spot, sems, 7 * p + kind, dp=target)

        def launch(*args, **kwargs):
            copy = message(*args, **kwargs)
            copy.start()
            sends.append(copy)

        def stage_own(p):
            if self.with_z:
                src = x if p == 0 else None
                if p > 0:
                    arrivals[p - 1].wait_recv()
            else:
                src = x.at[p]
            pair = [(0, place.near_x), (1, place.near_y)]
            for kind, target in pair if p % 2 == 0 else pair[::-1]:
                launch(p, kind, me, target, src)
            launch(p, 3, me, place.sibling, src)

        def stage_near(p):
            def from_x():
                message(p, 0, place.near_x, place.near_x).wait_recv()
                if p % 2 == 0:
                    launch(p, 2, place.near_x, place.near_y)
                launch(p, 4, place.near_x, place.sibling)

            def from_y():
                message(p, 1, place.near_y, place.near_y).wait_recv()
                if p % 2 == 1:
                    launch(p, 2, place.near_y, place.near_x)
                launch(p, 5, place.near_y, place.sibling)

            for part in (from_x, from_y) if p % 2 == 0 else (from_y, from_x):
                part()

        def stage_across(p):
            message(p, 2, place.across, place.near_x).wait_recv()
            launch(p, 6, place.across, place.sibling)

        for p in range(units + 2):
            if p < units:
                stage_own(p)
            yield
            if 0 <= p - 1 < units:
                stage_near(p - 1)
            if 0 <= p - 2 < units:
                stage_across(p - 2)
            yield
        keep.wait()
        base = place.sibling
        for p in range(units):
            for kind, chip in (
                (3, place.chip),
                (4, place.chip_x),
                (5, place.chip_y),
                (6, place.chip_xy),
            ):
                message(p, kind, 2 * chip + 1 - place.core, base).wait_recv()
        for copy in sends:
            copy.wait_send()


class ScatterPlane:
    def __init__(self, value, with_z, spread=False):
        self.with_z, self.spread = with_z, spread
        _, self.units, rows, width = value.shape
        self.inputs = [value.reshape(4, 2, self.units, rows, width)]
        self.in_specs = [pl.BlockSpec(memory_space=pltpu.VMEM)]
        units = self.units
        shape = (rows, width) if with_z else (units, rows, width)
        kind = jnp.float32
        if spread:
            shape, kind = (DEPTH, rows, width), jnp.bfloat16
        self.outputs = [jax.ShapeDtypeStruct(shape, kind)]
        self.out_specs = [pl.BlockSpec(memory_space=pltpu.VMEM)]
        buffer = pltpu.VMEM((units, rows, width), value.dtype)
        self.scratch = (
            sem_pair(4 * units)
            + [pltpu.VMEM((units, 4, rows, width), value.dtype)]
            + [buffer] * 6
        )
        if with_z:
            level = pltpu.VMEM((DEPTH - 1, rows, width), value.dtype)
            self.scratch += sem_pair(DEPTH - 1) + [level] * 2
        if spread:
            self.scratch += sem_pair(DEPTH - 1) + [pltpu.VMEM((rows, width), value.dtype)]

    def steps(self, place, inputs, outputs, scratch):
        (part,), (out,) = inputs, outputs
        sems, beside = scratch[0:2], scratch[2]
        d_send, d_recv, x_send, x_recv, y_send, y_recv = scratch[3:9]
        units, core = self.units, place.core
        other_core = 1 - core
        if self.with_z:
            z_sems, z_send, z_recv = scratch[9:11], scratch[11], scratch[12]
            near, far, other = place.levels
            order = [far, other, near, place.z]
        else:
            order = list(range(units))
        sends = []

        def launch(make, p):
            make(p).start()
            sends.append((make, p))

        def across(p):
            target = place.near_x if p % 2 == 0 else place.near_y
            return push(d_send.at[p], d_recv.at[p], sems, 4 * p + 1, dp=target)

        def to_x(p):
            return push(x_send.at[p], x_recv.at[p], sems, 4 * p + 2, dp=place.near_x)

        def to_y(p):
            return push(y_send.at[p], y_recv.at[p], sems, 4 * p + 3, dp=place.near_y)

        def to_sibling(p):
            return push(
                part.at[:, other_core, order[p]],
                beside.at[p],
                sems,
                4 * p,
                dp=place.sibling,
            )

        def both(p, chip):
            return [part.at[chip, core, order[p]], beside.at[p, chip]]

        def stage_one(p):
            to_sibling(p).wait_recv()
            add_rows(d_send.at[p], both(p, place.chip_xy))
            launch(across, p)
            if p % 2 == 0:
                add_rows(x_send.at[p], both(p, place.chip_x))
                launch(to_x, p)
            else:
                add_rows(y_send.at[p], both(p, place.chip_y))
                launch(to_y, p)

        def stage_two(p):
            across(p).wait_recv()
            if p % 2 == 0:
                add_rows(y_send.at[p], both(p, place.chip_y) + [d_recv.at[p]])
                launch(to_y, p)
            else:
                add_rows(x_send.at[p], both(p, place.chip_x) + [d_recv.at[p]])
                launch(to_x, p)

        def to_level(p):
            return push(z_send.at[p], z_recv.at[p], z_sems, p, tensor=order[p])

        def stage_three(p):
            to_x(p).wait_recv()
            to_y(p).wait_recv()
            pieces = both(p, place.chip) + [x_recv.at[p], y_recv.at[p]]
            if not self.with_z:
                add_rows(out.at[p], pieces)
            elif p < units - 1:
                add_rows(z_send.at[p], pieces)
                launch(to_level, p)
            else:
                for k in range(DEPTH - 1):
                    to_level(k).wait_recv()
                pieces += [z_recv.at[k] for k in range(DEPTH - 1)]
                add_rows(scratch[15] if self.spread else out, pieces)

        yield
        for p in range(units):
            launch(to_sibling, p)
        yield
        for p in range(units + 2):
            if p < units:
                stage_one(p)
            yield
            if 0 <= p - 1 < units:
                stage_two(p - 1)
            if 0 <= p - 2 < units:
                stage_three(p - 2)
            if p < units + 1:
                yield
        if self.spread:
            copies = []
            yield from spread_levels(place, scratch[15], out, scratch[13:15], copies)
            for copy in copies:
                copy.wait_send()
        for make, p in sends:
            make(p).wait_send()


def spread_levels(place, own, out, z_sems, sends):
    arrivals = []
    for k, level in enumerate(place.levels):
        copy = push(own, out.at[place.z], z_sems, k, tensor=level)
        copy.start()
        sends.append(copy)
        arrivals.append(push(own, out.at[level], z_sems, k, tensor=level))
    out[place.z] = own[...]
    yield
    for copy in arrivals:
        copy.wait_recv()


class GatherLevels:
    def __init__(self, value):
        self.inputs = [value]
        self.in_specs = [pl.BlockSpec(memory_space=pltpu.VMEM)]
        self.outputs = [jax.ShapeDtypeStruct((DEPTH,) + value.shape, value.dtype)]
        self.out_specs = [pl.BlockSpec(memory_space=pltpu.VMEM)]
        self.scratch = sem_pair(DEPTH - 1)

    def steps(self, place, inputs, outputs, scratch):
        sends = []
        yield from spread_levels(place, inputs[0], outputs[0], scratch[0:2], sends)
        for copy in sends:
            copy.wait_send()


class ScatterLevels:
    def __init__(self, value):
        _, rows, width = value.shape
        self.inputs = [value]
        self.in_specs = [pl.BlockSpec(memory_space=pltpu.VMEM)]
        self.outputs = [jax.ShapeDtypeStruct((rows, width), jnp.float32)]
        self.out_specs = [pl.BlockSpec(memory_space=pltpu.VMEM)]
        self.scratch = sem_pair(DEPTH - 1) + [pltpu.VMEM((DEPTH - 1, rows, width), value.dtype)]

    def steps(self, place, inputs, outputs, scratch):
        part, z_sems, landed = inputs[0], scratch[0:2], scratch[2]
        copies = [
            push(part.at[level], landed.at[k], z_sems, k, tensor=level)
            for k, level in enumerate(place.levels)
        ]
        for copy in copies:
            copy.start()
        yield
        yield
        yield
        for copy in copies:
            copy.wait_recv()
        add_rows(outputs[0], [part.at[place.z]] + [landed.at[k] for k in range(DEPTH - 1)])
        for copy in copies:
            copy.wait_send()


def greet(place):
    barrier = pltpu.get_barrier_semaphore()
    for target in (place.sibling, place.near_x, place.near_y):
        pl.semaphore_signal(barrier, inc=1, device_id={"dp": target}, device_id_type=MESH)
    for target in place.levels:
        pl.semaphore_signal(barrier, inc=1, device_id={"tensor": target}, device_id_type=MESH)
    pl.semaphore_wait(barrier, 6)


def held_back(walk, rounds):
    for _ in range(rounds):
        yield
    yield from walk


def exchange(tasks, collective_id, name, waits=None):
    waits = waits or [0] * len(tasks)

    def kernel(*refs):
        place = Place()
        greet(place)
        refs = list(refs)

        def take(counts):
            return [[refs.pop(0) for _ in range(count)] for count in counts]

        inputs = take([len(task.inputs) for task in tasks])
        outputs = take([len(task.outputs) for task in tasks])
        scratch = take([len(task.scratch) for task in tasks])
        running = [
            held_back(task.steps(place, a, b, c), wait)
            for task, a, b, c, wait in zip(tasks, inputs, outputs, scratch, waits)
        ]
        while running:
            for walk in list(running):
                if next(walk, running) is running:
                    running.remove(walk)

    def flat(pieces):
        return [one for piece in pieces for one in piece]

    moved = sum(one.size * one.dtype.itemsize for task in tasks for one in task.inputs)
    return pl.pallas_call(
        kernel,
        name=name,
        out_shape=flat(task.outputs for task in tasks),
        in_specs=flat(task.in_specs for task in tasks),
        out_specs=flat(task.out_specs for task in tasks),
        scratch_shapes=flat(task.scratch for task in tasks),
        compiler_params=pltpu.CompilerParams(
            collective_id=collective_id, has_side_effects=True, vmem_limit_bytes=56 << 20
        ),
        cost_estimate=pl.CostEstimate(flops=0, bytes_accessed=4 * moved, transcendentals=0),
    )(*flat(task.inputs for task in tasks))


KEY_BLOCK = 256


def dot_nt(left, right):
    return lax.dot_general(left, right, (((1,), (1,)), ((), ())), preferred_element_type=jnp.float32)


def dot_tn(left, right):
    return lax.dot_general(left, right, (((0,), (0,)), ((), ())), preferred_element_type=jnp.float32)


def turn(values, cos_wide, sin_wide):
    half = values.shape[1] // 2
    swapped = jnp.concatenate([values[:, half:], values[:, :half]], 1)
    return values * cos_wide + swapped * sin_wide


def block_of(k):
    return pl.ds(pl.multiple_of(k * KEY_BLOCK, KEY_BLOCK), KEY_BLOCK)


def masked_block(q_nope, q_rope, kv_ref, keys_ref, base, k, h):
    at = block_of(k)
    wide = NOPE + VD
    scores = dot_nt(q_nope, kv_ref[at, wide * h : wide * h + NOPE])
    scores = scores + dot_nt(q_rope, keys_ref[at, R : R + ROPE])
    key_pos = k * KEY_BLOCK + lax.broadcasted_iota(jnp.int32, scores.shape, 1)
    query_pos = base + lax.broadcasted_iota(jnp.int32, scores.shape, 0)
    return jnp.where(key_pos <= query_pos, scores, masked_score)


def attend_kernel(
    base_ref, x_ref, wq_ref, keys_ref, wup_ref, wo_ref, cos_ref, sin_ref,
    q_ref, kv_ref, o_ref, lse_ref, attn_ref, s_ref, sum_ref,
):
    base = base_ref[0]
    rows = x_ref.shape[0]
    blocks = keys_ref.shape[0] // KEY_BLOCK
    factor = (NOPE + ROPE) ** (-0.5)
    query = jnp.dot(x_ref[...], wq_ref[...], preferred_element_type=jnp.float32) * factor

    def expand(k, carry):
        at = block_of(k)
        kv_ref[at, :] = jnp.dot(
            keys_ref[at, :R], wup_ref[...], preferred_element_type=jnp.float32
        ).astype(jnp.bfloat16)
        return carry

    lax.fori_loop(0, blocks, expand, 0)
    for h in range(2):
        start = h * (NOPE + ROPE)
        q_nope = query[:, start : start + NOPE].astype(jnp.bfloat16)
        q_rope = turn(
            query[:, start + NOPE : start + NOPE + ROPE], cos_ref[...], sin_ref[...]
        ).astype(jnp.bfloat16)
        q_ref[:, 256 * h : 256 * h + NOPE] = q_nope
        q_ref[:, 256 * h + NOPE : 256 * h + NOPE + ROPE] = q_rope
        q_ref[:, 256 * h + NOPE + ROPE : 256 * (h + 1)] = jnp.zeros(
            (rows, 256 - NOPE - ROPE), jnp.bfloat16
        )

        def first(k, top, h=h, q_nope=q_nope, q_rope=q_rope):
            scores = masked_block(q_nope, q_rope, kv_ref, keys_ref, base, k, h)
            s_ref[k] = scores
            return jnp.maximum(top, jnp.maximum(scores[:, :128], scores[:, 128:]))

        top = lax.fori_loop(0, blocks, first, jnp.full((rows, 128), masked_score, jnp.float32))
        top = jnp.max(top, 1, keepdims=True)

        def second(k, carry, h=h, top=top):
            total, acc = carry
            weights = jnp.exp(s_ref[k] - top)
            total = total + weights[:, :128] + weights[:, 128:]
            value = kv_ref[block_of(k), 256 * h + NOPE : 256 * (h + 1)]
            acc = acc + jnp.dot(
                weights.astype(jnp.bfloat16), value, preferred_element_type=jnp.float32
            )
            return total, acc

        zero = jnp.zeros((rows, 128), jnp.float32)
        total, acc = lax.fori_loop(0, blocks, second, (zero, zero))
        total = jnp.sum(total, 1, keepdims=True)
        o_ref[:, VD * h : VD * (h + 1)] = (acc / total).astype(jnp.bfloat16)
        lse_ref[:, 128 * h : 128 * (h + 1)] = jnp.broadcast_to(top + jnp.log(total), (rows, 128))
    part = jnp.dot(o_ref[...], wo_ref[...], preferred_element_type=jnp.float32)

    @pl.when(pl.program_id(0) == 0)
    def _():
        sum_ref[...] = part

    @pl.when(pl.program_id(0) > 0)
    def _():
        sum_ref[...] += part

    @pl.when(pl.program_id(0) == pl.num_programs(0) - 1)
    def _():
        attn_ref[...] = sum_ref[...].astype(jnp.bfloat16)


def whole_block(shape):
    return pl.BlockSpec(shape, lambda i: (0,) * len(shape))


def column_block(shape):
    return pl.BlockSpec(shape, lambda i: (0, i))


def attend(base, x, wq, keys, wup, wo, cos_wide, sin_wide):
    rows, width = x.shape
    heads = wo.shape[0] // VD
    count = keys.shape[0]
    struct = jax.ShapeDtypeStruct
    return pl.pallas_call(
        attend_kernel,
        name="attend",
        grid=(heads // 2,),
        in_specs=[
            pl.BlockSpec(memory_space=pltpu.SMEM),
            whole_block((rows, width)),
            column_block((width, 2 * (NOPE + ROPE))),
            whole_block(keys.shape),
            column_block((R, 2 * (NOPE + VD))),
            pl.BlockSpec((2 * VD, width), lambda i: (i, 0)),
            whole_block(cos_wide.shape),
            whole_block(sin_wide.shape),
        ],
        out_specs=[
            column_block((rows, 512)),
            column_block((count, 512)),
            column_block((rows, 2 * VD)),
            column_block((rows, 256)),
            whole_block((rows, width)),
        ],
        out_shape=[
            struct((rows, heads * 256), jnp.bfloat16),
            struct((count, heads * 256), jnp.bfloat16),
            struct((rows, heads * VD), jnp.bfloat16),
            struct((rows, heads * 128), jnp.float32),
            struct((rows, width), jnp.bfloat16),
        ],
        scratch_shapes=[
            pltpu.VMEM((count // KEY_BLOCK, rows, KEY_BLOCK), jnp.float32),
            pltpu.VMEM((rows, width), jnp.float32),
        ],
        compiler_params=pltpu.CompilerParams(vmem_limit_bytes=48 << 20),
        cost_estimate=pl.CostEstimate(
            flops=7 * 10**9, bytes_accessed=20 << 20, transcendentals=2 << 20
        ),
    )(base, x, wq, keys, wup, wo, cos_wide, sin_wide)


def attend_back_kernel(
    base_ref, q_ref, kv_ref, keys_ref, lse_ref, da_ref, wo_ref, wup_ref, cos_ref, sin_ref,
    dq_ref, dup_ref, dlat_ref, p_ref, dp_ref, dkv_ref, lat_ref, rope_ref, up_ref, acc_ref,
):
    base = base_ref[0]
    rows = q_ref.shape[0]
    blocks = keys_ref.shape[0] // KEY_BLOCK
    factor = (NOPE + ROPE) ** (-0.5)
    step = pl.program_id(0)

    @pl.when(step == 0)
    def _():
        lat_ref[...] = jnp.zeros_like(lat_ref)
        rope_ref[...] = jnp.zeros_like(rope_ref)

    up_ref[...] = jnp.zeros_like(up_ref)
    acc_ref[...] = jnp.zeros_like(acc_ref)
    d_out = dot_nt(da_ref[...], wo_ref[...]).astype(jnp.bfloat16)
    deltas = []
    for h in range(2):
        q_nope = q_ref[:, 256 * h : 256 * h + NOPE]
        q_rope = q_ref[:, 256 * h + NOPE : 256 * h + NOPE + ROPE]
        lse = lse_ref[:, 128 * h : 128 * h + 1]
        d_head = d_out[:, VD * h : VD * (h + 1)]

        def first(k, delta, h=h, q_nope=q_nope, q_rope=q_rope, lse=lse, d_head=d_head):
            at = block_of(k)
            scores = masked_block(q_nope, q_rope, kv_ref, keys_ref, base, k, h)
            probs = jnp.exp(scores - lse)
            d_probs = dot_nt(d_head, kv_ref[at, 256 * h + NOPE : 256 * (h + 1)])
            p_ref[h, k] = probs
            dp_ref[h, k] = d_probs
            dkv_ref[at, 256 * h + NOPE : 256 * (h + 1)] = dot_tn(
                probs.astype(jnp.bfloat16), d_head
            ).astype(jnp.bfloat16)
            both = probs * d_probs
            return delta + both[:, :128] + both[:, 128:]

        delta = lax.fori_loop(0, blocks, first, jnp.zeros((rows, 128), jnp.float32))
        deltas.append(jnp.sum(delta, 1, keepdims=True))

    def second(k, carry):
        at = block_of(k)
        for h in range(2):
            q_nope = q_ref[:, 256 * h : 256 * h + NOPE]
            q_rope = q_ref[:, 256 * h + NOPE : 256 * h + NOPE + ROPE]
            d_scores = (p_ref[h, k] * (dp_ref[h, k] - deltas[h])).astype(jnp.bfloat16)
            acc_ref[:, 256 * h : 256 * h + NOPE] += jnp.dot(
                d_scores, kv_ref[at, 256 * h : 256 * h + NOPE], preferred_element_type=jnp.float32
            )
            acc_ref[:, 256 * h + NOPE : 256 * h + NOPE + ROPE] += jnp.dot(
                d_scores, keys_ref[at, R : R + ROPE], preferred_element_type=jnp.float32
            )
            dkv_ref[at, 256 * h : 256 * h + NOPE] = dot_tn(d_scores, q_nope).astype(jnp.bfloat16)
            rope_ref[at, :] += dot_tn(d_scores, q_rope)
        d_kv = dkv_ref[at, :]
        lat_ref[at, :] += dot_nt(d_kv, wup_ref[...])
        up_ref[...] += dot_tn(keys_ref[at, :R], d_kv)
        return carry

    lax.fori_loop(0, blocks, second, 0)
    pieces = []
    for h in range(2):
        pieces.append(acc_ref[:, 256 * h : 256 * h + NOPE])
        pieces.append(
            turn(
                acc_ref[:, 256 * h + NOPE : 256 * h + NOPE + ROPE], cos_ref[...], -sin_ref[...]
            )
        )
    dq_ref[...] = (jnp.concatenate(pieces, 1) * factor).astype(jnp.bfloat16)
    dup_ref[...] = up_ref[...].astype(jnp.bfloat16)

    @pl.when(step == pl.num_programs(0) - 1)
    def _():
        dlat_ref[:, :R] = lat_ref[...].astype(jnp.bfloat16)
        dlat_ref[:, R:] = rope_ref[...].astype(jnp.bfloat16)


def attend_back(base, q, kv, keys, lse, d_attn, wo, wup, cos_wide, sin_wide):
    rows, width = d_attn.shape
    heads = wo.shape[0] // VD
    count = keys.shape[0]
    blocks = count // KEY_BLOCK
    struct = jax.ShapeDtypeStruct
    square = pltpu.VMEM((2, blocks, rows, KEY_BLOCK), jnp.float32)
    return pl.pallas_call(
        attend_back_kernel,
        name="attend_back",
        grid=(heads // 2,),
        in_specs=[
            pl.BlockSpec(memory_space=pltpu.SMEM),
            column_block((rows, 512)),
            column_block((count, 512)),
            whole_block(keys.shape),
            column_block((rows, 256)),
            whole_block(d_attn.shape),
            pl.BlockSpec((2 * VD, width), lambda i: (i, 0)),
            column_block((R, 2 * (NOPE + VD))),
            whole_block(cos_wide.shape),
            whole_block(sin_wide.shape),
        ],
        out_specs=[
            column_block((rows, 2 * (NOPE + ROPE))),
            column_block((R, 2 * (NOPE + VD))),
            whole_block(keys.shape),
        ],
        out_shape=[
            struct((rows, heads * (NOPE + ROPE)), jnp.bfloat16),
            struct((R, heads * (NOPE + VD)), jnp.bfloat16),
            struct(keys.shape, jnp.bfloat16),
        ],
        scratch_shapes=[
            square,
            square,
            pltpu.VMEM((count, 512), jnp.bfloat16),
            pltpu.VMEM((count, R), jnp.float32),
            pltpu.VMEM((count, ROPE), jnp.float32),
            pltpu.VMEM((R, 512), jnp.float32),
            pltpu.VMEM((rows, 512), jnp.float32),
        ],
        compiler_params=pltpu.CompilerParams(vmem_limit_bytes=56 << 20),
        cost_estimate=pl.CostEstimate(
            flops=10**10, bytes_accessed=20 << 20, transcendentals=2 << 20
        ),
    )(base, q, kv, keys, lse, d_attn, wo, wup, cos_wide, sin_wide)


def kept(shape, **kwargs):
    return pl.BlockSpec(shape, lambda i: (0,) * len(shape), pipeline_mode=pl.Buffered(1), **kwargs)


def expert_kernel(
    experts, first_ref, x_ref, g_ref, route_ref, eg_ref, eu_ref, ed_ref, sg_ref, su_ref, sd_ref,
    act_ref, turned_ref, dx_ref, dw_ref, weight_ref, gate_ref, up_ref, plain_ref, dgu_ref,
):
    local_experts, units, _ = eg_ref.shape
    shared_units = sg_ref.shape[0]
    wide = act_ref.shape[1]
    rows = x_ref.shape[0]
    taken = local_experts * units

    @pl.when(pl.program_id(0) == 0)
    def _():
        for k, (routed, shared) in enumerate(
            ((eg_ref, sg_ref), (eu_ref, su_ref), (ed_ref, sd_ref))
        ):
            start = k * wide
            for e in range(local_experts):
                weight_ref[start + e * units : start + (e + 1) * units, :] = routed[e]
            weight_ref[start + taken : start + taken + shared_units, :] = shared[...]
            weight_ref[start + taken + shared_units : start + wide, :] = jnp.zeros(
                (wide - taken - shared_units, weight_ref.shape[1]), jnp.bfloat16
            )

    plain_ref[...] = dot_nt(g_ref[...], weight_ref[2 * wide :, :])
    gate_ref[...] = dot_nt(x_ref[...], weight_ref[:wide, :])
    up_ref[...] = dot_nt(x_ref[...], weight_ref[wide : 2 * wide, :])
    step = 16

    def piece(k, carry):
        at = pl.ds(pl.multiple_of(k * step, step), step)
        gate, up, plain = gate_ref[at, :], up_ref[at, :], plain_ref[at, :]
        column = lax.broadcasted_iota(jnp.int32, gate.shape, 1)
        lane = lax.broadcasted_iota(jnp.int32, (step, 128), 1)
        routes = route_ref[at, :].astype(jnp.float32)
        scale = jnp.ones(gate.shape, jnp.float32)
        for e in reversed(range(local_experts)):
            mine = lax.rem(lane, experts) == first_ref[0] + e
            weight = jnp.sum(jnp.where(mine, routes, 0.0), 1, keepdims=True)
            scale = jnp.where(column < (e + 1) * units, weight, scale)
        logistic = 1.0 / (1.0 + jnp.exp(-gate))
        silu = gate * logistic
        act = silu * up
        act_ref[at, :] = (act * scale).astype(jnp.bfloat16)
        d_act = plain * scale
        dgu_ref[at, :wide] = (
            d_act * up * logistic * (1.0 + gate * (1.0 - logistic))
        ).astype(jnp.bfloat16)
        dgu_ref[at, wide:] = (d_act * silu).astype(jnp.bfloat16)
        dots = act * plain
        out = jnp.zeros((step, 128), jnp.float32)
        for e in range(local_experts):
            inside = (column >= e * units) & (column < (e + 1) * units)
            total = jnp.sum(jnp.where(inside, dots, 0.0), 1, keepdims=True)
            out = jnp.where(lane == first_ref[0] + e, total, out)
        dw_ref[at, :] = out.astype(jnp.bfloat16)
        return carry

    lax.fori_loop(0, rows // step, piece, 0)
    turned_ref[: 2 * wide, :] = dgu_ref[...].T
    turned_ref[2 * wide :, :] = act_ref[...].T
    dx_ref[...] = jnp.dot(
        dgu_ref[...], weight_ref[: 2 * wide, :], preferred_element_type=jnp.float32
    ).astype(jnp.bfloat16)


def run_experts(experts, first, x, g, route, eg, eu, ed, sg, su, sd):
    tokens, width = x.shape
    local_experts, units, _ = eg.shape
    wide = -(-(local_experts * units + sg.shape[0]) // 128) * 128
    rows = 256
    struct = jax.ShapeDtypeStruct

    def row_block(columns):
        return pl.BlockSpec((rows, columns), lambda i: (i, 0))

    return pl.pallas_call(
        functools.partial(expert_kernel, experts),
        name="experts",
        grid=(tokens // rows,),
        in_specs=[
            pl.BlockSpec(memory_space=pltpu.SMEM),
            row_block(width),
            row_block(width),
            row_block(128),
        ]
        + [kept(one.shape) for one in (eg, eu, ed, sg, su, sd)],
        out_specs=[
            row_block(wide),
            pl.BlockSpec((3 * wide, rows), lambda i: (0, i)),
            row_block(width),
            row_block(128),
        ],
        out_shape=[
            struct((tokens, wide), jnp.bfloat16),
            struct((3 * wide, tokens), jnp.bfloat16),
            struct((tokens, width), jnp.bfloat16),
            struct((tokens, 128), jnp.bfloat16),
        ],
        scratch_shapes=[pltpu.VMEM((3 * wide, width), jnp.bfloat16)]
        + [pltpu.VMEM((rows, wide), jnp.float32)] * 3
        + [pltpu.VMEM((rows, 2 * wide), jnp.bfloat16)],
        compiler_params=pltpu.CompilerParams(vmem_limit_bytes=58 << 20),
        cost_estimate=pl.CostEstimate(
            flops=10 * tokens * width * wide, bytes_accessed=50 << 20, transcendentals=2 << 20
        ),
    )(first, x, g, route, eg, eu, ed, sg, su, sd)


def weight_step(ins, outs, extra):
    x_ref, g_ref, act_ref, turned_ref, ed_ref, sd_ref = ins
    eg_ref, eu_ref, edg_ref, shared_ref, sum_ref = outs
    (wd_ref,) = extra
    local_experts, units, _ = edg_ref.shape
    shared_units = shared_ref.shape[1]
    wide = act_ref.shape[1]
    taken = local_experts * units

    @pl.when(pl.program_id(0) == 0)
    def _():
        wd_ref[...] = jnp.zeros_like(wd_ref)

    def gradient(k, routed, right):
        part = jnp.dot(
            turned_ref[k * wide : (k + 1) * wide, :],
            right[...],
            preferred_element_type=jnp.float32,
        )
        for e in range(local_experts):
            routed[e] = part[e * units : (e + 1) * units].astype(jnp.bfloat16)
        shared_ref[k] = part[taken : taken + shared_units].astype(jnp.bfloat16)

    @pl.when(lax.rem(pl.program_id(0), 2) == 0)
    def _():
        gradient(0, eg_ref, x_ref)
        gradient(1, eu_ref, x_ref)

    @pl.when(lax.rem(pl.program_id(0), 2) == 1)
    def _():
        for e in range(local_experts):
            wd_ref[e * units : (e + 1) * units, :] = ed_ref[e]
        wd_ref[taken : taken + shared_units, :] = sd_ref[...]
        sum_ref[...] = jnp.dot(
            act_ref[...], wd_ref[...], preferred_element_type=jnp.float32
        ).astype(jnp.bfloat16)
        gradient(2, edg_ref, g_ref)


SLOTS = (0, 1, 1, 2, 4, 4, 7, 7, 10, 10, 13, 13, 16)


def run_weights(x, g, act, turned, ed, sd, tasks, collective_id):
    tokens, width = x.shape
    local_experts, units, _ = ed.shape
    shared_units = sd.shape[0]
    wide = act.shape[1]
    columns = 256
    steps = 2 * (width // columns)
    struct = jax.ShapeDtypeStruct

    def column(shape):
        return pl.BlockSpec(shape, lambda i: (0,) * (len(shape) - 1) + (i // 2,))

    ins = [x, g, act, turned, ed, sd]
    in_specs = [
        column((tokens, columns)),
        column((tokens, columns)),
        kept(act.shape),
        kept(turned.shape),
        column((local_experts, units, columns)),
        column((shared_units, columns)),
    ]
    out_specs = [column((local_experts, units, columns))] * 3 + [
        column((3, shared_units, columns)),
        column((tokens, columns)),
    ]
    out_shape = [struct((local_experts, units, width), jnp.bfloat16)] * 3 + [
        struct((3, shared_units, width), jnp.bfloat16),
        struct((tokens, width), jnp.bfloat16),
    ]
    scratch = [pltpu.VMEM((wide, columns), jnp.bfloat16)]
    own = (len(ins), len(out_specs), len(scratch))

    def kernel(*refs):
        refs = list(refs)

        def take(counts):
            return [[refs.pop(0) for _ in range(count)] for count in counts]

        inputs = take([own[0]] + [len(task.inputs) for task in tasks])
        outputs = take([own[1]] + [len(task.outputs) for task in tasks])
        extra = take([own[2]] + [len(task.scratch) for task in tasks])
        running = []
        if tasks:
            place = Place()
            running = [
                task.steps(place, a, b, c)
                for task, a, b, c in zip(tasks, inputs[1:], outputs[1:], extra[1:])
            ]
            for walk in running:
                next(walk)

        def rounds(slot, step):
            @pl.when(pl.program_id(0) == step)
            def _():
                if slot == 0:
                    greet(place)
                for _ in range(SLOTS.count(slot)):
                    for walk in running:
                        next(walk, None)

        if running:
            for slot in sorted(set(SLOTS) - {steps}):
                rounds(slot, slot)
        weight_step(inputs[0], outputs[0], extra[0])
        if running:
            rounds(steps, steps - 1)

    for task in tasks:
        for one in task.inputs:
            ins.append(one)
            in_specs.append(kept(one.shape))
        for one in task.outputs:
            out_shape.append(one)
            out_specs.append(kept(one.shape))
        scratch += task.scratch
    params = {"collective_id": collective_id, "has_side_effects": True} if tasks else {}
    return pl.pallas_call(
        kernel,
        name="weights",
        grid=(steps,),
        in_specs=in_specs,
        out_specs=out_specs,
        out_shape=out_shape,
        scratch_shapes=scratch,
        compiler_params=pltpu.CompilerParams(vmem_limit_bytes=61 << 20, **params),
        cost_estimate=pl.CostEstimate(
            flops=8 * tokens * width * wide, bytes_accessed=60 << 20, transcendentals=0
        ),
    )(*ins)


def shards(
    tokens,
    norm_attn_gain,
    query_weight,
    latent_down,
    latent_gain,
    latent_up,
    out_weight,
    norm_ffn_gain,
    router_weight,
    shared_gate,
    shared_up,
    shared_down,
    expert_gate,
    expert_up,
    expert_down,
    expert_ids,
    out_grad,
):
    tok_rows, model_width = tokens.shape
    head_count = out_weight.shape[0] // VD
    groups = lax.axis_size("dp")
    parts = lax.axis_size("tensor")
    my_group = lax.axis_index("dp")
    my_part = lax.axis_index("tensor")
    stride = groups // SEQ_DEVS
    local_experts, _, units = expert_gate.shape
    experts = local_experts * groups
    rows = tok_rows // parts
    shared_units = shared_gate.shape[1] // groups
    used_units = local_experts * units + shared_units
    spare_units = -used_units % 128
    seq_stretch = my_group // stride
    direct = groups == PLANE and parts == DEPTH

    residual_in = tokens.astype(jnp.float32)
    normed_in, inv_one = rms_forward(residual_in, norm_attn_gain)
    normed_low = low(normed_in)
    query_pos = seq_stretch * tok_rows + jnp.arange(tok_rows)
    cos_table, sin_table = rotation(query_pos)
    factor = (NOPE + ROPE) ** (-0.5)
    compressed = mat_dot(normed_low, latent_down)
    latent_normed, inv_latent = rms_forward(compressed[:, :R], latent_gain)
    key_rope = rotate(compressed[:, R:], cos_table, sin_table)
    own_latent = low(jnp.concatenate([latent_normed, key_rope], -1))
    if direct:
        halves = own_latent.reshape(2, tok_rows // 2, R + ROPE)
        (keys_latent,) = exchange([GatherPlane(halves, False)], 0, "gather_keys")
        keys_latent = keys_latent.reshape(groups * tok_rows, R + ROPE)
        key_pos = jnp.arange(keys_latent.shape[0])
    elif stride == 1:
        keys_latent = gather(own_latent, "dp")
        key_pos = jnp.arange(keys_latent.shape[0])
    else:
        earlier = [
            from_behind(own_latent, "dp", (SEQ_DEVS - 1 - block_index) * stride)
            for block_index in range(SEQ_DEVS - 1)
        ]
        keys_latent = jnp.concatenate(earlier + [own_latent], 0)
        key_pos = (seq_stretch - (SEQ_DEVS - 1)) * tok_rows + jnp.arange(keys_latent.shape[0])
    key_count = keys_latent.shape[0]
    if direct:
        late_grad, keys_latent = lax.optimization_barrier((out_grad, keys_latent))
        grad_all = gather(late_grad, "dp")
    else:
        grad_all = gather(out_grad, "dp")
    query = mat_dot(normed_low, query_weight).reshape(tok_rows, head_count, NOPE + ROPE)
    query = (
        jnp.concatenate(
            [
                query[..., :NOPE],
                rotate(query[..., NOPE:], cos_table[:, None, :], sin_table[:, None, :]),
            ],
            -1,
        )
        * factor
    )
    query_low = low(query)
    expanded = low(mat_dot(keys_latent[:, :R], latent_up)).reshape(
        key_count, head_count, NOPE + VD
    )
    visible = (key_pos[None, :] >= 0) & (key_pos[None, :] <= query_pos[:, None])

    def attention_scores():
        raw_scores = jnp.einsum(
            "qhd,khd->hqk",
            query_low[..., :NOPE],
            expanded[..., :NOPE],
            preferred_element_type=jnp.float32,
        )
        raw_scores = raw_scores + jnp.einsum(
            "qhd,kd->hqk",
            query_low[..., NOPE:],
            keys_latent[:, R:],
            preferred_element_type=jnp.float32,
        )
        return jnp.where(visible[None], raw_scores, masked_score)

    scores = attention_scores()
    top_score = jnp.max(scores, -1, keepdims=True)
    exp_scores = jnp.exp(scores - top_score)
    exp_total = jnp.sum(exp_scores, -1, keepdims=True)
    log_total = top_score + jnp.log(exp_total)
    probs_low = low(exp_scores / exp_total)
    heads_out = jnp.einsum(
        "hqk,khd->qhd", probs_low, expanded[..., NOPE:], preferred_element_type=jnp.float32
    )
    heads_low = low(heads_out.reshape(tok_rows, head_count * VD))
    if direct:
        cos_wide = jnp.concatenate([cos_table, cos_table], 1)
        sin_wide = jnp.concatenate([-sin_table, sin_table], 1)
        first_row = jnp.full((1,), my_group * tok_rows, jnp.int32)
        query_kept, expanded_kept, heads_low, log_kept, attn = attend(
            first_row, normed_low, query_weight, keys_latent, latent_up, out_weight, cos_wide, sin_wide
        )
        (attn,) = exchange(
            [ScatterLevels(attn.reshape(parts, rows, model_width))], 1, "scatter_attn"
        )
    else:
        attn = scatter(mat_dot(heads_low, out_weight), "tensor")

    def own_rows(value):
        return lax.dynamic_slice_in_dim(value, my_part * rows, rows, 0)

    hidden = own_rows(residual_in) + attn
    ffn_in, inv_two = rms_forward(hidden, norm_ffn_gain)
    ffn_low = low(ffn_in)
    router = router_weight.astype(jnp.float32)
    router_gates = jax.nn.sigmoid(
        jnp.dot(ffn_in, router, precision=highest, preferred_element_type=jnp.float32)
    )
    picked = jnp.any(
        own_rows(expert_ids)[..., None] == jnp.arange(experts)[None, None, :], 1
    ).astype(jnp.float32)
    chosen = picked * router_gates
    chosen_sum = jnp.sum(chosen, -1, keepdims=True)
    route = route_scale * chosen / chosen_sum
    route_high = low(route)
    route_rest = low(route - route_high.astype(jnp.float32))
    routes = jnp.concatenate([route_high, route_rest], 1)
    if direct:
        routes = jnp.pad(routes, ((0, 0), (0, 128 - 2 * experts)))
        ffn_all, routes = exchange(
            [GatherPlane(ffn_low, True), GatherPlane(routes, True)], 2, "gather_ffn"
        )
        ffn_all = ffn_all.reshape(-1, model_width)
        routes = routes.reshape(-1, 128)
        token_count = routes.shape[0]
        first_expert = jnp.full((1,), my_group * local_experts, jnp.int32)

        def own_units(value):
            return lax.dynamic_slice_in_dim(value, my_group * shared_units, shared_units, 0)

        shared_own = own_units(shared_gate.T), own_units(shared_up.T), own_units(shared_down)
        act_low, turned, ffn_grad, weight_grad = run_experts(
            experts,
            first_expert,
            ffn_all,
            grad_all,
            routes,
            expert_gate.transpose(0, 2, 1),
            expert_up.transpose(0, 2, 1),
            expert_down,
            *shared_own,
        )
        (
            expert_gate_grad,
            expert_up_grad,
            expert_down_grad,
            shared_grads,
            moe_out,
            ffn_grad,
            weight_grad,
        ) = run_weights(
            ffn_all,
            grad_all,
            act_low,
            turned,
            expert_down,
            shared_own[2],
            [
                ScatterPlane(ffn_grad.reshape(groups, parts, rows, model_width), True),
                ScatterPlane(weight_grad.reshape(groups, parts, rows, 128), True),
            ],
            3,
        )
        expert_gate_grad = expert_gate_grad.transpose(0, 2, 1).astype(jnp.float32)
        expert_up_grad = expert_up_grad.transpose(0, 2, 1).astype(jnp.float32)
        expert_down_grad = expert_down_grad.astype(jnp.float32)
        shared_grads = lax.all_to_all(
            shared_grads, "dp", split_axis=2, concat_axis=1, tiled=True
        )
        weight_grad = weight_grad[:, :experts]
    else:
        ffn_all = gather(jnp.concatenate([ffn_low, routes], 1), BOTH)
        routes = ffn_all[:, model_width:]
        ffn_all = ffn_all[:, :model_width]
        route_all = routes[:, :experts].astype(jnp.float32) + routes[
            :, experts : 2 * experts
        ].astype(jnp.float32)
        token_count = ffn_all.shape[0]
        route_own = lax.dynamic_slice_in_dim(route_all, my_group * local_experts, local_experts, 1)

        def joined(expert_weight, shared_weight):
            own = lax.dynamic_slice_in_dim(shared_weight, my_group * shared_units, shared_units, 1)
            pieces = [expert_weight[e] for e in range(local_experts)]
            return jnp.concatenate(
                pieces + [own, jnp.zeros((model_width, spare_units), jnp.bfloat16)], 1
            )

        gate_weight = joined(expert_gate, shared_gate)
        up_weight = joined(expert_up, shared_up)
        down_weight = jnp.concatenate(
            [expert_down[e] for e in range(local_experts)]
            + [
                lax.dynamic_slice_in_dim(shared_down, my_group * shared_units, shared_units, 0),
                jnp.zeros((spare_units, model_width), jnp.bfloat16),
            ],
            0,
        )
        scale = jnp.concatenate(
            [
                jnp.broadcast_to(route_own[:, e : e + 1], (token_count, units))
                for e in range(local_experts)
            ]
            + [jnp.ones((token_count, shared_units + spare_units), jnp.float32)],
            1,
        )
        plain_grad = contract_cols(grad_all, down_weight)
        gate_act = mat_dot(ffn_all, gate_weight)
        up_act = mat_dot(ffn_all, up_weight)
        logistic = jax.nn.sigmoid(gate_act)
        silu = gate_act * logistic
        act = silu * up_act
        act_low = low(act * scale)
        act_grad = plain_grad * scale
        gate_grad = low(act_grad * up_act * logistic * (1.0 + gate_act * (1.0 - logistic)))
        up_grad = low(act_grad * silu)
        weight_dots = act * plain_grad
        weight_grad = jnp.stack(
            [
                jnp.sum(weight_dots[:, e * units : (e + 1) * units], 1)
                for e in range(local_experts)
            ],
            1,
        )
        weight_grad = lax.dynamic_update_slice_in_dim(
            jnp.zeros((token_count, experts), jnp.bfloat16),
            low(weight_grad),
            my_group * local_experts,
            1,
        )
        ffn_grad = contract_cols(gate_grad, gate_weight) + contract_cols(up_grad, up_weight)
        ffn_grad = scatter(jnp.concatenate([low(ffn_grad), weight_grad], 1), BOTH)
        weight_grad = ffn_grad[:, model_width:]
        ffn_grad = ffn_grad[:, :model_width]
        moe_out = mat_dot(act_low, down_weight)

        down_grad = contract_rows(act_low, grad_all)
        gate_weight_grad = contract_rows(ffn_all, gate_grad)
        up_weight_grad = contract_rows(ffn_all, up_grad)
        expert_down_grad = down_grad[: local_experts * units].reshape(local_experts, units, -1)
        expert_gate_grad = jnp.stack(
            [gate_weight_grad[:, e * units : (e + 1) * units] for e in range(local_experts)]
        )
        expert_up_grad = jnp.stack(
            [up_weight_grad[:, e * units : (e + 1) * units] for e in range(local_experts)]
        )

        def swap(value):
            return lax.all_to_all(low(value), "dp", split_axis=0, concat_axis=1, tiled=True).astype(
                jnp.float32
            )

        first = local_experts * units
        shared_gate_grad = swap(gate_weight_grad[:, first:used_units])
        shared_up_grad = swap(up_weight_grad[:, first:used_units])
        shared_down_grad = lax.all_to_all(
            low(down_grad[first:used_units]), "dp", split_axis=1, concat_axis=0, tiled=True
        ).astype(jnp.float32)

    moe_out = lax.psum_scatter(low(moe_out), "dp", scatter_dimension=0, tiled=True)

    inner_sum = jnp.sum(weight_grad * chosen, -1, keepdims=True)
    chosen_grad = route_scale * (weight_grad / chosen_sum - inner_sum / (chosen_sum * chosen_sum))
    logit_grad = chosen_grad * chosen * (1.0 - chosen)
    router_grad = jnp.dot(
        ffn_in.T, logit_grad, precision=highest, preferred_element_type=jnp.float32
    )
    norm_grad = ffn_grad + jnp.dot(
        logit_grad, router.T, precision=highest, preferred_element_type=jnp.float32
    )
    hidden_extra, norm_ffn_grad = rms_backward(hidden, inv_two, norm_ffn_gain, norm_grad)
    hidden_grad = own_rows(out_grad).astype(jnp.float32) + hidden_extra
    if direct:
        (attn_grad_low,) = exchange([GatherLevels(low(hidden_grad))], 4, "gather_hidden")
        attn_grad_low = attn_grad_low.reshape(tok_rows, model_width)
    else:
        attn_grad_low = gather(low(hidden_grad), "tensor")

    out_weight_grad = scatter(contract_rows(heads_low, attn_grad_low), "dp", 1)
    if direct:
        query_grad_low, latent_up_grad, latent_grad = attend_back(
            first_row,
            query_kept,
            expanded_kept,
            keys_latent,
            log_kept,
            attn_grad_low,
            out_weight,
            latent_up,
            cos_wide,
            sin_wide,
        )
        moe_out, shared_grads, _ = lax.optimization_barrier(
            (moe_out, shared_grads, query_grad_low)
        )
        shared_grads = shared_grads.astype(jnp.float32)
        shared_gate_grad, shared_up_grad = shared_grads[0].T, shared_grads[1].T
        shared_down_grad = shared_grads[2]
    else:
        heads_grad = low(contract_cols(attn_grad_low, out_weight)).reshape(tok_rows, head_count, VD)
        attn_probs = jnp.exp(attention_scores() - log_total)
        probs_low = low(attn_probs)
        value_grad = jnp.einsum(
            "hqk,qhd->khd", probs_low, heads_grad, preferred_element_type=jnp.float32
        )
        prob_grad = jnp.einsum(
            "qhd,khd->hqk", heads_grad, expanded[..., NOPE:], preferred_element_type=jnp.float32
        )
        row_delta = jnp.sum(attn_probs * prob_grad, -1, keepdims=True)
        score_grad = low(attn_probs * (prob_grad - row_delta))
        nope_grad = jnp.einsum(
            "hqk,khd->qhd", score_grad, expanded[..., :NOPE], preferred_element_type=jnp.float32
        )
        rope_grad = jnp.einsum(
            "hqk,kd->qhd", score_grad, keys_latent[:, R:], preferred_element_type=jnp.float32
        )
        key_nope_grad = jnp.einsum(
            "hqk,qhd->khd", score_grad, query_low[..., :NOPE], preferred_element_type=jnp.float32
        )
        key_rope_grad = jnp.einsum(
            "hqk,qhd->kd", score_grad, query_low[..., NOPE:], preferred_element_type=jnp.float32
        )
        expand_grad = low(
            jnp.concatenate([key_nope_grad, value_grad], -1).reshape(
                key_count, head_count * (NOPE + VD)
            )
        )
        latent_up_grad = contract_rows(keys_latent[:, :R], expand_grad)
        latent_grad = jnp.concatenate([contract_cols(expand_grad, latent_up), key_rope_grad], -1)
        query_grad = (
            jnp.concatenate(
                [nope_grad, unrotate(rope_grad, cos_table[:, None, :], sin_table[:, None, :])], -1
            )
            * factor
        )
        query_grad_low = low(query_grad.reshape(tok_rows, head_count * (NOPE + ROPE)))
    block_out = low(hidden + scatter(moe_out, "tensor"))
    query_weight_grad = contract_rows(normed_low, query_grad_low)
    input_part = contract_cols(query_grad_low, query_weight)
    if direct:
        own_grad, input_sum = exchange(
            [
                ScatterPlane(low(latent_grad).reshape(groups, parts, rows, R + ROPE), True),
                ScatterLevels(low(input_part).reshape(parts, rows, model_width)),
            ],
            5,
            "scatter_latent",
        )
    else:
        if stride == 1:
            own_grad = scatter(scatter(latent_grad, "dp"), "tensor")
        else:
            own_grad = latent_grad[(SEQ_DEVS - 1) * tok_rows :]
            for block_index in range(SEQ_DEVS - 1):
                piece_grad = latent_grad[block_index * tok_rows : (block_index + 1) * tok_rows]
                own_grad = own_grad + from_behind(
                    low(piece_grad), "dp", -(SEQ_DEVS - 1 - block_index) * stride
                ).astype(piece_grad.dtype)
            own_grad = scatter(own_grad, "tensor")
        input_sum = scatter(input_part, "tensor")
        query_weight_grad = scatter(query_weight_grad, "dp")
        latent_up_grad = scatter(latent_up_grad, "dp")
    compressed_own = own_rows(compressed)
    normed_part, latent_gain_grad = rms_backward(
        compressed_own[:, :R], own_rows(inv_latent), latent_gain, own_grad[:, :R]
    )
    compressed_grad = low(
        jnp.concatenate(
            [normed_part, unrotate(own_grad[:, R:], own_rows(cos_table), own_rows(sin_table))], -1
        )
    )
    latent_down_grad = contract_rows(own_rows(normed_low), compressed_grad)
    normed_grad = input_sum + contract_cols(compressed_grad, latent_down)
    input_extra, norm_attn_grad = rms_backward(
        own_rows(residual_in), own_rows(inv_one), norm_attn_gain, normed_grad
    )
    tokens_grad = low(hidden_grad + input_extra)
    small = [norm_attn_grad, latent_gain_grad, norm_ffn_grad, router_grad]
    sizes = [one.size // groups for one in small]
    small = jnp.concatenate([one.reshape(groups, -1) for one in small], 1)
    if direct:
        small = jnp.pad(low(small), ((0, 0), (0, parts * 2048 - small.shape[1])))
        (
            latent_down_grad,
            small,
            tokens_grad,
            query_weight_grad,
            latent_up_grad,
            block_out,
        ) = exchange(
            [
                ScatterPlane(
                    low(latent_down_grad).reshape(groups, parts, rows, R + ROPE), True, True
                ),
                ScatterPlane(small.reshape(groups, parts, 16, 128), True, True),
                GatherLevels(tokens_grad),
                ScatterPlane(low(query_weight_grad).reshape(groups, 2, model_width // 16, -1), False),
                ScatterPlane(low(latent_up_grad).reshape(groups, 2, R // 16, -1), False),
                GatherLevels(block_out),
            ],
            6,
            "scatter_last",
            [0, 0, 0, 6, 6, 11],
        )
        latent_down_grad = latent_down_grad.reshape(-1, R + ROPE).astype(jnp.float32)
        small = small.reshape(-1).astype(jnp.float32)
        query_weight_grad = query_weight_grad.reshape(model_width // groups, -1)
        latent_up_grad = latent_up_grad.reshape(R // groups, -1)
        block_out = block_out.reshape(tok_rows, model_width)
        tokens_grad = tokens_grad.reshape(tok_rows, model_width)
    else:
        latent_down_grad = lax.psum(scatter(latent_down_grad, "dp"), "tensor")
        small = lax.psum(scatter(small, "dp"), "tensor").reshape(-1)
        tokens_grad = gather(tokens_grad, "tensor")
        block_out = gather(block_out, "tensor")
    offsets = [sum(sizes[:k]) for k in range(len(sizes))]
    norm_attn_grad, latent_gain_grad, norm_ffn_grad, router_grad = [
        small[start : start + size] for start, size in zip(offsets, sizes)
    ]

    return (
        block_out,
        tokens_grad,
        norm_attn_grad,
        query_weight_grad,
        latent_down_grad,
        latent_gain_grad,
        latent_up_grad,
        out_weight_grad,
        norm_ffn_grad,
        router_grad.reshape(-1, experts),
        shared_gate_grad,
        shared_up_grad,
        shared_down_grad,
        expert_gate_grad,
        expert_up_grad,
        expert_down_grad,
    )


def solution(mesh):
    in_specs = (
        P("dp", None),
        P(),
        P(None, "tensor"),
        P(),
        P(),
        P(None, "tensor"),
        P("tensor", None),
        P(),
        P(),
        P(None, "tensor"),
        P(None, "tensor"),
        P("tensor", None),
        P("dp", None, "tensor"),
        P("dp", None, "tensor"),
        P("dp", "tensor", None),
        P("dp", None),
        P("dp", None),
    )
    out_specs = (
        P("dp", None),
        P("dp", None),
        P("dp"),
        P("dp", "tensor"),
        P("dp", None),
        P("dp"),
        P("dp", "tensor"),
        P("tensor", "dp"),
        P("dp"),
        P("dp", None),
        P("dp", "tensor"),
        P("dp", "tensor"),
        P("tensor", "dp"),
        P("dp", None, "tensor"),
        P("dp", None, "tensor"),
        P("dp", "tensor", None),
    )
    return jax.shard_map(shards, mesh=mesh, in_specs=in_specs, out_specs=out_specs, check_vma=False)
```
